128 devices in a mesh: vocab: 8 (over z, core), dp: 16 (over x, y).
Axes of the slice: x: 4, y: 4, z: 4, core: 2. Of those that a mesh axis runs over, the one named last changes fastest.
Arguments:
- hidden: bfloat16 [5632, 4096], P('dp'), may hold values from -240 to 240
- output_projection_weight: bfloat16 [4096, 32768], P('dp', 'vocab'), may hold values from -0.25 to 0.25
- adapter_down_weight: bfloat16 [4096, 128], replicated, may hold values from -0.09375 to 0.09375
- adapter_up_weight: bfloat16 [128, 32768], P(None, 'vocab'), may hold values from -0.75 to 0.75
- labels: int32 [5632], P('dp'), may hold values from 0 to 32767
- token_job_index: int32 [5632], P('dp'), may hold values from 0 to 7, as said below
Outputs:
- logits: bfloat16 [5632, 32768], P('dp', 'vocab')
- logit_gradient_rows: bfloat16 [5632, 32768], P('dp', 'vocab')
- hidden_state_gradient: bfloat16 [5632, 4096], P('dp')
- token_loss: float32 [5632], P('dp')
- job_loss: float32 [8], replicated
The draws below stay inside these ranges and needn't reach their ends.
Inputs may be any that keep to these rules, and one draw needn't show every extreme that they name: `token_job_index`: a job may have no tokens at all, and the jobs' token counts differ widely.
All inputs are finite; a program needn't handle non-finite values.
Results may differ from the reference program's by a relative error of at most 0.014.
Values may be sent and summed in bfloat16 or wider, within the bound.
A program may use at most 256 MiB of HBM per device.

```python
import math
import jax
import jax.numpy as jnp
from jax import lax

MODEL_WIDTH = 4096
ADAPTER_JOBS = 8
ADAPTER_RANK = 16
TOKENS = 5632
VOCAB_ENTRIES = 32768


def draw_hidden(key, part):
    values = jnp.clip(jax.random.normal(key, (TOKENS, MODEL_WIDTH), jnp.float32), -6.0, 6.0)
    return values.astype(jnp.bfloat16)


def draw_token_job_index(key, part):
    order_key = jax.random.fold_in(key, 11)
    ticket_key = jax.random.fold_in(key, 12)
    order = jax.random.permutation(order_key, ADAPTER_JOBS).astype(jnp.int32)
    shares = [840 // (place + 1) for place in range(ADAPTER_JOBS - 1)] + [0]
    bounds_list = []
    running = 0
    for share in shares:
        running = running + share
        bounds_list.append(running)
    total_tickets = running
    bounds = jnp.array(bounds_list, dtype=jnp.int32)
    tickets = jax.random.randint(ticket_key, (TOKENS,), 0, total_tickets, dtype=jnp.int32)
    places = jnp.sum((tickets[:, None] >= bounds[None, :]).astype(jnp.int32), axis=1)
    return jnp.take(order, places).astype(jnp.int32)


def touch_ends(values, own_key, smallest, high):
    spot = [jax.random.randint(jax.random.fold_in(own_key, axis), (), 0, length) for axis, length in enumerate(values.shape)]
    main_axis = values.shape.index(max(values.shape))
    next_to = spot[:main_axis] + [(spot[main_axis] + 1) % values.shape[main_axis]] + spot[main_axis + 1:]
    return values.at[tuple(spot)].set(smallest).at[tuple(next_to)].set(high)


def shard_levels(own_key, extent, shards, smallest, high):
    gain, own = 1.0, jax.random.fold_in(own_key, 6)
    for dim, blocks in shards:
        draws = jnp.exp(jax.random.uniform(jax.random.fold_in(own, dim), (blocks,), jnp.float32, smallest / len(shards), high / len(shards)))
        gain = gain * jnp.repeat(draws, extent[dim] // blocks).reshape([-1 if axis == dim else 1 for axis in range(len(extent))])
    return gain


def bell_draw(rng, dims, width, bound, split=(), kind=jnp.bfloat16):
    level = shard_levels(rng, dims, split, -0.22, 0.18) if split else 1.0
    entries = jax.random.normal(rng, dims, jnp.float32) * width * level
    return jnp.minimum(jnp.maximum(entries, -bound), bound).astype(kind)


def setup_inputs(seed: int = 0) -> dict:
    key_list = jax.random.split(jax.random.key(seed), 7)
    return {
        "hidden": draw_hidden(jax.random.fold_in(key_list[6], 71), 0),
        "output_projection_weight": bell_draw(key_list[1], (MODEL_WIDTH, VOCAB_ENTRIES), (MODEL_WIDTH // 9) ** -0.5, 0.25, ((0, 16), (1, 8))),
        "adapter_down_weight": bell_draw(key_list[2], (MODEL_WIDTH, ADAPTER_JOBS * ADAPTER_RANK), MODEL_WIDTH ** -0.5, 0.09375),
        "adapter_up_weight": bell_draw(key_list[3], (ADAPTER_JOBS * ADAPTER_RANK, VOCAB_ENTRIES), (4 * ADAPTER_RANK) ** -0.5, 0.75, ((1, 8),)),
        "labels": touch_ends(jax.random.randint(key_list[4], (TOKENS,), 0, VOCAB_ENTRIES), jax.random.fold_in(key_list[4], 1), 0, VOCAB_ENTRIES - 1).astype(jnp.int32),
        "token_job_index": draw_token_job_index(jax.random.fold_in(key_list[6], 71), 0),
    }


def reference(hidden, output_projection_weight, adapter_down_weight, adapter_up_weight, labels, token_job_index):
    adapter_job_columns = ADAPTER_JOBS * ADAPTER_RANK
    col_job = lax.iota(jnp.int32, adapter_job_columns) // ADAPTER_RANK
    onehot = (token_job_index[:, None] == lax.iota(jnp.int32, ADAPTER_JOBS)[None, :]).astype(jnp.float32)
    counts = jnp.sum(onehot, axis=0)
    per_job = TOKENS / (ADAPTER_JOBS * jnp.maximum(counts, 1.0))
    block = math.gcd(TOKENS, 512)
    steps_count = TOKENS // block

    def one_block(index):
        start = (index * block).astype(jnp.int32)
        hidden_input = lax.dynamic_slice_in_dim(hidden, start, block, 0)
        lab = lax.dynamic_slice_in_dim(labels, start, block, 0)
        jid = lax.dynamic_slice_in_dim(token_job_index, start, block, 0)
        adapter_job_mask = (jid[:, None] == col_job[None, :]).astype(jnp.float32)
        adapter_input = (jnp.dot(hidden_input, adapter_down_weight, preferred_element_type=jnp.float32) * adapter_job_mask).astype(jnp.bfloat16)
        complete_logit_rows = jnp.dot(hidden_input, output_projection_weight, preferred_element_type=jnp.float32) + jnp.dot(adapter_input, adapter_up_weight, preferred_element_type=jnp.float32)
        row_max = jnp.max(complete_logit_rows, axis=1)
        shifted = jnp.exp(complete_logit_rows - row_max[:, None])
        exp_total = jnp.sum(shifted, axis=1)
        target_hit = lax.iota(jnp.int32, VOCAB_ENTRIES)[None, :] == lab[:, None]
        target = jnp.sum(jnp.where(target_hit, complete_logit_rows, 0.0), axis=1)
        token_loss = row_max + jnp.log(exp_total) - target
        token_weight = jnp.sum((jid[:, None] == lax.iota(jnp.int32, ADAPTER_JOBS)[None, :]).astype(jnp.float32) * per_job[None, :], axis=1)
        logit_gradient_rows = (token_weight[:, None] * (shifted / exp_total[:, None] - target_hit.astype(jnp.float32))).astype(jnp.bfloat16)
        adapter_gradient = jnp.dot(logit_gradient_rows, adapter_up_weight.T, preferred_element_type=jnp.float32)
        hidden_state_gradient = jnp.dot(logit_gradient_rows, output_projection_weight.T, preferred_element_type=jnp.float32) + jnp.dot(adapter_gradient * adapter_job_mask, adapter_down_weight.astype(jnp.float32).T, precision=lax.Precision.HIGHEST)
        return complete_logit_rows.astype(jnp.bfloat16), logit_gradient_rows, hidden_state_gradient.astype(jnp.bfloat16), token_loss

    logits, logit_gradient_rows, hidden_state_gradient, token_loss = lax.map(one_block, jnp.arange(steps_count, dtype=jnp.int32))
    logits = logits.reshape(TOKENS, VOCAB_ENTRIES)
    logit_gradient_rows = logit_gradient_rows.reshape(TOKENS, VOCAB_ENTRIES)
    hidden_state_gradient = hidden_state_gradient.reshape(TOKENS, MODEL_WIDTH)
    token_loss = token_loss.reshape(TOKENS)
    job_loss = jnp.sum(onehot * token_loss[:, None], axis=0) / jnp.maximum(counts, 1.0)
    return logits, logit_gradient_rows, hidden_state_gradient, token_loss, job_loss
```

```python
import functools

import jax
import jax.numpy as jnp
from jax import lax
from jax.experimental import pallas as pl
from jax.experimental.pallas import tpu as pltpu
from jax.sharding import Mesh
from jax.sharding import PartitionSpec as P

MESH = pl.DeviceIdType.MESH
F32 = jnp.float32
BF16 = jnp.bfloat16

JOBS = 8
RANK = 16
NX = NY = NZ = 4
NC = 2
T = 352
S = NX * T
HT = T // 2
D = 4096
DB = D // (NX * NY)
V = 4096
U = V // NX
CW = 256
NK = U // CW
SH = D // (NZ * NC)
TOKENS = S * NY
NB = S // 128


def fdot(a, b):
    return jnp.dot(a, b, preferred_element_type=F32)


def tdot(a, b):
    return lax.dot_general(a, b, (((1,), (1,)), ((), ())), preferred_element_type=F32)


def kernel(
    hid, w, ad, au, aux,
    lg, gr, hg, tl, jl,
    H, W5, WS, E, LT, G5, RC, RR, R0, XS, XR, FO, AG, COL, COL2, LI, AU, AX, STA, STB, JR, CN, JL,
    ssem, rsem, lsem,
):
    z, c, x, y = (lax.axis_index(a) for a in ("z", "c", "x", "y"))
    v = z * NC + c

    def al(i, m):
        return pl.multiple_of(i, m)

    def xn(r):
        return lax.rem(x + r, NX)

    def yn(r):
        return lax.rem(y + r, NY)

    def zn(r):
        return lax.rem(z + r, NZ)

    used = {"s": 0, "r": 0, "l": 0}

    def take(kind, n=1):
        at = used[kind]
        used[kind] = at + n
        return at

    pending = []

    def rcopy(src, dst, si, ri, dev):
        return pltpu.make_async_remote_copy(
            src_ref=src, dst_ref=dst, send_sem=ssem.at[si], recv_sem=rsem.at[ri],
            device_id=dev, device_id_type=MESH,
        )

    def send(src, dst, ri, dev, keep=pending):
        d = rcopy(src, dst, take("s"), ri, dev)
        d.start()
        keep.append(d)

    def got(dst, ri):
        rcopy(dst, dst, 0, ri, {"x": xn(1)}).wait_recv()

    def load(src, dst, keep):
        d = pltpu.make_async_copy(src, dst, lsem.at[take("l")])
        d.start()
        keep.append(d)

    def drain(keep):
        for d in keep:
            d.wait()
        keep.clear()

    def drain_sends(keep):
        for d in keep:
            d.wait_send()
        keep.clear()

    bar = pltpu.get_barrier_semaphore()
    peers = (
        [{"x": xn(r)} for r in (1, 2, 3)]
        + [{"y": yn(r)} for r in (1, 2, 3)]
        + [{"z": zn(a), "c": lax.rem(c + b, NC)} for a in range(NZ) for b in range(NC) if a or b]
    )
    for dev in peers:
        pl.semaphore_signal(bar, inc=1, device_id=dev, device_id_type=MESH)

    first, own_h, rest = [], [], []
    load(w, WS, first)
    for p in range(NX * NY):
        n = (p % NX) * NY + p // NX
        load(hid.at[:, pl.ds(n * DB, DB)], H.at[pl.ds(al(x * T, 16), T), pl.ds(p * DB, DB)], own_h)
    load(aux, AX.at[x], first)
    own_rows = pl.ds(al((y * NX + x) * DB, DB), DB)
    load(w.at[:, pl.ds(al(x * U, U), U)], W5.at[own_rows, pl.ds(0, U)], first)
    load(au.at[:, pl.ds(al(x * U, U), U)], AU, rest)
    for p in range(NX * NY):
        n = (p % NX) * NY + p // NX
        for q in range(2):
            load(
                ad.at[pl.ds(n * DB, DB), :],
                W5.at[pl.ds(p * DB, DB), pl.ds(U + q * 128, 128)],
                rest,
            )
    pl.semaphore_wait(bar, len(peers))

    ORDER = (1, 3, 2)
    wx = take("r", NK * 3)
    hx = take("r", 3)
    ax = take("r", 3)
    wy = take("r", NK * 4)
    hz = take("r", 3 * 4)
    hc = take("r", 3 * 5)

    def wblock(row, k):
        return W5.at[row, pl.ds(k * CW, CW)]

    def send_w(k):
        for r in ORDER:
            send(
                WS.at[:, pl.ds(al(xn(r) * U + k * CW, CW), CW)],
                wblock(own_rows, k), wx + k * 3 + r - 1, {"x": xn(r)},
            )

    drain(first)
    send_w(0)
    for r in ORDER:
        send(AX.at[x], AX.at[x], ax + r - 1, {"x": xn(r)})
    drain(own_h)
    hsends = []

    def hpiece(xb, share, lo=0, n=T):
        return H.at[pl.ds(al(xb * T + lo, 16), n), pl.ds(al(share * SH, SH), SH)]

    for r in ORDER:
        send(hpiece(x, v), hpiece(x, v), hx + r - 1, {"x": xn(r)}, hsends)
    for k in range(1, NK):
        send_w(k)

    def ysrc(dy, k, lo=0, n=NX * DB):
        return wblock(pl.ds(al(yn(dy) * (NX * DB) + lo, DB), n), k)

    HB = NX * DB // 2

    def w_own(k):
        for r in ORDER:
            row = pl.ds(al((y * NX + lax.rem(x + NX - r, NX)) * DB, DB), DB)
            got(wblock(row, k), wx + k * 3 + r - 1)
        send(ysrc(0, k), ysrc(0, k), wy + k * 4 + 0, {"y": yn(1)})
        send(ysrc(0, k), ysrc(0, k), wy + k * 4 + 1, {"y": yn(3)})

    def w_fwd(k):
        got(ysrc(3, k), wy + k * 4 + 0)
        send(ysrc(3, k, 0, HB), ysrc(3, k, 0, HB), wy + k * 4 + 2, {"y": yn(1)})
        got(ysrc(1, k), wy + k * 4 + 1)
        send(ysrc(1, k, HB, HB), ysrc(1, k, HB, HB), wy + k * 4 + 3, {"y": yn(3)})

    def w_end(k):
        got(ysrc(2, k, 0, HB), wy + k * 4 + 2)
        got(ysrc(2, k, HB, HB), wy + k * 4 + 3)

    other = {"c": 1 - c}

    def h_in(r):
        xb = lax.rem(x + NX - r, NX)
        got(hpiece(xb, v), hx + r - 1)
        mine = hpiece(xb, v)
        b = hz + (r - 1) * 4
        send(mine, mine, b + 0, {"z": zn(1)}, hsends)
        send(mine, mine, b + 1, {"z": zn(3)}, hsends)
        send(mine, mine, hc + (r - 1) * 5, other, hsends)

    def h_fwd(r):
        xb = lax.rem(x + NX - r, NX)
        b, d = hz + (r - 1) * 4, hc + (r - 1) * 5
        left, right = zn(3) * NC + c, zn(1) * NC + c
        got(hpiece(xb, left), b + 0)
        send(hpiece(xb, left, 0, HT), hpiece(xb, left, 0, HT), b + 2, {"z": zn(1)}, hsends)
        send(hpiece(xb, left), hpiece(xb, left), d + 1, other, hsends)
        got(hpiece(xb, right), b + 1)
        send(hpiece(xb, right, HT, HT), hpiece(xb, right, HT, HT), b + 3, {"z": zn(3)}, hsends)
        send(hpiece(xb, right), hpiece(xb, right), d + 2, other, hsends)

    def h_last(r):
        xb = lax.rem(x + NX - r, NX)
        b, d = hz + (r - 1) * 4, hc + (r - 1) * 5
        far = zn(2) * NC + c
        got(hpiece(xb, far, 0, HT), b + 2)
        send(hpiece(xb, far, 0, HT), hpiece(xb, far, 0, HT), d + 3, other, hsends)
        got(hpiece(xb, far, HT, HT), b + 3)
        send(hpiece(xb, far, HT, HT), hpiece(xb, far, HT, HT), d + 4, other, hsends)

    def h_end(r):
        xb = lax.rem(x + NX - r, NX)
        d = hc + (r - 1) * 5
        k = 1 - c
        got(hpiece(xb, v - c + k), d)
        got(hpiece(xb, zn(3) * NC + k), d + 1)
        got(hpiece(xb, zn(1) * NC + k), d + 2)
        got(hpiece(xb, zn(2) * NC + k, 0, HT), d + 3)
        got(hpiece(xb, zn(2) * NC + k, HT, HT), d + 4)

    w_own(0)
    for r in ORDER:
        h_in(r)
    w_own(1)
    w_fwd(0)
    h_fwd(1)
    w_own(2)
    h_fwd(3)
    h_last(1)
    w_fwd(1)
    h_fwd(2)
    h_last(3)
    w_own(3)

    for r in ORDER:
        got(AX.at[lax.rem(x + NX - r, NX)], ax + r - 1)
    sub = lax.broadcasted_iota(jnp.int32, (8, 128), 0).astype(F32)
    subi = lax.broadcasted_iota(jnp.int32, (8, 128), 0)
    counts = jnp.zeros((8, 128), F32)
    for xb in range(NX):
        for q in range(3):
            tile = AX[xb, q]
            n = min(128, T - q * 128)
            turned = jnp.concatenate([tile, jnp.zeros((120, 128), F32)], axis=0).T
            COL[pl.ds(xb * T + q * 128, n), :] = turned[:n]
            counts = counts + (tile[1:2, :] == sub).astype(F32)
    CN[y] = counts
    cn = take("r", 3)
    for r in (1, 3, 2):
        send(CN.at[y], CN.at[y], cn + r - 1, {"y": yn(r)})
    drain(rest)
    w_fwd(2)
    h_last(2)
    w_end(0)
    for r in ORDER:
        h_end(r)
    drain_sends(hsends)

    lane128 = lax.broadcasted_iota(jnp.int32, (T, 128), 1)
    rank_job = (lane128 // RANK).astype(F32)

    def lora_in(m, carry):
        rows = pl.ds(al(m * T, 16), T)
        hit = COL[rows, 1:2] == rank_job
        a = fdot(H[rows, :], W5[:, U : U + 128])
        LI[rows, :] = jnp.where(hit, a, 0.0).astype(BF16)
        return carry

    lax.fori_loop(0, NX, lora_in, 0)

    base = v * V + x * U
    lane_cw = lax.broadcasted_iota(jnp.int32, (T, CW), 1)
    lgs = take("r", NK * 3)
    outs = []
    my_cols = al(x * U, U)

    def forward(k):
        def step(m, carry):
            rows = pl.ds(al(m * T, 16), T)
            a = fdot(H[rows, :], W5[:, k * CW : (k + 1) * CW])
            a = a + fdot(LI[rows, :], AU[:, k * CW : (k + 1) * CW])
            LT[rows, k * CW : (k + 1) * CW] = a.astype(BF16)
            top = jnp.max(a, axis=1, keepdims=True)
            e = jnp.exp(a - top)
            E[k, rows, :] = e
            total = jnp.sum(e, axis=1, keepdims=True)
            cols = (lane_cw + (base + k * CW)).astype(F32)
            target = jnp.sum(jnp.where(cols == COL[rows, 0:1], a, 0.0), axis=1, keepdims=True)
            old = COL[rows, :]
            old = jnp.where(lane128 == 8 + k, top, old)
            old = jnp.where(lane128 == 12 + k, total, old)
            COL[rows, :] = jnp.where(lane128 == 16 + k, target, old)
            return carry

        lax.fori_loop(0, NX, step, 0)

    def send_logits(k):
        for r in ORDER:
            send(
                LT.at[pl.ds(al(xn(r) * T, 16), T), pl.ds(k * CW, CW)],
                lg.at[:, pl.ds(al(my_cols + k * CW, CW), CW)],
                lgs + k * 3 + r - 1, {"x": xn(r)},
            )
        load(
            LT.at[pl.ds(al(x * T, 16), T), pl.ds(k * CW, CW)],
            lg.at[:, pl.ds(al(my_cols + k * CW, CW), CW)], outs,
        )

    forward(0)
    send_logits(0)
    w_end(1)
    forward(1)
    send_logits(1)
    w_fwd(3)
    w_end(2)
    forward(2)
    send_logits(2)
    w_end(3)
    forward(3)

    def row_stats(b, carry):
        t = COL[pl.ds(al(b * 128, 128), 128), :].T
        m, s, g = t[8:12], t[12:16], t[16:20]
        top = jnp.max(m, axis=0, keepdims=True)
        s = jnp.sum(s * jnp.exp(m - top), axis=0, keepdims=True)
        g = jnp.sum(g, axis=0, keepdims=True)
        JR[b] = jnp.broadcast_to(t[1:2], (8, 128))
        STA[v, b] = jnp.where(subi == 0, top, jnp.where(subi == 1, s, jnp.where(subi == 2, g, 0.0)))
        return carry

    lax.fori_loop(0, NB, row_stats, 0)
    sa = take("r", 7)
    sb = take("r", 3)
    turns = [(a, b) for a in (2, 1, 3, 0) for b in range(NC) if a or b]
    for a, b in turns:
        dev = {"z": zn(a), "c": lax.rem(c + b, NC)}
        send(STA.at[v], STA.at[v], sa + a * NC + b - 1, dev)
    for a, b in turns:
        src = lax.rem(z + NZ - a, NZ) * NC + lax.rem(c + b, NC)
        got(STA.at[src], sa + a * NC + b - 1)

    def joined(parts):
        top = functools.reduce(jnp.maximum, [p[0:1] for p in parts])
        s = functools.reduce(jnp.add, [p[1:2] * jnp.exp(p[0:1] - top) for p in parts])
        g = functools.reduce(jnp.add, [p[2:3] for p in parts])
        return top, s, g

    def stage_b(b, carry):
        top, s, g = joined([STA[i, b] for i in range(NZ * NC)])
        STB[x, b] = jnp.where(subi == 0, top, jnp.where(subi == 1, s, jnp.where(subi == 2, g, 0.0)))
        return carry

    lax.fori_loop(0, NB, stage_b, 0)
    for r in (2, 1, 3):
        send(STB.at[x], STB.at[x], sb + r - 1, {"x": xn(r)})
    send_logits(3)
    for r in (1, 3, 2):
        got(CN.at[lax.rem(y + NY - r, NY)], cn + r - 1)
    counts = jnp.sum(CN[0] + CN[1] + CN[2] + CN[3], axis=1, keepdims=True)
    counts = jnp.maximum(counts, 1.0)
    per_job = TOKENS / (JOBS * counts)
    for r in (2, 1, 3):
        got(STB.at[lax.rem(x + NX - r, NX)], sb + r - 1)

    def finish(b, job_sums):
        top, s, g = joined([STB[i, b] for i in range(NX)])
        onehot = (JR[b] == sub).astype(F32)
        loss = top + jnp.log(s) - g
        weight = jnp.sum(onehot * per_job, axis=0, keepdims=True)
        tile = jnp.where(
            subi == 0, top,
            jnp.where(subi == 1, weight / s, jnp.where(subi == 2, weight, jnp.where(subi == 3, loss, 0.0))),
        )
        turned = jnp.concatenate([tile, jnp.zeros((120, 128), F32)], axis=0).T
        COL2[pl.ds(al(b * 128, 128), 128), :] = turned
        return job_sums + onehot * loss

    JL[y] = lax.fori_loop(0, NB, finish, jnp.zeros((8, 128), F32))
    jn = take("r", 3)
    for r in (1, 3, 2):
        send(JL.at[y], JL.at[y], jn + r - 1, {"y": yn(r)})
    tl[...] = COL2[pl.ds(al(x * T, 8), T), :]

    def gradient(m, carry):
        rows = pl.ds(al(m * T, 16), T)
        lab = COL[rows, 0:1]
        weight = COL2[rows, 2:3]
        for k in range(NK):
            f = jnp.exp(COL[rows, 8 + k : 9 + k] - COL2[rows, 0:1]) * COL2[rows, 1:2]
            cols = (lane_cw + (base + k * CW)).astype(F32)
            g = E[k, rows, :] * f - jnp.where(cols == lab, weight, 0.0)
            G5[m, :, k * CW : (k + 1) * CW] = g.astype(BF16)
        part = tdot(G5[m, :, 0:U], AU[...])
        part = jnp.where(COL[rows, 1:2] == rank_job, part, 0.0)
        high = part.astype(BF16)
        G5[m, :, U : U + 128] = high
        G5[m, :, U + 128 : U + 256] = (part - high.astype(F32)).astype(BF16)
        return carry

    lax.fori_loop(0, NX, gradient, 0)
    grs = take("r", 3)
    for r in ORDER:
        send(G5.at[xn(r), :, pl.ds(0, U)], gr.at[:, pl.ds(my_cols, U)], grs + r - 1, {"x": xn(r)})
    load(G5.at[x, :, pl.ds(0, U)], gr.at[:, pl.ds(my_cols, U)], outs)

    cs_s, cs_r = take("s", 16), take("r", 16)
    ring_s, ring_r = take("s", 12), take("r", 12)

    def zt(s, h):
        return lax.rem(z + NZ + (2 * h - 1) * (s + 1), NZ)

    def unit(s, h, j, core):
        at = al((zt(s, h) * NC + core) * SH + h * CW, CW)
        g = G5[:, pl.ds(al(j * HT, 16), HT), :].reshape(NX * HT, U + 256)
        return tdot(g, W5[pl.ds(at, CW), :])

    def ps(i):
        return H.at[pl.ds(al(lax.rem(i, 2) * (S // 2), 16), S // 2), pl.ds(al(i // 2 * CW, CW), CW)]

    def ps_copy(i):
        return rcopy(ps(i), RC.at[i], cs_s + i, cs_r + i, other)

    def for_core(s):
        def step(q, carry):
            j, h = q // 2, lax.rem(q, 2)
            i = s * 4 + h * 2 + j
            ps(i)[...] = unit(s, h, j, 1 - c).astype(BF16)
            ps_copy(i).start()
            return carry

        lax.fori_loop(0, 4, step, 0)

    def ring_copy(s, h, j):
        i = h * 2 + j
        src = R0.at[i] if s == 0 else RR.at[(s - 1) * 4 + i]
        return rcopy(
            src, RR.at[s * 4 + i], ring_s + s * 4 + i, ring_r + s * 4 + i,
            {"z": lax.rem(z + NZ + 1 - 2 * h, NZ)},
        )

    def own_step(s, h, j):
        i = h * 2 + j
        a = unit(s, h, j, c)
        ps_copy(s * 4 + i).wait_recv()
        a = a + RC[s * 4 + i].astype(F32)
        if s:
            ring_copy(s - 1, h, j).wait_recv()
            a = a + RR[(s - 1) * 4 + i].astype(F32)
        return a

    def own(s):
        def step(q, carry):
            j, h = q // 2, lax.rem(q, 2)
            i = h * 2 + j
            a = own_step(s, h, j).astype(BF16)
            if s == 0:
                R0[i] = a
            else:
                RR[(s - 1) * 4 + i] = a
            ring_copy(s, h, j).start()
            return carry

        lax.fori_loop(0, 4, step, 0)

    for_core(0)
    for_core(1)
    own(0)
    for_core(2)
    own(1)
    for_core(3)
    own(2)

    xr = take("r", 6)
    ag = take("r", 6)
    cc = take("r", 4 + 12)

    def hg_cols(zz, core, h):
        return pl.ds(al(((NC * core + h) * NY + zz) * DB, DB), DB)

    def spread(src, zz, j, sem):
        for h in range(2):
            piece = src.at[:, pl.ds(h * CW, CW)]
            dst = hg.at[pl.ds(j * HT, HT), hg_cols(zz, c, h)]
            send(piece, dst, sem + h, other)
            load(piece, dst, outs)

    for j in range(2):
        for h in range(2):
            XS[j, :, :, h * CW : (h + 1) * CW] = own_step(3, h, j).astype(BF16).reshape(NX, HT, CW)
        for r in (2, 1, 3):
            send(XS.at[j, xn(r)], XR.at[j, r - 1], xr + j * 3 + r - 1, {"x": xn(r)})
        total = XS[j, x].astype(F32)
        for r in (1, 3, 2):
            got(XR.at[j, r - 1], xr + j * 3 + r - 1)
            total = total + XR[j, r - 1].astype(F32)
        FO[j] = total.astype(BF16)
        for r in (2, 1, 3):
            send(FO.at[j], AG.at[r - 1, j], ag + j * 3 + r - 1, {"z": zn(r)})
        spread(FO.at[j], z, j, cc + j * 2)
    for j in range(2):
        for r in (1, 3, 2):
            got(AG.at[r - 1, j], ag + j * 3 + r - 1)
            spread(AG.at[r - 1, j], lax.rem(z + NZ - r, NZ), j, cc + 4 + (j * 3 + r - 1) * 2)

    for r in (1, 3, 2):
        got(JL.at[lax.rem(y + NY - r, NY)], jn + r - 1)
    sums = jnp.sum(JL[0] + JL[1] + JL[2] + JL[3], axis=1, keepdims=True)
    jl[...] = jnp.broadcast_to(sums / counts, (8, 128))

    for k in range(NK):
        for r in ORDER:
            cols = al(lax.rem(x + NX - r, NX) * U + k * CW, CW)
            got(lg.at[:, pl.ds(cols, CW)], lgs + k * 3 + r - 1)
    for r in ORDER:
        got(gr.at[:, pl.ds(al(lax.rem(x + NX - r, NX) * U, U), U)], grs + r - 1)
    for j in range(2):
        for h in range(2):
            rows = pl.ds(j * HT, HT)
            got(hg.at[rows, hg_cols(z, 1 - c, h)], cc + j * 2 + h)
            for r in (1, 3, 2):
                zz = lax.rem(z + NZ - r, NZ)
                got(hg.at[rows, hg_cols(zz, 1 - c, h)], cc + 4 + (j * 3 + r - 1) * 2 + h)

    def core_sent(i, carry):
        ps_copy(i).wait_send()
        return carry

    lax.fori_loop(0, 16, core_sent, 0)
    for s in range(3):
        for h in range(2):
            for j in range(2):
                ring_copy(s, h, j).wait_send()
    drain_sends(pending)
    drain(outs)
    assert used["s"] <= NSEND and used["r"] <= NRECV and used["l"] <= NLOAD, used


NSEND, NRECV, NLOAD = 192, 176, 88


def vmem(*shape, dtype=BF16):
    return pltpu.VMEM(shape, dtype)


def shards(hidden, weight, down, up, labels, jobs):
    pad = 3 * 128 - T
    lab = jnp.pad(labels.astype(F32), (0, pad)).reshape(3, 1, 128)
    job = jnp.pad(jobs.astype(F32), (0, pad), constant_values=-1.0).reshape(3, 1, 128)
    aux = jnp.concatenate([lab, job, jnp.zeros((3, 6, 128), F32)], axis=1)
    hbm = pl.BlockSpec(memory_space=pl.ANY)
    vm = pl.BlockSpec(memory_space=pltpu.VMEM)
    logits, rows, grad, loss, job_loss = pl.pallas_call(
        kernel,
        out_shape=(
            jax.ShapeDtypeStruct((T, V), BF16),
            jax.ShapeDtypeStruct((T, V), BF16),
            jax.ShapeDtypeStruct((T, D), BF16),
            jax.ShapeDtypeStruct((T, 128), F32),
            jax.ShapeDtypeStruct((8, 128), F32),
        ),
        in_specs=[hbm] * 5,
        out_specs=(hbm, hbm, hbm, vm, vm),
        scratch_shapes=[
            vmem(S, D),
            vmem(D, U + 256),
            vmem(DB, V),
            vmem(NK, S, CW, dtype=F32),
            vmem(S, U),
            vmem(NX, T, U + 256),
            vmem(16, S // 2, CW),
            vmem(12, S // 2, CW),
            vmem(4, S // 2, CW),
            vmem(2, NX, HT, SH),
            vmem(2, 3, HT, SH),
            vmem(2, HT, SH),
            vmem(3, 2, HT, SH),
            vmem(S, 128, dtype=F32),
            vmem(S, 128, dtype=F32),
            vmem(S, 128),
            vmem(128, U),
            vmem(NX, 3, 8, 128, dtype=F32),
            vmem(NZ * NC, NB, 8, 128, dtype=F32),
            vmem(NX, NB, 8, 128, dtype=F32),
            vmem(NB, 8, 128, dtype=F32),
            vmem(NY, 8, 128, dtype=F32),
            vmem(NY, 8, 128, dtype=F32),
            pltpu.SemaphoreType.DMA((NSEND,)),
            pltpu.SemaphoreType.DMA((NRECV,)),
            pltpu.SemaphoreType.DMA((NLOAD,)),
        ],
        compiler_params=pltpu.CompilerParams(
            collective_id=0, has_side_effects=True, vmem_limit_bytes=66 * 1024 * 1024 - 4 * 1024 * 1024
        ),
        name="step",
    )(hidden, weight, down, up, aux)
    return logits, rows, grad, loss[:, 3], job_loss[:, 0]


def solution(mesh):
    split = Mesh(mesh.devices.reshape(NZ, NC, NX, NY), ("z", "c", "x", "y"))
    dp, vocab = ("x", "y"), ("z", "c")
    return jax.shard_map(
        shards,
        mesh=split,
        in_specs=(P(dp, None), P(dp, vocab), P(), P(None, vocab), P(dp), P(dp)),
        out_specs=(P(dp, vocab), P(dp, vocab), P(dp, None), P(dp), P()),
        check_vma=False,
    )
```

```python
import functools

import jax
import jax.numpy as jnp
from jax import lax
from jax.experimental import pallas as pl
from jax.experimental.pallas import tpu as pltpu
from jax.sharding import Mesh
from jax.sharding import PartitionSpec as P

MESH = pl.DeviceIdType.MESH
F32 = jnp.float32
BF16 = jnp.bfloat16

JOBS = 8
RANK = 16
NX = NY = NZ = 4
NC = 2
T = 352
S = NX * T
HT = T // 2
D = 4096
DB = D // (NX * NY)
V = 4096
U = V // NX
CW = 256
NK = U // CW
SH = D // (NZ * NC)
TOKENS = S * NY
NB = S // 128


def fdot(a, b):
    return jnp.dot(a, b, preferred_element_type=F32)


def tdot(a, b):
    return lax.dot_general(a, b, (((1,), (1,)), ((), ())), preferred_element_type=F32)


def kernel(
    hid, w, ad, au, aux,
    lg, gr, hg, tl, jl,
    H, W5, WS, E, LT, G5, RR, R0, XS, XR, FO, AG, COL, COL2, LI, AU, AX, STA, STB, JR, CN, JL,
    ssem, rsem, lsem,
):
    z, c, x, y = (lax.axis_index(a) for a in ("z", "c", "x", "y"))
    v = z * NC + c

    def al(i, m):
        return pl.multiple_of(i, m)

    def xn(r):
        return lax.rem(x + r, NX)

    def yn(r):
        return lax.rem(y + r, NY)

    def zn(r):
        return lax.rem(z + r, NZ)

    used = {"s": 0, "r": 0, "l": 0}

    def take(kind, n=1):
        at = used[kind]
        used[kind] = at + n
        return at

    pending = []

    def rcopy(src, dst, si, ri, dev):
        return pltpu.make_async_remote_copy(
            src_ref=src, dst_ref=dst, send_sem=ssem.at[si], recv_sem=rsem.at[ri],
            device_id=dev, device_id_type=MESH,
        )

    def send(src, dst, ri, dev, keep=pending):
        d = rcopy(src, dst, take("s"), ri, dev)
        d.start()
        keep.append(d)

    def got(dst, ri):
        rcopy(dst, dst, 0, ri, {"x": xn(1)}).wait_recv()

    def load(src, dst, keep):
        d = pltpu.make_async_copy(src, dst, lsem.at[take("l")])
        d.start()
        keep.append(d)

    def drain(keep):
        for d in keep:
            d.wait()
        keep.clear()

    def drain_sends(keep):
        for d in keep:
            d.wait_send()
        keep.clear()

    scope = []

    def phase(name):
        if scope:
            scope.pop().__exit__(None, None, None)
        if name:
            scope.append(jax.named_scope(name))
            scope[0].__enter__()

    phase("entry")
    bar = pltpu.get_barrier_semaphore()
    peers = (
        [{"x": xn(r)} for r in (1, 2, 3)]
        + [{"y": yn(r)} for r in (1, 2, 3)]
        + [{"z": zn(a), "c": lax.rem(c + b, NC)} for a in range(NZ) for b in range(NC) if a or b]
    )
    for dev in peers:
        pl.semaphore_signal(bar, inc=1, device_id=dev, device_id_type=MESH)

    first, own_h, rest = [], [], []
    load(w, WS, first)
    for p in range(NX * NY):
        n = (p % NX) * NY + p // NX
        load(hid.at[:, pl.ds(n * DB, DB)], H.at[pl.ds(al(x * T, 16), T), pl.ds(p * DB, DB)], own_h)
    load(aux, AX.at[x], first)
    own_rows = pl.ds(al((y * NX + x) * DB, DB), DB)
    load(w.at[:, pl.ds(al(x * U, U), U)], W5.at[own_rows, pl.ds(0, U)], first)
    load(au.at[:, pl.ds(al(x * U, U), U)], AU, rest)
    for p in range(NX * NY):
        n = (p % NX) * NY + p // NX
        for q in range(2):
            load(
                ad.at[pl.ds(n * DB, DB), :],
                W5.at[pl.ds(p * DB, DB), pl.ds(U + q * 128, 128)],
                rest,
            )
    pl.semaphore_wait(bar, len(peers))

    ORDER = (1, 3, 2)
    wx = take("r", NK * 3)
    hx = take("r", 3)
    ax = take("r", 3)
    wy = take("r", NK * NX * 3)
    hz = take("r", 3 * 4)
    hc = take("r", 3 * 5)
    lgs = take("r", NK * 3)
    lgs_s = take("s", NK * 3)
    lgs_l = take("l", NK)

    def xp(r):
        return lax.rem(x + NX - r, NX)

    def wblock(row, k):
        return W5.at[row, pl.ds(k * CW, CW)]

    def send_w(k):
        for r in ORDER:
            send(
                WS.at[:, pl.ds(al(xn(r) * U + k * CW, CW), CW)],
                wblock(own_rows, k), wx + k * 3 + r - 1, {"x": xn(r)},
            )

    def piece(dy, r, k):
        return wblock(pl.ds(al((yn(dy) * NX + xp(r)) * DB, DB), DB), k)

    def y_own(k, r):
        src = piece(0, r, k)
        if r:
            got(src, wx + k * 3 + r - 1)
        at = wy + (k * NX + r) * 3
        send(src, src, at, {"y": yn(1)})
        send(src, src, at + 1, {"y": yn(3)})

    def y_fwd(k, r):
        at = wy + (k * NX + r) * 3
        if r in (0, 2):
            src = piece(3, r, k)
            got(src, at)
            send(src, src, at + 2, {"y": yn(1)})
        else:
            src = piece(1, r, k)
            got(src, at + 1)
            send(src, src, at + 2, {"y": yn(3)})

    def w_end(k):
        for r in (0, 1, 3, 2):
            at = wy + (k * NX + r) * 3
            if r in (0, 2):
                got(piece(1, r, k), at + 1)
            else:
                got(piece(3, r, k), at)
            got(piece(2, r, k), at + 2)

    hsends = []
    other = {"c": 1 - c}

    def hpiece(xb, share, lo=0, n=T):
        return H.at[pl.ds(al(xb * T + lo, 16), n), pl.ds(al(share * SH, SH), SH)]

    def h_in(r):
        mine = hpiece(xp(r), v)
        got(mine, hx + r - 1)
        b = hz + (r - 1) * 4
        send(mine, mine, b + 0, {"z": zn(1)}, hsends)
        send(mine, mine, b + 1, {"z": zn(3)}, hsends)
        send(mine, mine, hc + (r - 1) * 5, other, hsends)

    def h_fwd(r):
        xb = xp(r)
        b, d = hz + (r - 1) * 4, hc + (r - 1) * 5
        left, right = zn(3) * NC + c, zn(1) * NC + c
        got(hpiece(xb, left), b + 0)
        send(hpiece(xb, left, 0, HT), hpiece(xb, left, 0, HT), b + 2, {"z": zn(1)}, hsends)
        send(hpiece(xb, left), hpiece(xb, left), d + 1, other, hsends)
        got(hpiece(xb, right), b + 1)
        send(hpiece(xb, right, HT, HT), hpiece(xb, right, HT, HT), b + 3, {"z": zn(3)}, hsends)
        send(hpiece(xb, right), hpiece(xb, right), d + 2, other, hsends)

    def h_last(r):
        xb = xp(r)
        b, d = hz + (r - 1) * 4, hc + (r - 1) * 5
        far = zn(2) * NC + c
        got(hpiece(xb, far, 0, HT), b + 2)
        send(hpiece(xb, far, 0, HT), hpiece(xb, far, 0, HT), d + 3, other, hsends)
        got(hpiece(xb, far, HT, HT), b + 3)
        send(hpiece(xb, far, HT, HT), hpiece(xb, far, HT, HT), d + 4, other, hsends)

    def h_end(r):
        xb = xp(r)
        d = hc + (r - 1) * 5
        k = 1 - c
        got(hpiece(xb, v - c + k), d)
        got(hpiece(xb, zn(3) * NC + k), d + 1)
        got(hpiece(xb, zn(1) * NC + k), d + 2)
        got(hpiece(xb, zn(2) * NC + k, 0, HT), d + 3)
        got(hpiece(xb, zn(2) * NC + k, HT, HT), d + 4)

    lane128 = lax.broadcasted_iota(jnp.int32, (T, 128), 1)
    rank_job = (lane128 // RANK).astype(F32)
    base = v * V + x * U
    lane_cw = lax.broadcasted_iota(jnp.int32, (T, CW), 1)
    outs = []
    my_cols = al(x * U, U)

    def lora_in(r):
        rows = pl.ds(al(xp(r) * T, 16), T)
        hit = COL[rows, 1:2] == rank_job
        a = fdot(H[rows, :], W5[:, U : U + 128])
        LI[rows, :] = jnp.where(hit, a, 0.0).astype(BF16)

    def lg_cols(k):
        return pl.ds(al(my_cols + k * CW, CW), CW)

    def lg_remote(k, r):
        i = k * 3 + NX - 1 - r
        src = LT.at[pl.ds(al(xp(r) * T, 16), T), pl.ds(al(k * CW, CW), CW)]
        return rcopy(src, lg.at[:, lg_cols(k)], lgs_s + i, lgs + i, {"x": xp(r)})

    def lg_local(k):
        src = LT.at[pl.ds(al(x * T, 16), T), pl.ds(al(k * CW, CW), CW)]
        return pltpu.make_async_copy(src, lg.at[:, lg_cols(k)], lsem.at[lgs_l + k])

    def task(k, r):
        rows = pl.ds(al(xp(r) * T, 16), T)
        cols = pl.ds(al(k * CW, CW), CW)
        a = fdot(H[rows, :], W5[:, cols])
        a = a + fdot(LI[rows, :], AU[:, cols])
        LT[rows, cols] = a.astype(BF16)
        top = jnp.max(a, axis=1, keepdims=True)
        e = jnp.exp(a - top)
        E[k, rows, :] = e
        total = jnp.sum(e, axis=1, keepdims=True)
        ids = (lane_cw + (base + k * CW)).astype(F32)
        target = jnp.sum(jnp.where(ids == COL[rows, 0:1], a, 0.0), axis=1, keepdims=True)
        old = COL[rows, :]
        old = jnp.where(lane128 == 8 + k, top, old)
        old = jnp.where(lane128 == 12 + k, total, old)
        COL[rows, :] = jnp.where(lane128 == 16 + k, target, old)

    def tasks(k0, nk, o0, no):
        def step(i, carry):
            k, o = k0 + i // no, o0 + lax.rem(i, no)
            r = jnp.where(o == 2, 3, jnp.where(o == 3, 2, o))
            task(k, r)
            if o0:
                lg_remote(k, r).start()
            else:
                pl.when(r > 0)(lambda: lg_remote(k, r).start())
                pl.when(r == 0)(lambda: lg_local(k).start())
            return carry

        lax.fori_loop(0, nk * no, step, 0)

    drain(first)
    send_w(0)
    for r in ORDER:
        send(AX.at[x], AX.at[x], ax + r - 1, {"x": xn(r)})
    send_w(1)
    for k in range(3):
        y_own(k, 0)
    drain(own_h)
    for r in ORDER:
        send(hpiece(x, v), hpiece(x, v), hx + r - 1, {"x": xn(r)}, hsends)
    send_w(2)
    send_w(3)
    phase("p1a")
    y_fwd(0, 0)
    for r in ORDER:
        y_own(0, r)
    phase("p1b")
    for r in ORDER:
        y_own(1, r)
    phase("p1c")
    y_fwd(0, 1)
    y_fwd(0, 3)
    phase("h_in13")
    h_in(1)
    h_in(3)
    phase("p1d")
    y_fwd(0, 2)
    y_own(3, 0)
    y_fwd(1, 0)
    y_fwd(1, 1)
    phase("h_in2")
    h_in(2)
    phase("p1e")
    y_fwd(1, 3)
    y_fwd(1, 2)
    phase("cols")

    for r in ORDER:
        got(AX.at[xp(r)], ax + r - 1)
    sub = lax.broadcasted_iota(jnp.int32, (8, 128), 0).astype(F32)
    subi = lax.broadcasted_iota(jnp.int32, (8, 128), 0)
    counts = jnp.zeros((8, 128), F32)
    for xb in range(NX):
        for q in range(3):
            tile = AX[xb, q]
            n = min(128, T - q * 128)
            turned = jnp.concatenate([tile, jnp.zeros((120, 128), F32)], axis=0).T
            COL[pl.ds(xb * T + q * 128, n), :] = turned[:n]
            counts = counts + (tile[1:2, :] == sub).astype(F32)
    CN[y] = counts
    cn = take("r", 3)
    for r in (1, 3, 2):
        send(CN.at[y], CN.at[y], cn + r - 1, {"y": yn(r)})
    drain(rest)
    lora_in(0)
    phase("h_fwd1")
    h_fwd(1)
    phase("w_end0")
    w_end(0)
    phase("t0_0")
    tasks(0, 1, 0, 1)
    phase("y_own2")
    for r in ORDER:
        y_own(2, r)
    phase("w_end1")
    w_end(1)
    phase("t1_0")
    tasks(1, 1, 0, 1)
    phase("h_fwd3")
    h_fwd(3)
    phase("y_own3")
    for r in ORDER:
        y_own(3, r)
    phase("h_last1")
    h_last(1)
    phase("y_fwd2")
    y_fwd(2, 0)
    y_fwd(2, 1)
    phase("h_fwd2")
    h_fwd(2)
    phase("h_end1")
    h_end(1)
    phase("t01_1")
    lora_in(1)
    tasks(0, 2, 1, 1)
    phase("y_fwd2b")
    y_fwd(2, 3)
    y_fwd(2, 2)
    phase("h_last3")
    h_last(3)
    h_end(3)
    phase("t01_3")
    lora_in(3)
    tasks(0, 2, 2, 1)
    phase("y_fwd3")
    y_fwd(3, 0)
    y_fwd(3, 1)
    phase("w_end2")
    w_end(2)
    phase("t2")
    tasks(2, 1, 0, 3)
    phase("h_last2")
    h_last(2)
    h_end(2)
    phase("t012_2")
    lora_in(2)
    tasks(0, 3, 3, 1)
    phase("y_fwd3b")
    y_fwd(3, 3)
    y_fwd(3, 2)
    drain_sends(hsends)
    phase("w_end3")
    w_end(3)
    phase("t3")
    tasks(3, 1, 0, 4)
    phase("stats_a")

    def row_stats(b, carry):
        t = COL[pl.ds(al(b * 128, 128), 128), :].T
        m, s, g = t[8:12], t[12:16], t[16:20]
        top = jnp.max(m, axis=0, keepdims=True)
        s = jnp.sum(s * jnp.exp(m - top), axis=0, keepdims=True)
        g = jnp.sum(g, axis=0, keepdims=True)
        JR[b] = jnp.broadcast_to(t[1:2], (8, 128))
        STA[v, b] = jnp.where(subi == 0, top, jnp.where(subi == 1, s, jnp.where(subi == 2, g, 0.0)))
        return carry

    lax.fori_loop(0, NB, row_stats, 0, unroll=True)
    sa = take("r", 7)
    sb = take("r", 3)
    turns = [(a, b) for a in (2, 1, 3, 0) for b in range(NC) if a or b]
    for a, b in turns:
        dev = {"z": zn(a), "c": lax.rem(c + b, NC)}
        send(STA.at[v], STA.at[v], sa + a * NC + b - 1, dev)
    for a, b in turns:
        src = lax.rem(z + NZ - a, NZ) * NC + lax.rem(c + b, NC)
        got(STA.at[src], sa + a * NC + b - 1)

    def joined(parts):
        top = functools.reduce(jnp.maximum, [p[0:1] for p in parts])
        s = functools.reduce(jnp.add, [p[1:2] * jnp.exp(p[0:1] - top) for p in parts])
        g = functools.reduce(jnp.add, [p[2:3] for p in parts])
        return top, s, g

    def stage_b(b, carry):
        top, s, g = joined([STA[i, b] for i in range(NZ * NC)])
        STB[x, b] = jnp.where(subi == 0, top, jnp.where(subi == 1, s, jnp.where(subi == 2, g, 0.0)))
        return carry

    phase("stats_b")
    lax.fori_loop(0, NB, stage_b, 0, unroll=True)
    for r in (2, 1, 3):
        send(STB.at[x], STB.at[x], sb + r - 1, {"x": xn(r)})
    for r in (1, 3, 2):
        got(CN.at[lax.rem(y + NY - r, NY)], cn + r - 1)
    counts = jnp.sum(CN[0] + CN[1] + CN[2] + CN[3], axis=1, keepdims=True)
    counts = jnp.maximum(counts, 1.0)
    per_job = TOKENS / (JOBS * counts)
    for r in (2, 1, 3):
        got(STB.at[lax.rem(x + NX - r, NX)], sb + r - 1)

    def finish(b, job_sums):
        top, s, g = joined([STB[i, b] for i in range(NX)])
        onehot = (JR[b] == sub).astype(F32)
        loss = top + jnp.log(s) - g
        weight = jnp.sum(onehot * per_job, axis=0, keepdims=True)
        tile = jnp.where(
            subi == 0, top,
            jnp.where(subi == 1, weight / s, jnp.where(subi == 2, weight, jnp.where(subi == 3, loss, 0.0))),
        )
        turned = jnp.concatenate([tile, jnp.zeros((120, 128), F32)], axis=0).T
        COL2[pl.ds(al(b * 128, 128), 128), :] = turned
        return job_sums + onehot * loss

    phase("finish")
    JL[y] = lax.fori_loop(0, NB, finish, jnp.zeros((8, 128), F32), unroll=True)
    jn = take("r", 3)
    for r in (1, 3, 2):
        send(JL.at[y], JL.at[y], jn + r - 1, {"y": yn(r)})

    grs = take("r", 6)

    def gradient(j):
        def step(m, carry):
            half = pl.ds(j * HT, HT)
            rows = pl.ds(al(m * T + j * HT, 16), HT)
            lab = COL[rows, 0:1]
            weight = COL2[rows, 2:3]
            for k in range(NK):
                f = jnp.exp(COL[rows, 8 + k : 9 + k] - COL2[rows, 0:1]) * COL2[rows, 1:2]
                ids = (lane_cw[:HT] + (base + k * CW)).astype(F32)
                g = E[k, rows, :] * f - jnp.where(ids == lab, weight, 0.0)
                G5[m, half, k * CW : (k + 1) * CW] = g.astype(BF16)
            part = tdot(G5[m, half, 0:U], AU[...])
            part = jnp.where(COL[rows, 1:2] == rank_job[:HT], part, 0.0)
            high = part.astype(BF16)
            G5[m, half, U : U + 128] = high
            G5[m, half, U + 128 : U + 256] = (part - high.astype(F32)).astype(BF16)
            return carry

        lax.fori_loop(0, NX, step, 0)

    def send_rows(j):
        half = pl.ds(j * HT, HT)
        dst = gr.at[half, pl.ds(my_cols, U)]
        for r in ORDER:
            send(G5.at[xn(r), half, pl.ds(0, U)], dst, grs + j * 3 + r - 1, {"x": xn(r)})
        load(G5.at[x, half, pl.ds(0, U)], dst, outs)

    cs_s, cs_r = take("s", 16), take("r", 16)
    ring_s, ring_r = take("s", 12), take("r", 12)

    def zt(s, h):
        return lax.rem(z + NZ + (2 * h - 1) * (s + 1), NZ)

    def unit(s, h, j, core):
        at = al((zt(s, h) * NC + core) * SH + h * CW, CW)
        g = G5[:, pl.ds(al(j * HT, 16), HT), :].reshape(NX * HT, U + 256)
        return tdot(g, W5[pl.ds(at, CW), :])

    def ps(i):
        return H.at[pl.ds(al(lax.rem(i, 2) * (S // 2), 16), S // 2), pl.ds(al(i // 2 * CW, CW), CW)]

    def rc(i):
        cols = pl.ds(al(D // 2 + i // 2 * CW, CW), CW)
        return H.at[pl.ds(al(lax.rem(i, 2) * (S // 2), 16), S // 2), cols]

    def ps_copy(i):
        return rcopy(ps(i), rc(i), cs_s + i, cs_r + i, other)

    def for_core(s, j0=0, nj=2):
        def step(q, carry):
            j, h = j0 + q // 2, lax.rem(q, 2)
            i = s * 4 + h * 2 + j
            ps(i)[...] = unit(s, h, j, 1 - c).astype(BF16)
            ps_copy(i).start()
            return carry

        lax.fori_loop(0, 2 * nj, step, 0)

    def ring_copy(s, h, j):
        i = h * 2 + j
        src = R0.at[i] if s == 0 else RR.at[(s - 1) * 4 + i]
        return rcopy(
            src, RR.at[s * 4 + i], ring_s + s * 4 + i, ring_r + s * 4 + i,
            {"z": lax.rem(z + NZ + 1 - 2 * h, NZ)},
        )

    def own_step(s, h, j):
        i = h * 2 + j
        a = unit(s, h, j, c)
        ps_copy(s * 4 + i).wait_recv()
        a = a + rc(s * 4 + i)[...].astype(F32)
        if s:
            ring_copy(s - 1, h, j).wait_recv()
            a = a + RR[(s - 1) * 4 + i].astype(F32)
        return a

    def own(s, j0=0, nj=2):
        def step(q, carry):
            j, h = j0 + q // 2, lax.rem(q, 2)
            i = h * 2 + j
            a = own_step(s, h, j).astype(BF16)
            if s == 0:
                R0[i] = a
            else:
                RR[(s - 1) * 4 + i] = a
            ring_copy(s, h, j).start()
            return carry

        lax.fori_loop(0, 2 * nj, step, 0)

    phase("grad0")
    gradient(0)
    phase("core00")
    for_core(0, 0, 1)
    send_rows(0)
    tl[...] = COL2[pl.ds(al(x * T, 8), T), :]
    phase("own00")
    own(0, 0, 1)
    phase("grad1")
    gradient(1)
    phase("core01")
    for_core(0, 1, 1)
    send_rows(1)
    phase("own01")
    own(0, 1, 1)
    phase("core1")
    for_core(1)
    phase("own1")
    own(1)
    phase("core2")
    for_core(2)
    phase("own2")
    own(2)
    phase("core3")
    for_core(3)

    xr = take("r", 6)
    ag = take("r", 6)
    cc = take("r", 4 + 12)

    def hg_cols(zz, core, h):
        return pl.ds(al(((NC * core + h) * NY + zz) * DB, DB), DB)

    def spread(src, zz, j, sem):
        for h in range(2):
            piece = src.at[:, pl.ds(h * CW, CW)]
            dst = hg.at[pl.ds(j * HT, HT), hg_cols(zz, c, h)]
            send(piece, dst, sem + h, other)
            load(piece, dst, outs)

    for j in range(2):
        phase("own3")
        for h in range(2):
            XS[j, :, :, h * CW : (h + 1) * CW] = own_step(3, h, j).astype(BF16).reshape(NX, HT, CW)
        phase("xsum")
        for r in (2, 1, 3):
            send(XS.at[j, xn(r)], XR.at[j, r - 1], xr + j * 3 + r - 1, {"x": xn(r)})
        total = XS[j, x].astype(F32)
        for r in (1, 3, 2):
            got(XR.at[j, r - 1], xr + j * 3 + r - 1)
            total = total + XR[j, r - 1].astype(F32)
        FO[j] = total.astype(BF16)
        phase("spread")
        for r in (2, 1, 3):
            send(FO.at[j], AG.at[r - 1, j], ag + j * 3 + r - 1, {"z": zn(r)})
        spread(FO.at[j], z, j, cc + j * 2)
    phase("gathered")
    for j in range(2):
        for r in (1, 3, 2):
            got(AG.at[r - 1, j], ag + j * 3 + r - 1)
            spread(AG.at[r - 1, j], lax.rem(z + NZ - r, NZ), j, cc + 4 + (j * 3 + r - 1) * 2)

    for r in (1, 3, 2):
        got(JL.at[lax.rem(y + NY - r, NY)], jn + r - 1)
    sums = jnp.sum(JL[0] + JL[1] + JL[2] + JL[3], axis=1, keepdims=True)
    jl[...] = jnp.broadcast_to(sums / counts, (8, 128))

    phase("arrivals")
    for k in range(NK):
        for r in ORDER:
            cols = al(xp(r) * U + k * CW, CW)
            got(lg.at[:, pl.ds(cols, CW)], lgs + k * 3 + r - 1)
            lg_remote(k, r).wait_send()
        lg_local(k).wait()
    for j in range(2):
        for r in ORDER:
            cols = pl.ds(al(xp(r) * U, U), U)
            got(gr.at[pl.ds(j * HT, HT), cols], grs + j * 3 + r - 1)
    for j in range(2):
        for h in range(2):
            rows = pl.ds(j * HT, HT)
            got(hg.at[rows, hg_cols(z, 1 - c, h)], cc + j * 2 + h)
            for r in (1, 3, 2):
                zz = lax.rem(z + NZ - r, NZ)
                got(hg.at[rows, hg_cols(zz, 1 - c, h)], cc + 4 + (j * 3 + r - 1) * 2 + h)

    def core_sent(i, carry):
        ps_copy(i).wait_send()
        return carry

    lax.fori_loop(0, 16, core_sent, 0)
    for s in range(3):
        for h in range(2):
            for j in range(2):
                ring_copy(s, h, j).wait_send()
    phase("drain")
    drain_sends(pending)
    drain(outs)
    phase(None)
    assert used["s"] <= NSEND and used["r"] <= NRECV and used["l"] <= NLOAD, used


NSEND, NRECV, NLOAD = 224, 208, 88


def vmem(*shape, dtype=BF16):
    return pltpu.VMEM(shape, dtype)


def shards(hidden, weight, down, up, labels, jobs):
    pad = 3 * 128 - T
    lab = jnp.pad(labels.astype(F32), (0, pad)).reshape(3, 1, 128)
    job = jnp.pad(jobs.astype(F32), (0, pad), constant_values=-1.0).reshape(3, 1, 128)
    aux = jnp.concatenate([lab, job, jnp.zeros((3, 6, 128), F32)], axis=1)
    hbm = pl.BlockSpec(memory_space=pl.ANY)
    vm = pl.BlockSpec(memory_space=pltpu.VMEM)
    logits, rows, grad, loss, job_loss = pl.pallas_call(
        kernel,
        out_shape=(
            jax.ShapeDtypeStruct((T, V), BF16),
            jax.ShapeDtypeStruct((T, V), BF16),
            jax.ShapeDtypeStruct((T, D), BF16),
            jax.ShapeDtypeStruct((T, 128), F32),
            jax.ShapeDtypeStruct((8, 128), F32),
        ),
        in_specs=[hbm] * 5,
        out_specs=(hbm, hbm, hbm, vm, vm),
        scratch_shapes=[
            vmem(S, D),
            vmem(D, U + 256),
            vmem(DB, V),
            vmem(NK, S, CW, dtype=F32),
            vmem(S, U),
            vmem(NX, T, U + 256),
            vmem(12, S // 2, CW),
            vmem(4, S // 2, CW),
            vmem(2, NX, HT, SH),
            vmem(2, 3, HT, SH),
            vmem(2, HT, SH),
            vmem(3, 2, HT, SH),
            vmem(S, 128, dtype=F32),
            vmem(S, 128, dtype=F32),
            vmem(S, 128),
            vmem(128, U),
            vmem(NX, 3, 8, 128, dtype=F32),
            vmem(NZ * NC, NB, 8, 128, dtype=F32),
            vmem(NX, NB, 8, 128, dtype=F32),
            vmem(NB, 8, 128, dtype=F32),
            vmem(NY, 8, 128, dtype=F32),
            vmem(NY, 8, 128, dtype=F32),
            pltpu.SemaphoreType.DMA((NSEND,)),
            pltpu.SemaphoreType.DMA((NRECV,)),
            pltpu.SemaphoreType.DMA((NLOAD,)),
        ],
        compiler_params=pltpu.CompilerParams(
            collective_id=0, has_side_effects=True, vmem_limit_bytes=56 * 1024 * 1024
        ),
        name="step",
    )(hidden, weight, down, up, aux)
    return logits, rows, grad, loss[:, 3], job_loss[:, 0]


def solution(mesh):
    split = Mesh(mesh.devices.reshape(NZ, NC, NX, NY), ("z", "c", "x", "y"))
    dp, vocab = ("x", "y"), ("z", "c")
    return jax.shard_map(
        shards,
        mesh=split,
        in_specs=(P(dp, None), P(dp, vocab), P(), P(None, vocab), P(dp), P(dp)),
        out_specs=(P(dp, vocab), P(dp, vocab), P(dp, None), P(dp), P()),
        check_vma=False,
    )
```

```python
import functools

import jax
import jax.numpy as jnp
from jax import lax
from jax.experimental import pallas as pl
from jax.experimental.pallas import tpu as pltpu
from jax.sharding import Mesh
from jax.sharding import PartitionSpec as P

MESH = pl.DeviceIdType.MESH
F32 = jnp.float32
BF16 = jnp.bfloat16

JOBS = 8
RANK = 16
NX = NY = NZ = 4
NC = 2
T = 352
S = NX * T
HT = T // 2
LEN = (96, 96, 80, 80)
OFF = (0, 96, 192, 272)
NQ = len(LEN)
D = 4096
DB = D // (NX * NY)
V = 4096
U = V // NX
CW = 256
NK = U // CW
SH = D // (NZ * NC)
TOKENS = S * NY
NB = S // 128


def fdot(a, b):
    return jnp.dot(a, b, preferred_element_type=F32)


def tdot(a, b):
    return lax.dot_general(a, b, (((1,), (1,)), ((), ())), preferred_element_type=F32)


def kernel(
    hid, w, ad, au, ids_in,
    lg, gr, hg, small,
    H, W5, WS, E, LT, G5, RR, XS, XR, FO, AG, COL, COL2, LI, AU, AX, STA, STB, JR, CN, JL,
    ssem, rsem, lsem,
):
    z, c, x, y = (lax.axis_index(a) for a in ("z", "c", "x", "y"))
    v = z * NC + c

    def al(i, m):
        return pl.multiple_of(i, m)

    def xn(r):
        return lax.rem(x + r, NX)

    def yn(r):
        return lax.rem(y + r, NY)

    def zn(r):
        return lax.rem(z + r, NZ)

    used = {"s": 0, "r": 0, "l": 0}

    def take(kind, n=1):
        at = used[kind]
        used[kind] = at + n
        return at

    pending = []

    def rcopy(src, dst, si, ri, dev):
        return pltpu.make_async_remote_copy(
            src_ref=src, dst_ref=dst, send_sem=ssem.at[si], recv_sem=rsem.at[ri],
            device_id=dev, device_id_type=MESH,
        )

    def send(src, dst, ri, dev, keep=pending):
        d = rcopy(src, dst, take("s"), ri, dev)
        d.start()
        keep.append(d)

    def got(dst, ri):
        rcopy(dst, dst, 0, ri, {"x": xn(1)}).wait_recv()

    def load(src, dst, keep):
        d = pltpu.make_async_copy(src, dst, lsem.at[take("l")])
        d.start()
        keep.append(d)

    def drain(keep):
        for d in keep:
            d.wait()
        keep.clear()

    def drain_sends(keep):
        for d in keep:
            d.wait_send()
        keep.clear()

    scope = []

    def phase(name):
        if scope:
            scope.pop().__exit__(None, None, None)
        if name:
            scope.append(jax.named_scope(name))
            scope[0].__enter__()

    phase("entry")
    bar = pltpu.get_barrier_semaphore()
    peers = (
        [{"x": xn(r)} for r in (1, 2, 3)]
        + [{"y": yn(r)} for r in (1, 2, 3)]
        + [{"z": zn(a), "c": lax.rem(c + b, NC)} for a in range(NZ) for b in range(NC) if a or b]
    )
    for dev in peers:
        pl.semaphore_signal(bar, inc=1, device_id=dev, device_id_type=MESH)

    first, own_h, rest = [], [], []
    load(w, WS, first)
    for p in range(NX * NY):
        n = (p % NX) * NY + p // NX
        load(hid.at[:, pl.ds(n * DB, DB)], H.at[pl.ds(al(x * T, 16), T), pl.ds(p * DB, DB)], own_h)
    for q in range(3):
        n = min(128, T - q * 128)
        AX[x, q] = jnp.full((8, 128), -1.0, F32)
        AX[x, q, 0:2, 0:n] = ids_in[:, q * 128 : q * 128 + n].astype(F32)
    own_rows = pl.ds(al((y * NX + x) * DB, DB), DB)
    load(w.at[:, pl.ds(al(x * U, U), U)], W5.at[own_rows, pl.ds(0, U)], first)
    load(au.at[:, pl.ds(al(x * U, U), U)], AU, rest)
    for p in range(NX * NY):
        n = (p % NX) * NY + p // NX
        for q in range(2):
            load(
                ad.at[pl.ds(n * DB, DB), :],
                W5.at[pl.ds(p * DB, DB), pl.ds(U + q * 128, 128)],
                rest,
            )
    pl.semaphore_wait(bar, len(peers))

    ORDER = (1, 3, 2)
    wx = take("r", NK * 3)
    hx = take("r", 3)
    ax = take("r", 3)
    wy = take("r", NK * NX * 3)
    hz = take("r", 3 * 4)
    hc = take("r", 3 * 5)
    lgs = take("r", NK * 3)
    lgs_s = take("s", NK * 3)
    lgs_l = take("l", NK)

    def xp(r):
        return lax.rem(x + NX - r, NX)

    def wblock(row, k):
        return W5.at[row, pl.ds(k * CW, CW)]

    def send_w(k):
        for r in ORDER:
            send(
                WS.at[:, pl.ds(al(xn(r) * U + k * CW, CW), CW)],
                wblock(own_rows, k), wx + k * 3 + r - 1, {"x": xn(r)},
            )

    def piece(dy, r, k):
        return wblock(pl.ds(al((yn(dy) * NX + xp(r)) * DB, DB), DB), k)

    def y_own(k, r):
        src = piece(0, r, k)
        if r:
            got(src, wx + k * 3 + r - 1)
        at = wy + (k * NX + r) * 3
        send(src, src, at, {"y": yn(1)})
        send(src, src, at + 1, {"y": yn(3)})

    def y_fwd(k, r):
        at = wy + (k * NX + r) * 3
        if r in (0, 2):
            src = piece(3, r, k)
            got(src, at)
            send(src, src, at + 2, {"y": yn(1)})
        else:
            src = piece(1, r, k)
            got(src, at + 1)
            send(src, src, at + 2, {"y": yn(3)})

    def w_end(k):
        for r in (0, 1, 3, 2):
            at = wy + (k * NX + r) * 3
            if r in (0, 2):
                got(piece(1, r, k), at + 1)
            else:
                got(piece(3, r, k), at)
            got(piece(2, r, k), at + 2)

    hsends = []
    other = {"c": 1 - c}

    def hpiece(xb, share, lo=0, n=T):
        return H.at[pl.ds(al(xb * T + lo, 16), n), pl.ds(al(share * SH, SH), SH)]

    def h_in(r):
        mine = hpiece(xp(r), v)
        got(mine, hx + r - 1)
        b = hz + (r - 1) * 4
        send(mine, mine, b + 0, {"z": zn(1)}, hsends)
        send(mine, mine, b + 1, {"z": zn(3)}, hsends)
        send(mine, mine, hc + (r - 1) * 5, other, hsends)

    def h_fwd(r):
        xb = xp(r)
        b, d = hz + (r - 1) * 4, hc + (r - 1) * 5
        left, right = zn(3) * NC + c, zn(1) * NC + c
        got(hpiece(xb, left), b + 0)
        send(hpiece(xb, left, 0, HT), hpiece(xb, left, 0, HT), b + 2, {"z": zn(1)}, hsends)
        send(hpiece(xb, left), hpiece(xb, left), d + 1, other, hsends)
        got(hpiece(xb, right), b + 1)
        send(hpiece(xb, right, HT, HT), hpiece(xb, right, HT, HT), b + 3, {"z": zn(3)}, hsends)
        send(hpiece(xb, right), hpiece(xb, right), d + 2, other, hsends)

    def h_last(r):
        xb = xp(r)
        b, d = hz + (r - 1) * 4, hc + (r - 1) * 5
        far = zn(2) * NC + c
        got(hpiece(xb, far, 0, HT), b + 2)
        send(hpiece(xb, far, 0, HT), hpiece(xb, far, 0, HT), d + 3, other, hsends)
        got(hpiece(xb, far, HT, HT), b + 3)
        send(hpiece(xb, far, HT, HT), hpiece(xb, far, HT, HT), d + 4, other, hsends)

    def h_end(r):
        xb = xp(r)
        d = hc + (r - 1) * 5
        k = 1 - c
        got(hpiece(xb, v - c + k), d)
        got(hpiece(xb, zn(3) * NC + k), d + 1)
        got(hpiece(xb, zn(1) * NC + k), d + 2)
        got(hpiece(xb, zn(2) * NC + k, 0, HT), d + 3)
        got(hpiece(xb, zn(2) * NC + k, HT, HT), d + 4)

    lane128 = lax.broadcasted_iota(jnp.int32, (T, 128), 1)
    rank_job = (lane128 // RANK).astype(F32)
    base = v * V + x * U
    lane_cw = lax.broadcasted_iota(jnp.int32, (T, CW), 1)
    outs = []
    my_cols = al(x * U, U)

    def lora_in(r):
        rows = pl.ds(al(xp(r) * T, 16), T)
        hit = COL[rows, 1:2] == rank_job
        a = fdot(H[rows, :], W5[:, U : U + 128])
        LI[rows, :] = jnp.where(hit, a, 0.0).astype(BF16)

    def lg_cols(k):
        return pl.ds(al(my_cols + k * CW, CW), CW)

    def lg_remote(k, r):
        i = k * 3 + NX - 1 - r
        src = LT.at[pl.ds(al(xp(r) * T, 16), T), pl.ds(al(k * CW, CW), CW)]
        return rcopy(src, lg.at[:, lg_cols(k)], lgs_s + i, lgs + i, {"x": xp(r)})

    def lg_local(k):
        src = LT.at[pl.ds(al(x * T, 16), T), pl.ds(al(k * CW, CW), CW)]
        return pltpu.make_async_copy(src, lg.at[:, lg_cols(k)], lsem.at[lgs_l + k])

    def task(k, r):
        rows = pl.ds(al(xp(r) * T, 16), T)
        cols = pl.ds(al(k * CW, CW), CW)
        a = fdot(H[rows, :], W5[:, cols])
        a = a + fdot(LI[rows, :], AU[:, cols])
        LT[rows, cols] = a.astype(BF16)
        top = jnp.max(a, axis=1, keepdims=True)
        e = jnp.exp(a - top)
        E[k, rows, :] = e
        total = jnp.sum(e, axis=1, keepdims=True)
        ids = (lane_cw + (base + k * CW)).astype(F32)
        target = jnp.sum(jnp.where(ids == COL[rows, 0:1], a, 0.0), axis=1, keepdims=True)
        old = COL[rows, :]
        old = jnp.where(lane128 == 8 + k, top, old)
        old = jnp.where(lane128 == 12 + k, total, old)
        COL[rows, :] = jnp.where(lane128 == 16 + k, target, old)

    def tasks(k0, nk, o0, no, out=True):
        def step(i, carry):
            k, o = k0 + i // no, o0 + lax.rem(i, no)
            r = jnp.where(o == 2, 3, jnp.where(o == 3, 2, o))
            task(k, r)
            if not out:
                return carry
            if o0:
                lg_remote(k, r).start()
            else:
                pl.when(r > 0)(lambda: lg_remote(k, r).start())
                pl.when(r == 0)(lambda: lg_local(k).start())
            return carry

        lax.fori_loop(0, nk * no, step, 0)

    drain(first)
    send_w(0)
    for r in ORDER:
        send(AX.at[x], AX.at[x], ax + r - 1, {"x": xn(r)})
    send_w(1)
    for k in range(3):
        y_own(k, 0)
    drain(own_h)
    for r in ORDER:
        send(hpiece(x, v), hpiece(x, v), hx + r - 1, {"x": xn(r)}, hsends)
    send_w(2)
    send_w(3)
    phase("p1a")
    y_fwd(0, 0)
    for r in ORDER:
        y_own(0, r)
    phase("p1b")
    for r in ORDER:
        y_own(1, r)
    phase("p1c")
    y_fwd(0, 1)
    y_fwd(0, 3)
    phase("h_in13")
    h_in(1)
    h_in(3)
    phase("p1d")
    y_fwd(0, 2)
    y_own(3, 0)
    y_fwd(1, 0)
    y_fwd(1, 1)
    phase("cols")

    for r in ORDER:
        got(AX.at[xp(r)], ax + r - 1)
    sub = lax.broadcasted_iota(jnp.int32, (8, 128), 0).astype(F32)
    counts = jnp.zeros((8, 128), F32)
    for xb in range(NX):
        for q in range(3):
            tile = AX[xb, q]
            n = min(128, T - q * 128)
            turned = jnp.concatenate([tile, jnp.zeros((120, 128), F32)], axis=0).T
            COL[pl.ds(xb * T + q * 128, n), :] = turned[:n]
            counts = counts + (tile[1:2, :] == sub).astype(F32)
    CN[y] = counts
    cn = take("r", 3)
    for r in (1, 3, 2):
        send(CN.at[y], CN.at[y], cn + r - 1, {"y": yn(r)})
    drain(rest)
    lora_in(0)
    phase("p1e")
    y_fwd(1, 3)
    y_fwd(1, 2)
    phase("h_fwd1")
    h_fwd(1)
    phase("h_in2")
    h_in(2)
    phase("w_end0")
    w_end(0)
    phase("t0_0")
    tasks(0, 1, 0, 1)
    phase("y_own2")
    for r in ORDER:
        y_own(2, r)
    phase("h_fwd3")
    h_fwd(3)
    phase("y_own3")
    for r in ORDER:
        y_own(3, r)
    phase("w_end1")
    w_end(1)
    phase("t1_0")
    tasks(1, 1, 0, 1)
    phase("h_last1")
    h_last(1)
    h_end(1)
    phase("t01_1")
    lora_in(1)
    tasks(0, 2, 1, 1)
    phase("y_fwd2")
    for r in (0, 1, 3, 2):
        y_fwd(2, r)
    phase("h_fwd2")
    h_fwd(2)
    phase("h_last3")
    h_last(3)
    phase("y_fwd3")
    y_fwd(3, 0)
    y_fwd(3, 1)
    phase("h_end3")
    h_end(3)
    phase("t01_3")
    lora_in(3)
    tasks(0, 2, 2, 1)
    phase("y_fwd3b")
    y_fwd(3, 3)
    y_fwd(3, 2)
    phase("h_last2")
    h_last(2)
    h_end(2)
    phase("t01_2")
    lora_in(2)
    tasks(0, 2, 3, 1)
    drain_sends(hsends)
    phase("w_end2")
    w_end(2)
    phase("t2")
    tasks(2, 1, 0, 4)
    phase("w_end3")
    w_end(3)
    phase("t3")
    tasks(3, 1, 0, 4, False)
    phase("stats_a")

    STA[v] = jnp.broadcast_to(jnp.ones((1, 1, 1), F32), (3, 16, 128))
    JR[...] = jnp.full((16, 128), -1.0, F32)
    for b in range(NB):
        t = COL[b * 128 : (b + 1) * 128, :].T
        m, e, g = t[8:12], t[12:16], t[16:20]
        top = jnp.max(m, axis=0, keepdims=True)
        STA[v, 0, b : b + 1, :] = top
        STA[v, 1, b : b + 1, :] = jnp.sum(e * jnp.exp(m - top), axis=0, keepdims=True)
        STA[v, 2, b : b + 1, :] = jnp.sum(g, axis=0, keepdims=True)
        JR[b : b + 1, :] = t[1:2]
    sa = take("r", 7)
    sb = take("r", 3)
    turns = [(a, b) for a in (2, 1, 3, 0) for b in range(NC) if a or b]
    for a, b in turns:
        dev = {"z": zn(a), "c": lax.rem(c + b, NC)}
        send(STA.at[v], STA.at[v], sa + a * NC + b - 1, dev)
    phase("counts")
    for r in (1, 3, 2):
        got(CN.at[lax.rem(y + NY - r, NY)], cn + r - 1)
    counts = jnp.sum(CN[0] + CN[1] + CN[2] + CN[3], axis=1, keepdims=True)
    counts = jnp.maximum(counts, 1.0)
    per_job = TOKENS / (JOBS * counts)
    jobs = JR[...]
    weight = jnp.zeros((16, 128), F32)
    for j in range(JOBS):
        weight = jnp.where(jobs == float(j), per_job[j : j + 1, :], weight)
    phase("stats_w")
    for a, b in turns:
        src = lax.rem(z + NZ - a, NZ) * NC + lax.rem(c + b, NC)
        got(STA.at[src], sa + a * NC + b - 1)

    def joined(ref, n):
        top = functools.reduce(jnp.maximum, [ref[i, 0] for i in range(n)])
        e = functools.reduce(jnp.add, [ref[i, 1] * jnp.exp(ref[i, 0] - top) for i in range(n)])
        return top, e, functools.reduce(jnp.add, [ref[i, 2] for i in range(n)])

    STB[x, 0], STB[x, 1], STB[x, 2] = joined(STA, NZ * NC)
    phase("stats_b")
    for r in (2, 1, 3):
        send(STB.at[x], STB.at[x], sb + r - 1, {"x": xn(r)})
    for r in ORDER:
        lg_remote(NK - 1, r).start()
    lg_local(NK - 1).start()
    for r in (2, 1, 3):
        got(STB.at[xp(r)], sb + r - 1)
    phase("finish")
    top, e, g = joined(STB, NX)
    loss = top + jnp.log(e) - g
    scaled = weight / e
    blank = jnp.zeros((124, 128), F32)
    for b in range(NB):
        parts = [i[b : b + 1] for i in (top, scaled, weight, loss)]
        COL2[b * 128 : (b + 1) * 128, :] = jnp.concatenate(parts + [blank], axis=0).T

    grs = take("r", 6)

    def gradient(j):
        part = pl.ds(OFF[j], LEN[j])

        def step(m, carry):
            rows = pl.ds(al(m * T + OFF[j], 16), LEN[j])
            lab = COL[rows, 0:1]
            weight = COL2[rows, 2:3]
            for k in range(NK):
                f = jnp.exp(COL[rows, 8 + k : 9 + k] - COL2[rows, 0:1]) * COL2[rows, 1:2]
                ids = (lane_cw[: LEN[j]] + (base + k * CW)).astype(F32)
                g = E[k, rows, :] * f - jnp.where(ids == lab, weight, 0.0)
                G5[m, part, k * CW : (k + 1) * CW] = g.astype(BF16)
            lora = tdot(G5[m, part, 0:U], AU[...])
            lora = jnp.where(COL[rows, 1:2] == rank_job[: LEN[j]], lora, 0.0)
            high = lora.astype(BF16)
            G5[m, part, U : U + 128] = high
            G5[m, part, U + 128 : U + 256] = (lora - high.astype(F32)).astype(BF16)
            return carry

        lax.fori_loop(0, NX, step, 0)

    def send_rows(i):
        part = pl.ds(OFF[2 * i], LEN[2 * i] * 2)
        dst = gr.at[part, pl.ds(my_cols, U)]
        for r in ORDER:
            send(G5.at[xn(r), part, pl.ds(0, U)], dst, grs + i * 3 + r - 1, {"x": xn(r)})
        load(G5.at[x, part, pl.ds(0, U)], dst, outs)

    cs_s, cs_r = take("s", 32), take("r", 32)
    ring_s, ring_r = take("s", 24), take("r", 24)

    def zt(s, h):
        return lax.rem(z + NZ + (2 * h - 1) * (s + 1), NZ)

    def span(j):
        return pl.ds(NX * OFF[j], NX * LEN[j])

    def unit(s, h, j, core):
        at = al((zt(s, h) * NC + core) * SH + h * CW, CW)
        g = G5[:, OFF[j] : OFF[j] + LEN[j], :].reshape(NX * LEN[j], U + 256)
        return tdot(g, W5[pl.ds(at, CW), :])

    def ps(s, h, j, at=0):
        return H.at[span(j), pl.ds(al(at + (s * 2 + h) * CW, CW), CW)]

    def ps_copy(s, h, j):
        i = (s * 2 + h) * NQ + j
        return rcopy(ps(s, h, j), ps(s, h, j, D // 2), cs_s + i, cs_r + i, other)

    def ring_copy(s, h, j):
        i = (s * 2 + h) * NQ + j
        return rcopy(
            RR.at[s, h, span(j)], RR.at[s + 1, h, span(j)], ring_s + i, ring_r + i,
            {"z": lax.rem(z + NZ + 1 - 2 * h, NZ)},
        )

    def for_core(s, j):
        def step(h, carry):
            ps(s, h, j)[...] = unit(s, h, j, 1 - c).astype(BF16)
            ps_copy(s, h, j).start()
            return carry

        lax.fori_loop(0, 2, step, 0)

    def mine(s, h, j):
        a = unit(s, h, j, c)
        ps_copy(s, h, j).wait_recv()
        return a + ps(s, h, j, D // 2)[...].astype(F32)

    def with_ring(s, h, j):
        a = mine(s, h, j)
        ring_copy(s - 1, h, j).wait_recv()
        return a + RR[s, h, span(j), :].astype(F32)

    def own(s, j, get):
        def step(h, carry):
            RR[s, h, span(j), :] = get(s, h, j).astype(BF16)
            ring_copy(s, h, j).start()
            return carry

        lax.fori_loop(0, 2, step, 0)

    phase("grad0")
    gradient(0)
    phase("core00")
    for_core(0, 0)
    phase("grad1")
    gradient(1)
    send_rows(0)
    phase("own00")
    own(0, 0, mine)
    phase("core01")
    for_core(0, 1)
    phase("grad2")
    gradient(2)
    phase("own01")
    own(0, 1, mine)
    phase("core02")
    for_core(0, 2)
    phase("grad3")
    gradient(3)
    send_rows(1)
    phase("own02")
    own(0, 2, mine)
    phase("core03")
    for_core(0, 3)
    for_core(1, 0)
    phase("own03")
    own(0, 3, mine)
    phase("core1")
    for j in range(1, NQ):
        for_core(1, j)

    phase("losses")
    sums = [jnp.sum(jnp.where(jobs == float(j), loss, 0.0), axis=0, keepdims=True) for j in range(JOBS)]
    JL[y] = jnp.concatenate(sums, axis=0)
    jn = take("r", 3)
    for r in (1, 3, 2):
        send(JL.at[y], JL.at[y], jn + r - 1, {"y": yn(r)})
    for q in range(3):
        n = min(128, T - q * 128)
        t = COL2[pl.ds(al(x * T + q * 128, 8), n), :]
        if n < 128:
            t = jnp.concatenate([t, jnp.zeros((128 - n, 128), F32)], axis=0)
        small[0:1, q * 128 : (q + 1) * 128] = t.T[3:4]
    for r in (1, 3, 2):
        got(JL.at[lax.rem(y + NY - r, NY)], jn + r - 1)
    total = jnp.sum(JL[0] + JL[1] + JL[2] + JL[3], axis=1, keepdims=True) / counts
    total = jnp.concatenate([jnp.broadcast_to(total, (8, 128)), jnp.zeros((120, 128), F32)], axis=0)
    small[0:1, 384:512] = total.T[0:1]

    phase("ring")

    def ring_step(s, carry):
        for j in range(NQ):
            own(s, j, with_ring)
            for_core(s + 1, j)
        return carry

    lax.fori_loop(1, NZ - 1, ring_step, 0)

    xr = take("r", 3 * NQ)
    ag = take("r", 3 * NQ)
    cc = take("r", 4 * 2 * NQ)

    def hg_cols(zz, core, h):
        return pl.ds(al(((NC * core + h) * NY + zz) * DB, DB), DB)

    def spread(src, zz, j, sem):
        for h in range(2):
            piece = src.at[pl.ds(OFF[j], LEN[j]), pl.ds(h * CW, CW)]
            dst = hg.at[pl.ds(OFF[j], LEN[j]), hg_cols(zz, c, h)]
            send(piece, dst, sem + h, other)
            load(piece, dst, outs)

    def last(j):
        part = pl.ds(OFF[j], LEN[j])
        phase("last%d" % j)
        for h in range(2):
            a = with_ring(NZ - 1, h, j)
            XS[:, OFF[j] : OFF[j] + LEN[j], h * CW : (h + 1) * CW] = a.astype(BF16).reshape(NX, LEN[j], CW)
        for r in (2, 1, 3):
            send(XS.at[xn(r), part], XR.at[r - 1, part], xr + j * 3 + r - 1, {"x": xn(r)})

    def x_sum(j):
        part = pl.ds(OFF[j], LEN[j])
        phase("xsum%d" % j)
        total = XS[x, part, :].astype(F32)
        for r in (1, 3, 2):
            got(XR.at[r - 1, part], xr + j * 3 + r - 1)
            total = total + XR[r - 1, part, :].astype(F32)
        FO[part, :] = total.astype(BF16)
        for r in (2, 1, 3):
            send(FO.at[part], AG.at[r - 1, part], ag + j * 3 + r - 1, {"z": zn(r)})
        spread(FO, z, j, cc + j * 8)

    def gather(j):
        part = pl.ds(OFF[j], LEN[j])
        phase("gather%d" % j)
        for r in (1, 3, 2):
            got(AG.at[r - 1, part], ag + j * 3 + r - 1)
            spread(AG.at[r - 1], lax.rem(z + NZ - r, NZ), j, cc + j * 8 + 2 * r)

    last(0)
    last(1)
    x_sum(0)
    last(2)
    x_sum(1)
    last(3)
    x_sum(2)
    gather(0)
    x_sum(3)
    gather(1)
    gather(2)
    gather(3)

    phase("arrivals")
    for k in range(NK):
        for r in ORDER:
            cols = al(xp(r) * U + k * CW, CW)
            got(lg.at[:, pl.ds(cols, CW)], lgs + k * 3 + r - 1)
            lg_remote(k, r).wait_send()
        lg_local(k).wait()
    for i in range(2):
        for r in ORDER:
            part = pl.ds(OFF[2 * i], LEN[2 * i] * 2)
            got(gr.at[part, pl.ds(al(xp(r) * U, U), U)], grs + i * 3 + r - 1)
    for j in range(NQ):
        rows = pl.ds(OFF[j], LEN[j])
        for h in range(2):
            got(hg.at[rows, hg_cols(z, 1 - c, h)], cc + j * 8 + h)
            for r in (1, 3, 2):
                got(hg.at[rows, hg_cols(lax.rem(z + NZ - r, NZ), 1 - c, h)], cc + j * 8 + 2 * r + h)
    for s in range(NZ):
        for h in range(2):
            for j in range(NQ):
                ps_copy(s, h, j).wait_send()
                if s < NZ - 1:
                    ring_copy(s, h, j).wait_send()
    phase("drain")
    drain_sends(pending)
    drain(outs)
    phase(None)
    assert used["s"] <= NSEND and used["r"] <= NRECV and used["l"] <= NLOAD, used


NSEND, NRECV, NLOAD = 320, 304, 112


def vmem(*shape, dtype=BF16):
    return pltpu.VMEM(shape, dtype)


def shards(hidden, weight, down, up, labels, jobs):
    hbm = pl.BlockSpec(memory_space=pl.ANY)
    vm = pl.BlockSpec(memory_space=pltpu.VMEM)
    logits, rows, grad, small = pl.pallas_call(
        kernel,
        out_shape=(
            jax.ShapeDtypeStruct((T, V), BF16),
            jax.ShapeDtypeStruct((T, V), BF16),
            jax.ShapeDtypeStruct((T, D), BF16),
            jax.ShapeDtypeStruct((1, 512), F32),
        ),
        in_specs=[hbm] * 4 + [vm],
        out_specs=(hbm, hbm, hbm, vm),
        scratch_shapes=[
            vmem(S, D),
            vmem(D, U + 256),
            vmem(DB, V),
            vmem(NK, S, CW, dtype=F32),
            vmem(S, U),
            vmem(NX, T, U + 256),
            vmem(NZ, 2, S, CW),
            vmem(NX, T, SH),
            vmem(3, T, SH),
            vmem(T, SH),
            vmem(3, T, SH),
            vmem(S, 128, dtype=F32),
            vmem(S, 128, dtype=F32),
            vmem(S, 128),
            vmem(128, U),
            vmem(NX, 3, 8, 128, dtype=F32),
            vmem(NZ * NC, 3, 16, 128, dtype=F32),
            vmem(NX, 3, 16, 128, dtype=F32),
            vmem(16, 128, dtype=F32),
            vmem(NY, 8, 128, dtype=F32),
            vmem(NY, 8, 128, dtype=F32),
            pltpu.SemaphoreType.DMA((NSEND,)),
            pltpu.SemaphoreType.DMA((NRECV,)),
            pltpu.SemaphoreType.DMA((NLOAD,)),
        ],
        compiler_params=pltpu.CompilerParams(
            collective_id=0, has_side_effects=True, vmem_limit_bytes=58 * 1024 * 1024
        ),
        name="step",
    )(hidden, weight, down, up, jnp.stack([labels, jobs]))
    return logits, rows, grad, small[0, :T], small[0, 384 : 384 + JOBS]


def solution(mesh):
    split = Mesh(mesh.devices.reshape(NZ, NC, NX, NY), ("z", "c", "x", "y"))
    dp, vocab = ("x", "y"), ("z", "c")
    return jax.shard_map(
        shards,
        mesh=split,
        in_specs=(P(dp, None), P(dp, vocab), P(), P(None, vocab), P(dp), P(dp)),
        out_specs=(P(dp, vocab), P(dp, vocab), P(dp, None), P(dp), P()),
        check_vma=False,
    )
```

```python
import functools

import jax
import jax.numpy as jnp
from jax import lax
from jax.experimental import pallas as pl
from jax.experimental.pallas import tpu as pltpu
from jax.sharding import Mesh
from jax.sharding import PartitionSpec as P

MESH = pl.DeviceIdType.MESH
F32 = jnp.float32
BF16 = jnp.bfloat16

JOBS = 8
RANK = 16
NX = NY = NZ = 4
NC = 2
T = 352
S = NX * T
HT = T // 2
LEN = (96, 96, 80, 80)
OFF = (0, 96, 192, 272)
NQ = len(LEN)
D = 4096
DB = D // (NX * NY)
V = 4096
U = V // NX
CW = 256
NK = U // CW
SH = D // (NZ * NC)
TOKENS = S * NY
NB = S // 128


def fdot(a, b):
    return jnp.dot(a, b, preferred_element_type=F32)


def tdot(a, b):
    return lax.dot_general(a, b, (((1,), (1,)), ((), ())), preferred_element_type=F32)


def kernel(
    hid, w, ad, au, lab_in, job_in,
    lg, gr, hg, small,
    H, W5, WS, E, LT, G5, RR, XS, XR, FO, COL, COL2, LI, AU, AX, STA, STB, JR, CN, JL,
    ssem, rsem, lsem,
):
    z, c, x, y = (lax.axis_index(a) for a in ("z", "c", "x", "y"))
    v = z * NC + c

    def al(i, m):
        return pl.multiple_of(i, m)

    def xn(r):
        return lax.rem(x + r, NX)

    def yn(r):
        return lax.rem(y + r, NY)

    def zn(r):
        return lax.rem(z + r, NZ)

    used = {"s": 0, "r": 0, "l": 0}

    def take(kind, n=1):
        at = used[kind]
        used[kind] = at + n
        return at

    def rcopy(src, dst, si, ri, dev):
        return pltpu.make_async_remote_copy(
            src_ref=src, dst_ref=dst, send_sem=ssem.at[si], recv_sem=rsem.at[ri],
            device_id=dev, device_id_type=MESH,
        )

    def send(src, dst, si, ri, dev):
        rcopy(src, dst, si, ri, dev).start()

    def got(ref, ri):
        rcopy(ref, ref, 0, ri, {"x": xn(1)}).wait_recv()

    def sent(ref, si):
        rcopy(ref, ref, si, 0, {"x": xn(1)}).wait_send()

    def load(src, dst, li):
        pltpu.make_async_copy(src, dst, lsem.at[li]).start()

    def loaded(ref, li):
        pltpu.make_async_copy(ref, ref, lsem.at[li]).wait()

    scope = []

    def phase(name):
        if scope:
            scope.pop().__exit__(None, None, None)
        if name:
            scope.append(jax.named_scope(name))
            scope[0].__enter__()

    phase("entry")
    bar = pltpu.get_barrier_semaphore()
    peers = (
        [{"x": xn(r)} for r in (1, 2, 3)]
        + [{"y": yn(r)} for r in (1, 2, 3)]
        + [{"z": zn(a), "c": lax.rem(c + b, NC)} for a in range(NZ) for b in range(NC) if a or b]
    )
    for dev in peers:
        pl.semaphore_signal(bar, inc=1, device_id=dev, device_id_type=MESH)

    l_w, l_own, l_h, l_up, l_down = (take("l") for _ in range(5))
    load(w, WS, l_w)
    own_rows = pl.ds(al((y * NX + x) * DB, DB), DB)
    load(w.at[:, pl.ds(al(x * U, U), U)], W5.at[own_rows, pl.ds(0, U)], l_own)
    for p in range(NX * NY):
        n = (p % NX) * NY + p // NX
        load(hid.at[:, pl.ds(n * DB, DB)], H.at[pl.ds(al(x * T, 16), T), pl.ds(p * DB, DB)], l_h)
    load(au.at[:, pl.ds(al(x * U, U), U)], AU, l_up)
    for p in range(NX * NY):
        n = (p % NX) * NY + p // NX
        for q in range(2):
            load(
                ad.at[pl.ds(n * DB, DB), :],
                W5.at[pl.ds(p * DB, DB), pl.ds(U + q * 128, 128)],
                l_down,
            )
    for q in range(3):
        n = min(128, T - q * 128)
        AX[x, q] = jnp.full((8, 128), -1.0, F32)
        AX[x, q, 0:1, 0:n] = lab_in[pl.ds(q * 128, n)].astype(F32).reshape(1, n)
        AX[x, q, 1:2, 0:n] = job_in[pl.ds(q * 128, n)].astype(F32).reshape(1, n)
    pl.semaphore_wait(bar, len(peers))

    ORDER = (1, 3, 2)
    wx = take("r", NK * 3)
    hx = take("r", 3)
    ax, lgs, cn, sa, sb, grs, jn, cc = (take("r") for _ in range(8))
    wy = take("r", NK * 5)
    hz = take("r", 3 * 3)
    hc = take("r", 3)
    ws_s, h_s, ax_s, lg_s, cn_s, sa_s, sb_s, gr_s, cs_s, ring_s, jn_s, x_s, ag_s, cc_s = (
        take("s") for _ in range(14)
    )

    def xp(r):
        return lax.rem(x + NX - r, NX)

    def wblock(row, k):
        return W5.at[row, pl.ds(k * CW, CW)]

    def send_w(k):
        for r in ORDER:
            send(
                WS.at[:, pl.ds(al(xn(r) * U + k * CW, CW), CW)],
                wblock(own_rows, k), ws_s, wx + k * 3 + r - 1, {"x": xn(r)},
            )

    def piece(dy, r, k):
        return wblock(pl.ds(al((yn(dy) * NX + xp(r)) * DB, DB), DB), k)

    def y_own(k, r):
        src = piece(0, r, k)
        if r:
            got(src, wx + k * 3 + r - 1)
        at = wy + k * 5
        send(src, src, ws_s, at + (r if r in (0, 2) else 4), {"y": yn(1)})
        send(src, src, ws_s, at + (4 if r in (0, 2) else r), {"y": yn(3)})

    def y_fwd(k, r):
        at = wy + k * 5
        src = piece(3 if r in (0, 2) else 1, r, k)
        got(src, at + r)
        send(src, src, ws_s, at + 4, {"y": yn(1 if r in (0, 2) else 3)})

    def w_end(k):
        got(wblock(pl.ds(0, 8 * DB), k), wy + k * 5 + 4)

    other = {"c": 1 - c}

    def hpiece(xb, share, lo=0, n=T):
        return H.at[pl.ds(al(xb * T + lo, 16), n), pl.ds(al(share * SH, SH), SH)]

    def h_send(at, ri, dev):
        send(at, at, h_s, ri, dev)

    def h_in(r):
        mine = hpiece(xp(r), v)
        got(mine, hx + r - 1)
        b = hz + (r - 1) * 3
        h_send(mine, b + 0, {"z": zn(1)})
        h_send(mine, b + 1, {"z": zn(3)})
        h_send(mine, hc + r - 1, other)

    def h_fwd(r):
        xb = xp(r)
        b, d = hz + (r - 1) * 3, hc + r - 1
        left, right = zn(3) * NC + c, zn(1) * NC + c
        got(hpiece(xb, left), b + 0)
        h_send(hpiece(xb, left, 0, HT), b + 2, {"z": zn(1)})
        h_send(hpiece(xb, left), d, other)
        got(hpiece(xb, right), b + 1)
        h_send(hpiece(xb, right, HT, HT), b + 2, {"z": zn(3)})
        h_send(hpiece(xb, right), d, other)

    def h_last(r):
        far = hpiece(xp(r), zn(2) * NC + c)
        got(far, hz + (r - 1) * 3 + 2)
        h_send(far, hc + r - 1, other)

    def h_end(r):
        got(H.at[pl.ds(0, T), pl.ds(0, NZ * SH)], hc + r - 1)

    lane128 = lax.broadcasted_iota(jnp.int32, (T, 128), 1)
    rank_job = (lane128 // RANK).astype(F32)
    base = v * V + x * U
    lane_cw = lax.broadcasted_iota(jnp.int32, (T, CW), 1)
    my_cols = al(x * U, U)

    def lora_in(r):
        rows = pl.ds(al(xp(r) * T, 16), T)
        hit = COL[rows, 1:2] == rank_job
        a = fdot(H[rows, :], W5[:, U : U + 128])
        LI[rows, :] = jnp.where(hit, a, 0.0).astype(BF16)

    def lg_cols(k):
        return pl.ds(al(my_cols + k * CW, CW), CW)

    def lg_remote(k, r):
        src = LT.at[pl.ds(al(xp(r) * T, 16), T), pl.ds(al(k * CW, CW), CW)]
        send(src, lg.at[:, lg_cols(k)], lg_s, lgs, {"x": xp(r)})

    def lg_local(k):
        cols = pl.ds(al(k * CW, CW), CW)
        lg[:, lg_cols(k)] = LT[pl.ds(al(x * T, 16), T), cols]

    def task(k, r):
        rows = pl.ds(al(xp(r) * T, 16), T)
        cols = pl.ds(al(k * CW, CW), CW)
        a = fdot(H[rows, :], W5[:, cols])
        a = a + fdot(LI[rows, :], AU[:, cols])
        LT[rows, cols] = a.astype(BF16)
        top = jnp.max(a, axis=1, keepdims=True)
        e = jnp.exp(a - top)
        E[k, rows, :] = e
        total = jnp.sum(e, axis=1, keepdims=True)
        ids = (lane_cw + (base + k * CW)).astype(F32)
        target = jnp.sum(jnp.where(ids == COL[rows, 0:1], a, 0.0), axis=1, keepdims=True)
        old = COL[rows, :]
        old = jnp.where(lane128 == 8 + k, top, old)
        old = jnp.where(lane128 == 12 + k, total, old)
        COL[rows, :] = jnp.where(lane128 == 16 + k, target, old)

    def tasks(k0, nk, o0, no, out=True):
        def step(i, carry):
            k, o = k0 + i // no, o0 + lax.rem(i, no)
            r = jnp.where(o == 2, 3, jnp.where(o == 3, 2, o))
            task(k, r)
            if not out:
                return carry
            if o0:
                lg_remote(k, r)
            else:
                pl.when(r > 0)(lambda: lg_remote(k, r))
                pl.when(r == 0)(lambda: lg_local(k))
            return carry

        lax.fori_loop(0, nk * no, step, 0)

    loaded(WS, l_w)
    loaded(W5.at[own_rows, pl.ds(0, U)], l_own)
    send_w(0)
    for r in ORDER:
        send(AX.at[x], AX.at[x], ax_s, ax, {"x": xn(r)})
    for k in range(3):
        y_own(k, 0)
    loaded(H.at[pl.ds(0, T), :], l_h)

    def send_h(r):
        send(hpiece(x, v), hpiece(x, v), h_s, hx + r - 1, {"x": xn(r)})

    send_h(1)
    send_h(3)
    send_w(1)
    send_h(2)
    send_w(2)
    send_w(3)
    phase("p1a")
    y_fwd(0, 0)
    for r in ORDER:
        y_own(0, r)
    y_own(3, 0)
    phase("h_in13")
    h_in(1)
    h_in(3)
    y_fwd(1, 0)
    phase("p1c")
    y_fwd(0, 1)
    y_fwd(0, 3)
    phase("p1b")
    for r in ORDER:
        y_own(1, r)
    y_fwd(0, 2)
    phase("cols")

    got(AX.at[0:3], ax)
    sub = lax.broadcasted_iota(jnp.int32, (8, 128), 0).astype(F32)
    counts = jnp.zeros((8, 128), F32)
    for xb in range(NX):
        for q in range(3):
            tile = AX[xb, q]
            n = min(128, T - q * 128)
            turned = jnp.concatenate([tile, jnp.zeros((120, 128), F32)], axis=0).T
            COL[pl.ds(xb * T + q * 128, n), :] = turned[:n]
            counts = counts + (tile[1:2, :] == sub).astype(F32)
    CN[y] = counts
    for r in (1, 3, 2):
        send(CN.at[y], CN.at[y], cn_s, cn, {"y": yn(r)})
    loaded(AU, l_up)
    loaded(W5.at[:, pl.ds(U, 256)], l_down)
    lora_in(0)
    phase("h_fwd1")
    h_fwd(1)
    phase("p1e")
    y_fwd(1, 1)
    y_fwd(1, 3)
    phase("h_in2")
    h_in(2)
    phase("p1f")
    y_fwd(1, 2)
    phase("w_end0")
    w_end(0)
    phase("t0_0")
    tasks(0, 1, 0, 1)
    phase("y_own2")
    for r in ORDER:
        y_own(2, r)
    phase("h_fwd3")
    h_fwd(3)
    phase("y_own3")
    for r in ORDER:
        y_own(3, r)
    phase("w_end1")
    w_end(1)
    phase("t1_0")
    tasks(1, 1, 0, 1)
    phase("h_last1")
    h_last(1)
    h_end(1)
    phase("t01_1")
    lora_in(1)
    tasks(0, 2, 1, 1)
    phase("y_fwd2")
    for r in (0, 1, 3, 2):
        y_fwd(2, r)
    phase("h_fwd2")
    h_fwd(2)
    phase("h_last3")
    h_last(3)
    phase("y_fwd3")
    y_fwd(3, 0)
    y_fwd(3, 1)
    phase("h_end3")
    h_end(3)
    phase("t01_3")
    lora_in(3)
    tasks(0, 2, 2, 1)
    phase("y_fwd3b")
    y_fwd(3, 3)
    y_fwd(3, 2)
    phase("h_last2")
    h_last(2)
    h_end(2)
    phase("t01_2")
    lora_in(2)
    tasks(0, 2, 3, 1)
    sent(H.at[pl.ds(0, 3 * T), :], h_s)
    phase("w_end2")
    w_end(2)
    phase("t2")
    tasks(2, 1, 0, 4)
    phase("w_end3")
    w_end(3)
    phase("t3")
    tasks(3, 1, 0, 4, False)
    phase("stats_a")

    STA[v] = jnp.broadcast_to(jnp.ones((1, 1, 1), F32), (3, 16, 128))
    JR[...] = jnp.full((16, 128), -1.0, F32)
    for b in range(NB):
        t = COL[b * 128 : (b + 1) * 128, :].T
        m, e, g = t[8:12], t[12:16], t[16:20]
        top = jnp.max(m, axis=0, keepdims=True)
        STA[v, 0, b : b + 1, :] = top
        STA[v, 1, b : b + 1, :] = jnp.sum(e * jnp.exp(m - top), axis=0, keepdims=True)
        STA[v, 2, b : b + 1, :] = jnp.sum(g, axis=0, keepdims=True)
        JR[b : b + 1, :] = t[1:2]
    turns = [(a, b) for a in (2, 1, 3, 0) for b in range(NC) if a or b]
    for a, b in turns:
        dev = {"z": zn(a), "c": lax.rem(c + b, NC)}
        send(STA.at[v], STA.at[v], sa_s, sa, dev)
    phase("counts")
    got(CN.at[0:3], cn)
    counts = jnp.sum(CN[0] + CN[1] + CN[2] + CN[3], axis=1, keepdims=True)
    counts = jnp.maximum(counts, 1.0)
    per_job = TOKENS / (JOBS * counts)
    jobs = JR[...]
    weight = jnp.zeros((16, 128), F32)
    for j in range(JOBS):
        weight = jnp.where(jobs == float(j), per_job[j : j + 1, :], weight)
    phase("stats_w")
    got(STA.at[0:7], sa)

    def joined(ref, n):
        top = functools.reduce(jnp.maximum, [ref[i, 0] for i in range(n)])
        e = functools.reduce(jnp.add, [ref[i, 1] * jnp.exp(ref[i, 0] - top) for i in range(n)])
        return top, e, functools.reduce(jnp.add, [ref[i, 2] for i in range(n)])

    STB[x, 0], STB[x, 1], STB[x, 2] = joined(STA, NZ * NC)
    phase("stats_b")
    for r in (2, 1, 3):
        send(STB.at[x], STB.at[x], sb_s, sb, {"x": xn(r)})
    for r in ORDER:
        lg_remote(NK - 1, r)
    lg_local(NK - 1)
    got(STB.at[0:3], sb)
    phase("finish")
    top, e, g = joined(STB, NX)
    loss = top + jnp.log(e) - g
    scaled = weight / e
    blank = jnp.zeros((124, 128), F32)
    for b in range(NB):
        parts = [i[b : b + 1] for i in (top, scaled, weight, loss)]
        COL2[b * 128 : (b + 1) * 128, :] = jnp.concatenate(parts + [blank], axis=0).T

    def gradient(j):
        part = pl.ds(OFF[j], LEN[j])

        def step(m, carry):
            rows = pl.ds(al(m * T + OFF[j], 16), LEN[j])
            lab = COL[rows, 0:1]
            weight = COL2[rows, 2:3]
            for k in range(NK):
                f = jnp.exp(COL[rows, 8 + k : 9 + k] - COL2[rows, 0:1]) * COL2[rows, 1:2]
                ids = (lane_cw[: LEN[j]] + (base + k * CW)).astype(F32)
                g = E[k, rows, :] * f - jnp.where(ids == lab, weight, 0.0)
                G5[m, part, k * CW : (k + 1) * CW] = g.astype(BF16)
            return carry

        lax.fori_loop(0, NX, step, 0)
        rows = G5[:, OFF[j] : OFF[j] + LEN[j], 0:U].reshape(NX * LEN[j], U)
        lora = tdot(rows, AU[...]).reshape(NX, LEN[j], 128)
        for m in range(NX):
            job = COL[m * T + OFF[j] : m * T + OFF[j] + LEN[j], 1:2]
            one = jnp.where(job == rank_job[: LEN[j]], lora[m], 0.0)
            high = one.astype(BF16)
            G5[m, part, U : U + 128] = high
            G5[m, part, U + 128 : U + 256] = (one - high.astype(F32)).astype(BF16)

    def send_rows(i):
        part = pl.ds(OFF[2 * i], LEN[2 * i] * 2)
        for r in ORDER:
            send(G5.at[xn(r), part, pl.ds(0, U)], gr.at[part, pl.ds(my_cols, U)], gr_s, grs, {"x": xn(r)})
        gr[part, pl.ds(my_cols, U)] = G5[x, part, 0:U]

    cs_r = take("r", 32)
    ring_r = take("r", 24)

    def zt(s, h):
        return lax.rem(z + NZ + (2 * h - 1) * (s + 1), NZ)

    def span(j):
        return pl.ds(NX * OFF[j], NX * LEN[j])

    def unit(s, h, j, core):
        at = al((zt(s, h) * NC + core) * SH + h * CW, CW)
        g = G5[:, OFF[j] : OFF[j] + LEN[j], :].reshape(NX * LEN[j], U + 256)
        return tdot(g, W5[pl.ds(at, CW), :])

    def ps(s, h, j, at=0):
        return H.at[span(j), pl.ds(al(at + (s * 2 + h) * CW, CW), CW)]

    def ps_copy(s, h, j):
        i = (s * 2 + h) * NQ + j
        return rcopy(ps(s, h, j), ps(s, h, j, D // 2), cs_s, cs_r + i, other)

    def ring_copy(s, h, j):
        i = (s * 2 + h) * NQ + j
        return rcopy(
            RR.at[s, h, span(j)], RR.at[s + 1, h, span(j)], ring_s, ring_r + i,
            {"z": lax.rem(z + NZ + 1 - 2 * h, NZ)},
        )

    def for_core(s, j):
        def step(h, carry):
            ps(s, h, j)[...] = unit(s, h, j, 1 - c).astype(BF16)
            ps_copy(s, h, j).start()
            return carry

        lax.fori_loop(0, 2, step, 0)

    def mine(s, h, j):
        a = unit(s, h, j, c)
        ps_copy(s, h, j).wait_recv()
        return a + ps(s, h, j, D // 2)[...].astype(F32)

    def with_ring(s, h, j):
        a = mine(s, h, j)
        ring_copy(s - 1, h, j).wait_recv()
        return a + RR[s, h, span(j), :].astype(F32)

    def own(s, j, get):
        def step(h, carry):
            RR[s, h, span(j), :] = get(s, h, j).astype(BF16)
            ring_copy(s, h, j).start()
            return carry

        lax.fori_loop(0, 2, step, 0)

    phase("grad0")
    gradient(0)
    phase("core00")
    for_core(0, 0)
    phase("own00")
    own(0, 0, mine)
    phase("grad1")
    gradient(1)
    send_rows(0)
    phase("core01")
    for_core(0, 1)
    phase("grad2")
    gradient(2)
    phase("own01")
    own(0, 1, mine)
    phase("core02")
    for_core(0, 2)
    phase("grad3")
    gradient(3)
    send_rows(1)
    phase("own02")
    own(0, 2, mine)
    phase("core03")
    for_core(0, 3)
    for_core(1, 0)
    phase("own03")
    own(0, 3, mine)
    phase("core1")
    for j in range(1, NQ):
        for_core(1, j)

    phase("losses")
    sums = [jnp.sum(jnp.where(jobs == float(j), loss, 0.0), axis=0, keepdims=True) for j in range(JOBS)]
    JL[y] = jnp.concatenate(sums, axis=0)
    for r in (1, 3, 2):
        send(JL.at[y], JL.at[y], jn_s, jn, {"y": yn(r)})
    for q in range(3):
        n = min(128, T - q * 128)
        t = COL2[pl.ds(al(x * T + q * 128, 8), n), :]
        if n < 128:
            t = jnp.concatenate([t, jnp.zeros((128 - n, 128), F32)], axis=0)
        small[0:1, q * 128 : (q + 1) * 128] = t.T[3:4]
    got(JL.at[0:3], jn)
    total = jnp.sum(JL[0] + JL[1] + JL[2] + JL[3], axis=1, keepdims=True) / counts
    total = jnp.concatenate([jnp.broadcast_to(total, (8, 128)), jnp.zeros((120, 128), F32)], axis=0)
    small[0:1, 384:512] = total.T[0:1]

    phase("ring")

    def ring_step(s, carry):
        for j in range(NQ):
            own(s, j, with_ring)
            for_core(s + 1, j)
        return carry

    lax.fori_loop(1, NZ - 1, ring_step, 0)

    xr = take("r", NQ)
    ag = take("r", 3 * NQ)

    def hg_at(zz, j, h):
        cols = pl.ds(al(((NC * c + h) * NY + zz) * DB, DB), DB)
        return hg.at[pl.ds(OFF[j], LEN[j]), cols]

    def last(j):
        part = pl.ds(OFF[j], LEN[j])
        phase("last%d" % j)
        for h in range(2):
            a = with_ring(NZ - 1, h, j)
            XS[:, OFF[j] : OFF[j] + LEN[j], h * CW : (h + 1) * CW] = a.astype(BF16).reshape(NX, LEN[j], CW)
        for r in (2, 1, 3):
            send(XS.at[xn(r), part], XR.at[r - 1, part], x_s, xr + j, {"x": xn(r)})

    def x_sum(j):
        part = pl.ds(OFF[j], LEN[j])
        phase("xsum%d" % j)
        got(XR.at[:, part], xr + j)
        total = XS[x, part, :].astype(F32)
        for r in (1, 3, 2):
            total = total + XR[r - 1, part, :].astype(F32)
        FO[part, :] = total.astype(BF16)
        for h in range(2):
            src = FO.at[part, pl.ds(h * CW, CW)]
            for r in (2, 1, 3):
                send(src, hg_at(z, j, h), ag_s, ag + j * 3 + r - 1, {"z": zn(r)})
            send(src, hg_at(z, j, h), cc_s, cc, other)
            hg_at(z, j, h)[...] = FO[part, h * CW : (h + 1) * CW]

    def gather(j):
        phase("gather%d" % j)
        for r in (1, 3, 2):
            got(hg.at[pl.ds(OFF[j], LEN[j]), pl.ds(0, SH)], ag + j * 3 + r - 1)
            for h in range(2):
                src = hg_at(lax.rem(z + NZ - r, NZ), j, h)
                send(src, src, cc_s, cc, other)

    last(0)
    last(1)
    x_sum(0)
    last(2)
    x_sum(1)
    last(3)
    x_sum(2)
    gather(0)
    x_sum(3)
    gather(1)
    gather(2)
    gather(3)

    phase("arrivals")
    got(lg.at[:, pl.ds(0, 3 * U)], lgs)
    got(gr.at[:, pl.ds(0, 3 * U)], grs)
    got(hg.at[:, pl.ds(0, NZ * SH)], cc)
    phase("drain")
    sent(W5.at[pl.ds(0, 60 * DB // NX), pl.ds(0, U)], ws_s)
    sent(AX.at[0:3], ax_s)
    sent(lg.at[:, pl.ds(0, 3 * U)], lg_s)
    sent(CN.at[0:3], cn_s)
    sent(STA.at[0:7], sa_s)
    sent(STB.at[0:3], sb_s)
    sent(gr.at[:, pl.ds(0, 3 * U)], gr_s)
    sent(H.at[:, pl.ds(0, D // 2)], cs_s)
    sent(RR.at[0:3], ring_s)
    sent(JL.at[0:3], jn_s)
    sent(XR, x_s)
    sent(XR, ag_s)
    sent(hg.at[:, pl.ds(0, NZ * SH)], cc_s)
    phase(None)
    assert used == {"s": NSEND, "r": NRECV, "l": NLOAD}, used


NSEND, NRECV, NLOAD = 14, 127, 5


def emit(lgv, grv, hgv, small, lg, gr, hg, tl, jl, sem):
    copies = [
        pltpu.make_async_copy(src, dst, sem.at[i])
        for i, (src, dst) in enumerate(((lgv, lg), (grv, gr), (hgv, hg)))
    ]
    for d in copies:
        d.start()
    tl[...] = small[0, :T]
    jl[...] = small[0, 384 : 384 + JOBS]
    for d in copies:
        d.wait()


def vmem(*shape, dtype=BF16):
    return pltpu.VMEM(shape, dtype)


def shards(hidden, weight, down, up, labels, jobs):
    hbm = pl.BlockSpec(memory_space=pl.ANY)
    vm = pl.BlockSpec(memory_space=pltpu.VMEM)
    held = pl.pallas_call(
        kernel,
        out_shape=(vmem(T, V), vmem(T, V), vmem(T, D), vmem(1, 512, dtype=F32)),
        in_specs=[hbm] * 4 + [vm] * 2,
        out_specs=(vm, vm, vm, vm),
        scratch_shapes=[
            vmem(S, D),
            vmem(D, U + 256),
            vmem(DB, V),
            vmem(NK, S, CW, dtype=F32),
            vmem(S, U),
            vmem(NX, T, U + 256),
            vmem(NZ, 2, S, CW),
            vmem(NX, T, SH),
            vmem(3, T, SH),
            vmem(T, SH),
            vmem(S, 128, dtype=F32),
            vmem(S, 128, dtype=F32),
            vmem(S, 128),
            vmem(128, U),
            vmem(NX, 3, 8, 128, dtype=F32),
            vmem(NZ * NC, 3, 16, 128, dtype=F32),
            vmem(NX, 3, 16, 128, dtype=F32),
            vmem(16, 128, dtype=F32),
            vmem(NY, 8, 128, dtype=F32),
            vmem(NY, 8, 128, dtype=F32),
            pltpu.SemaphoreType.DMA((NSEND,)),
            pltpu.SemaphoreType.DMA((NRECV,)),
            pltpu.SemaphoreType.DMA((NLOAD,)),
        ],
        compiler_params=pltpu.CompilerParams(
            collective_id=0, has_side_effects=True, vmem_limit_bytes=52 * 1024 * 1024
        ),
        name="step",
    )(hidden, weight, down, up, labels, jobs)
    return pl.pallas_call(
        emit,
        out_shape=(
            jax.ShapeDtypeStruct((T, V), BF16),
            jax.ShapeDtypeStruct((T, V), BF16),
            jax.ShapeDtypeStruct((T, D), BF16),
            jax.ShapeDtypeStruct((T,), F32),
            jax.ShapeDtypeStruct((JOBS,), F32),
        ),
        in_specs=[vm] * 4,
        out_specs=(hbm, hbm, hbm, vm, vm),
        scratch_shapes=[pltpu.SemaphoreType.DMA((3,))],
        compiler_params=pltpu.CompilerParams(vmem_limit_bytes=1024 * 1024),
        name="emit",
    )(*(pltpu.with_memory_space_constraint(i, pltpu.VMEM) for i in held))


def solution(mesh):
    split = Mesh(mesh.devices.reshape(NZ, NC, NX, NY), ("z", "c", "x", "y"))
    dp, vocab = ("x", "y"), ("z", "c")
    return jax.shard_map(
        shards,
        mesh=split,
        in_specs=(P(dp, None), P(dp, vocab), P(), P(None, vocab), P(dp), P(dp)),
        out_specs=(P(dp, vocab), P(dp, vocab), P(dp, None), P(dp), P()),
        check_vma=False,
    )
```

```python
import functools

import jax
import jax.numpy as jnp
from jax import lax
from jax.experimental import pallas as pl
from jax.experimental.pallas import tpu as pltpu
from jax.sharding import Mesh
from jax.sharding import PartitionSpec as P

MESH = pl.DeviceIdType.MESH
F32 = jnp.float32
BF16 = jnp.bfloat16

JOBS = 8
RANK = 16
NX = NY = NZ = 4
NC = 2
T = 352
S = NX * T
HT = T // 2
LEN = (80, 112, 96, 64)
OFF = (0, 80, 192, 288)
NQ = len(LEN)
D = 4096
DB = D // (NX * NY)
V = 4096
U = V // NX
CW = 256
NK = U // CW
SH = D // (NZ * NC)
TOKENS = S * NY
NB = S // 128


def fdot(a, b):
    return jnp.dot(a, b, preferred_element_type=F32)


def tdot(a, b):
    return lax.dot_general(a, b, (((1,), (1,)), ((), ())), preferred_element_type=F32)


def kernel(
    hid, w, ad, au, lab_in, job_in,
    lg, gr, hg, small,
    H, W5, WS, E, LT, G5, RR, XS, XR, FO, COL, COL2, LI, AU, AX, STA, STB, JR, CN, JL,
    ssem, rsem, lsem,
):
    z, c, x, y = (lax.axis_index(a) for a in ("z", "c", "x", "y"))
    v = z * NC + c

    def al(i, m):
        return pl.multiple_of(i, m)

    def xn(r):
        return lax.rem(x + r, NX)

    def yn(r):
        return lax.rem(y + r, NY)

    def zn(r):
        return lax.rem(z + r, NZ)

    used = {"s": 0, "r": 0, "l": 0}

    def take(kind, n=1):
        at = used[kind]
        used[kind] = at + n
        return at

    def rcopy(src, dst, si, ri, dev):
        return pltpu.make_async_remote_copy(
            src_ref=src, dst_ref=dst, send_sem=ssem.at[si], recv_sem=rsem.at[ri],
            device_id=dev, device_id_type=MESH,
        )

    def send(src, dst, si, ri, dev):
        rcopy(src, dst, si, ri, dev).start()

    def got(ref, ri):
        rcopy(ref, ref, 0, ri, {"x": xn(1)}).wait_recv()

    def sent(ref, si):
        rcopy(ref, ref, si, 0, {"x": xn(1)}).wait_send()

    def load(src, dst, li):
        pltpu.make_async_copy(src, dst, lsem.at[li]).start()

    def loaded(ref, li):
        pltpu.make_async_copy(ref, ref, lsem.at[li]).wait()

    scope = []

    def phase(name):
        if scope:
            scope.pop().__exit__(None, None, None)
        if name:
            scope.append(jax.named_scope(name))
            scope[0].__enter__()

    phase("entry")
    bar = pltpu.get_barrier_semaphore()
    peers = (
        [{"x": xn(r)} for r in (1, 2, 3)]
        + [{"y": yn(r)} for r in (1, 2, 3)]
        + [{"z": zn(a), "c": lax.rem(c + b, NC)} for a in range(NZ) for b in range(NC) if a or b]
    )
    for dev in peers:
        pl.semaphore_signal(bar, inc=1, device_id=dev, device_id_type=MESH)

    l_w, l_own, l_h, l_up, l_down = (take("l") for _ in range(5))
    load(w, WS, l_w)
    own_rows = pl.ds(al((y * NX + x) * DB, DB), DB)
    load(w.at[:, pl.ds(al(x * U, U), U)], W5.at[own_rows, pl.ds(0, U)], l_own)
    for p in range(NX * NY):
        n = (p % NX) * NY + p // NX
        load(hid.at[:, pl.ds(n * DB, DB)], H.at[pl.ds(al(x * T, 16), T), pl.ds(p * DB, DB)], l_h)
    load(au.at[:, pl.ds(al(x * U, U), U)], AU, l_up)
    for p in range(NX * NY):
        n = (p % NX) * NY + p // NX
        for q in range(2):
            load(
                ad.at[pl.ds(n * DB, DB), :],
                W5.at[pl.ds(p * DB, DB), pl.ds(U + q * 128, 128)],
                l_down,
            )
    for q in range(3):
        n = min(128, T - q * 128)
        AX[x, q] = jnp.full((8, 128), -1.0, F32)
        AX[x, q, 0:1, 0:n] = lab_in[pl.ds(q * 128, n)].astype(F32).reshape(1, n)
        AX[x, q, 1:2, 0:n] = job_in[pl.ds(q * 128, n)].astype(F32).reshape(1, n)
    pl.semaphore_wait(bar, len(peers))

    ORDER = (1, 3, 2)
    wx = take("r", NK * 3)
    hx = take("r", 3)
    ax, lgs, cn, sa, sb, grs, jn, cc = (take("r") for _ in range(8))
    wy = take("r", NK * 6)
    hz = take("r", 3 * 3)
    hc = take("r", 3)
    ws_s, h_s, ax_s, lg_s, cn_s, sa_s, sb_s, gr_s, cs_s, ring_s, jn_s, x_s, ag_s, cc_s = (
        take("s") for _ in range(14)
    )

    def xp(r):
        return lax.rem(x + NX - r, NX)

    def wblock(row, k):
        return W5.at[row, pl.ds(k * CW, CW)]

    def send_w(k):
        for r in ORDER:
            send(
                WS.at[:, pl.ds(al(xn(r) * U + k * CW, CW), CW)],
                wblock(own_rows, k), ws_s, wx + k * 3 + r - 1, {"x": xn(r)},
            )

    def piece(dy, r, k):
        return wblock(pl.ds(al((yn(dy) * NX + xp(r)) * DB, DB), DB), k)

    def y_own(k, r):
        src = piece(0, r, k)
        if r:
            got(src, wx + k * 3 + r - 1)
        at = wy + k * 6
        send(src, src, ws_s, at + (r if r in (0, 2) else 4), {"y": yn(1)})
        send(src, src, ws_s, at + (4 if r in (0, 2) else r), {"y": yn(3)})

    def y_fwd(k, r):
        at = wy + k * 6
        src = piece(3 if r in (0, 2) else 1, r, k)
        got(src, at + r)
        send(src, src, ws_s, at + 5, {"y": yn(1 if r in (0, 2) else 3)})

    def w_near(k):
        got(wblock(pl.ds(0, 4 * DB), k), wy + k * 6 + 4)

    def w_far(k):
        got(wblock(pl.ds(0, 4 * DB), k), wy + k * 6 + 5)

    def w_end(k):
        w_near(k)
        w_far(k)

    other = {"c": 1 - c}

    def hpiece(xb, share, lo=0, n=T):
        return H.at[pl.ds(al(xb * T + lo, 16), n), pl.ds(al(share * SH, SH), SH)]

    def h_send(at, ri, dev):
        send(at, at, h_s, ri, dev)

    def h_in(r):
        mine = hpiece(xp(r), v)
        got(mine, hx + r - 1)
        b = hz + (r - 1) * 3
        h_send(mine, b + 0, {"z": zn(1)})
        h_send(mine, b + 1, {"z": zn(3)})
        h_send(mine, hc + r - 1, other)

    def h_fwd(r):
        xb = xp(r)
        b, d = hz + (r - 1) * 3, hc + r - 1
        left, right = zn(3) * NC + c, zn(1) * NC + c
        got(hpiece(xb, left), b + 0)
        h_send(hpiece(xb, left, 0, HT), b + 2, {"z": zn(1)})
        h_send(hpiece(xb, left), d, other)
        got(hpiece(xb, right), b + 1)
        h_send(hpiece(xb, right, HT, HT), b + 2, {"z": zn(3)})
        h_send(hpiece(xb, right), d, other)

    def h_last(r):
        far = hpiece(xp(r), zn(2) * NC + c)
        got(far, hz + (r - 1) * 3 + 2)
        h_send(far, hc + r - 1, other)

    def h_end(r):
        got(H.at[pl.ds(0, T), pl.ds(0, NZ * SH)], hc + r - 1)

    lane128 = lax.broadcasted_iota(jnp.int32, (T, 128), 1)
    rank_job = (lane128 // RANK).astype(F32)
    base = v * V + x * U
    lane_cw = lax.broadcasted_iota(jnp.int32, (T, CW), 1)
    my_cols = al(x * U, U)

    def lora_in(r):
        rows = pl.ds(al(xp(r) * T, 16), T)
        hit = COL[rows, 1:2] == rank_job
        a = fdot(H[rows, :], W5[:, U : U + 128])
        LI[rows, :] = jnp.where(hit, a, 0.0).astype(BF16)

    def lg_cols(k):
        return pl.ds(al(my_cols + k * CW, CW), CW)

    def lg_remote(k, r):
        src = LT.at[pl.ds(al(xp(r) * T, 16), T), pl.ds(al(k * CW, CW), CW)]
        send(src, lg.at[:, lg_cols(k)], lg_s, lgs, {"x": xp(r)})

    def lg_local(k):
        cols = pl.ds(al(k * CW, CW), CW)
        lg[:, lg_cols(k)] = LT[pl.ds(al(x * T, 16), T), cols]

    def part_of(rows, cols, dy):
        deep = pl.ds(al(yn(dy) * NX * DB, DB), NX * DB)
        return fdot(H[rows, deep], W5[deep, cols])

    def early(k, r):
        rows = pl.ds(al(xp(r) * T, 16), T)
        cols = pl.ds(al(k * CW, CW), CW)
        E[k, rows, :] = part_of(rows, cols, 0) + part_of(rows, cols, 1) + part_of(rows, cols, 3)

    def task(k, r, rest=False):
        rows = pl.ds(al(xp(r) * T, 16), T)
        cols = pl.ds(al(k * CW, CW), CW)
        if rest:
            a = E[k, rows, :] + part_of(rows, cols, 2)
        else:
            a = fdot(H[rows, :], W5[:, cols])
        a = a + fdot(LI[rows, :], AU[:, cols])
        LT[rows, cols] = a.astype(BF16)
        top = jnp.max(a, axis=1, keepdims=True)
        e = jnp.exp(a - top)
        E[k, rows, :] = e
        total = jnp.sum(e, axis=1, keepdims=True)
        ids = (lane_cw + (base + k * CW)).astype(F32)
        target = jnp.sum(jnp.where(ids == COL[rows, 0:1], a, 0.0), axis=1, keepdims=True)
        old = COL[rows, :]
        old = jnp.where(lane128 == 8 + k, top, old)
        old = jnp.where(lane128 == 12 + k, total, old)
        COL[rows, :] = jnp.where(lane128 == 16 + k, target, old)

    def turn(o):
        return jnp.where(o == 2, 3, jnp.where(o == 3, 2, o))

    def tasks(k0, nk, o0, no):
        def step(i, carry):
            k, o = k0 + i // no, o0 + lax.rem(i, no)
            r = turn(o)
            task(k, r)
            if o0:
                lg_remote(k, r)
            else:
                pl.when(r > 0)(lambda: lg_remote(k, r))
                pl.when(r == 0)(lambda: lg_local(k))
            return carry

        lax.fori_loop(0, nk * no, step, 0)

    def each_block(f):
        def step(o, carry):
            f(turn(o))
            return carry

        lax.fori_loop(0, NX, step, 0)

    loaded(WS, l_w)
    loaded(W5.at[own_rows, pl.ds(0, U)], l_own)
    send_w(0)
    for r in ORDER:
        send(AX.at[x], AX.at[x], ax_s, ax, {"x": xn(r)})
    for k in range(3):
        y_own(k, 0)
    loaded(H.at[pl.ds(0, T), :], l_h)

    def send_h(r):
        send(hpiece(x, v), hpiece(x, v), h_s, hx + r - 1, {"x": xn(r)})

    send_h(1)
    send_h(3)
    send_w(1)
    send_h(2)
    send_w(2)
    send_w(3)
    phase("p1a")
    y_fwd(0, 0)
    for r in ORDER:
        y_own(0, r)
    y_own(3, 0)
    phase("h_in13")
    h_in(1)
    h_in(3)
    phase("p1b")
    y_fwd(1, 0)
    y_fwd(0, 1)
    y_fwd(0, 3)
    for r in ORDER:
        y_own(1, r)
    y_fwd(0, 2)
    phase("cols")

    got(AX.at[0:3], ax)
    sub = lax.broadcasted_iota(jnp.int32, (8, 128), 0).astype(F32)
    counts = jnp.zeros((8, 128), F32)
    for xb in range(NX):
        for q in range(3):
            tile = AX[xb, q]
            n = min(128, T - q * 128)
            turned = jnp.concatenate([tile, jnp.zeros((120, 128), F32)], axis=0).T
            COL[pl.ds(xb * T + q * 128, n), :] = turned[:n]
            counts = counts + (tile[1:2, :] == sub).astype(F32)
    CN[y] = counts
    for r in (1, 3, 2):
        send(CN.at[y], CN.at[y], cn_s, cn, {"y": yn(r)})
    loaded(AU, l_up)
    loaded(W5.at[:, pl.ds(U, 256)], l_down)
    lora_in(0)
    phase("h_fwd1")
    h_fwd(1)
    phase("h_in2")
    h_in(2)
    phase("p1c")
    y_fwd(1, 1)
    y_fwd(1, 3)
    phase("h_fwd3")
    h_fwd(3)
    phase("y_fwd1")
    y_fwd(1, 2)
    phase("y_own2")
    for r in ORDER:
        y_own(2, r)
    phase("h_last1")
    h_last(1)
    phase("w_end0")
    w_end(0)
    phase("t0_0")
    tasks(0, 1, 0, 1)
    phase("h_end1")
    h_end(1)
    phase("t0_1")
    lora_in(1)
    tasks(0, 1, 1, 1)
    phase("y_own3")
    for r in ORDER:
        y_own(3, r)
    phase("w_end1")
    w_end(1)
    phase("t1_01")
    tasks(1, 1, 0, 2)
    phase("h_fwd2")
    h_fwd(2)
    phase("y_fwd2")
    y_fwd(2, 0)
    y_fwd(2, 1)
    phase("h_last3")
    h_last(3)
    h_end(3)
    phase("t01_3")
    lora_in(3)
    tasks(0, 2, 2, 1)
    phase("y_fwd2b")
    y_fwd(2, 3)
    y_fwd(2, 2)
    y_fwd(3, 0)
    phase("h_last2")
    h_last(2)
    y_fwd(3, 1)
    h_end(2)
    phase("t01_2")
    lora_in(2)
    tasks(0, 2, 3, 1)
    sent(H.at[pl.ds(0, 3 * T), :], h_s)
    phase("y_fwd3")
    y_fwd(3, 3)
    y_fwd(3, 2)
    phase("w_near3")
    w_near(3)
    phase("t3a")
    each_block(functools.partial(early, NK - 1))
    phase("w_end2")
    w_end(2)
    phase("t2")
    tasks(2, 1, 0, 4)
    phase("w_far3")
    w_far(3)
    phase("t3b")
    each_block(functools.partial(task, NK - 1, rest=True))
    phase("stats_a")

    STA[v] = jnp.broadcast_to(jnp.ones((1, 1, 1), F32), (3, 16, 128))
    JR[...] = jnp.full((16, 128), -1.0, F32)
    for b in range(NB):
        t = COL[b * 128 : (b + 1) * 128, :].T
        m, e, g = t[8:12], t[12:16], t[16:20]
        top = jnp.max(m, axis=0, keepdims=True)
        STA[v, 0, b : b + 1, :] = top
        STA[v, 1, b : b + 1, :] = jnp.sum(e * jnp.exp(m - top), axis=0, keepdims=True)
        STA[v, 2, b : b + 1, :] = jnp.sum(g, axis=0, keepdims=True)
        JR[b : b + 1, :] = t[1:2]
    turns = [(a, b) for a in (2, 1, 3, 0) for b in range(NC) if a or b]
    for a, b in turns:
        dev = {"z": zn(a), "c": lax.rem(c + b, NC)}
        send(STA.at[v], STA.at[v], sa_s, sa, dev)
    phase("counts")
    got(CN.at[0:3], cn)
    counts = jnp.sum(CN[0] + CN[1] + CN[2] + CN[3], axis=1, keepdims=True)
    counts = jnp.maximum(counts, 1.0)
    per_job = TOKENS / (JOBS * counts)
    jobs = JR[...]
    weight = jnp.zeros((16, 128), F32)
    for j in range(JOBS):
        weight = jnp.where(jobs == float(j), per_job[j : j + 1, :], weight)
    phase("stats_w")
    got(STA.at[0:7], sa)

    def joined(ref, n):
        top = functools.reduce(jnp.maximum, [ref[i, 0] for i in range(n)])
        e = functools.reduce(jnp.add, [ref[i, 1] * jnp.exp(ref[i, 0] - top) for i in range(n)])
        return top, e, functools.reduce(jnp.add, [ref[i, 2] for i in range(n)])

    STB[x, 0], STB[x, 1], STB[x, 2] = joined(STA, NZ * NC)
    phase("stats_b")
    for r in (2, 1, 3):
        send(STB.at[x], STB.at[x], sb_s, sb, {"x": xn(r)})
    for r in ORDER:
        lg_remote(NK - 1, r)
    lg_local(NK - 1)
    got(STB.at[0:3], sb)
    phase("finish")
    top, e, g = joined(STB, NX)
    loss = top + jnp.log(e) - g
    scaled = weight / e
    blank = jnp.zeros((124, 128), F32)
    for b in range(NB):
        parts = [i[b : b + 1] for i in (top, scaled, weight, loss)]
        COL2[b * 128 : (b + 1) * 128, :] = jnp.concatenate(parts + [blank], axis=0).T

    def gradient(j):
        part = pl.ds(OFF[j], LEN[j])

        def step(m, carry):
            rows = pl.ds(al(m * T + OFF[j], 16), LEN[j])
            lab = COL[rows, 0:1]
            weight = COL2[rows, 2:3]
            for k in range(NK):
                f = jnp.exp(COL[rows, 8 + k : 9 + k] - COL2[rows, 0:1]) * COL2[rows, 1:2]
                ids = (lane_cw[: LEN[j]] + (base + k * CW)).astype(F32)
                g = E[k, rows, :] * f - jnp.where(ids == lab, weight, 0.0)
                G5[m, part, k * CW : (k + 1) * CW] = g.astype(BF16)
            return carry

        lax.fori_loop(0, NX, step, 0, unroll=True)
        rows = G5[:, OFF[j] : OFF[j] + LEN[j], 0:U].reshape(NX * LEN[j], U)
        lora = tdot(rows, AU[...]).reshape(NX, LEN[j], 128)
        for m in range(NX):
            job = COL[m * T + OFF[j] : m * T + OFF[j] + LEN[j], 1:2]
            one = jnp.where(job == rank_job[: LEN[j]], lora[m], 0.0)
            high = one.astype(BF16)
            G5[m, part, U : U + 128] = high
            G5[m, part, U + 128 : U + 256] = (one - high.astype(F32)).astype(BF16)

    def send_rows(i):
        part = pl.ds(OFF[2 * i], LEN[2 * i] + LEN[2 * i + 1])
        for r in ORDER:
            send(G5.at[xn(r), part, pl.ds(0, U)], gr.at[part, pl.ds(my_cols, U)], gr_s, grs, {"x": xn(r)})
        gr[part, pl.ds(my_cols, U)] = G5[x, part, 0:U]

    cs_r = take("r", 32)
    ring_r = take("r", 24)

    def zt(s, h):
        return lax.rem(z + NZ + (2 * h - 1) * (s + 1), NZ)

    def span(j):
        return pl.ds(NX * OFF[j], NX * LEN[j])

    def unit(s, h, j, core):
        at = al((zt(s, h) * NC + core) * SH + h * CW, CW)
        g = G5[:, OFF[j] : OFF[j] + LEN[j], :].reshape(NX * LEN[j], U + 256)
        return tdot(g, W5[pl.ds(at, CW), :])

    def ps(s, h, j, at=0):
        return H.at[span(j), pl.ds(al(at + (s * 2 + h) * CW, CW), CW)]

    def ps_copy(s, h, j):
        i = (s * 2 + h) * NQ + j
        return rcopy(ps(s, h, j), ps(s, h, j, D // 2), cs_s, cs_r + i, other)

    def ring_copy(s, h, j):
        i = (s * 2 + h) * NQ + j
        return rcopy(
            RR.at[s, h, span(j)], RR.at[s + 1, h, span(j)], ring_s, ring_r + i,
            {"z": lax.rem(z + NZ + 1 - 2 * h, NZ)},
        )

    def for_core(s, j):
        def step(h, carry):
            ps(s, h, j)[...] = unit(s, h, j, 1 - c).astype(BF16)
            ps_copy(s, h, j).start()
            return carry

        lax.fori_loop(0, 2, step, 0)

    def mine(s, h, j):
        a = unit(s, h, j, c)
        ps_copy(s, h, j).wait_recv()
        return a + ps(s, h, j, D // 2)[...].astype(F32)

    def with_ring(s, h, j):
        a = mine(s, h, j)
        ring_copy(s - 1, h, j).wait_recv()
        return a + RR[s, h, span(j), :].astype(F32)

    def own(s, j, get):
        def step(h, carry):
            RR[s, h, span(j), :] = get(s, h, j).astype(BF16)
            ring_copy(s, h, j).start()
            return carry

        lax.fori_loop(0, 2, step, 0)

    def losses_out():
        phase("losses")
        sums = [jnp.sum(jnp.where(jobs == float(j), loss, 0.0), axis=0, keepdims=True) for j in range(JOBS)]
        JL[y] = jnp.concatenate(sums, axis=0)
        for r in (1, 3, 2):
            send(JL.at[y], JL.at[y], jn_s, jn, {"y": yn(r)})
        for q in range(3):
            n = min(128, T - q * 128)
            t = COL2[pl.ds(al(x * T + q * 128, 8), n), :]
            if n < 128:
                t = jnp.concatenate([t, jnp.zeros((128 - n, 128), F32)], axis=0)
            small[0:1, q * 128 : (q + 1) * 128] = t.T[3:4]

    def losses_in():
        phase("losses2")
        got(JL.at[0:3], jn)
        total = jnp.sum(JL[0] + JL[1] + JL[2] + JL[3], axis=1, keepdims=True) / counts
        total = jnp.concatenate([jnp.broadcast_to(total, (8, 128)), jnp.zeros((120, 128), F32)], axis=0)
        small[0:1, 384:512] = total.T[0:1]

    first_units = (
        "g0 c00 g1 r0 o00 c01 g2 o01 c02 g3 r1 o02 c03 c10 o03 c11 o10 c12 o11 c13 o12"
        " c20 o13 c21 o20 c22 o21 c23 o22 c30 o23 c31"
    )
    for op in first_units.split():
        phase(op)
        n = [int(i) for i in op[1:]]
        if op[0] == "g":
            gradient(n[0])
        elif op[0] == "r":
            send_rows(n[0])
        elif op[0] == "c":
            for_core(*n)
        else:
            own(*n, with_ring if n[0] else mine)

    xr = take("r", NQ)
    ag = take("r", 3 * NQ)

    def hg_at(zz, j, h):
        cols = pl.ds(al(((NC * c + h) * NY + zz) * DB, DB), DB)
        return hg.at[pl.ds(OFF[j], LEN[j]), cols]

    def last(j):
        part = pl.ds(OFF[j], LEN[j])
        phase("last%d" % j)
        for h in range(2):
            a = with_ring(NZ - 1, h, j)
            XS[:, OFF[j] : OFF[j] + LEN[j], h * CW : (h + 1) * CW] = a.astype(BF16).reshape(NX, LEN[j], CW)
        for r in (2, 1, 3):
            send(XS.at[xn(r), part], XR.at[r - 1, part], x_s, xr + j, {"x": xn(r)})

    def x_sum(j):
        part = pl.ds(OFF[j], LEN[j])
        phase("xsum%d" % j)
        got(XR.at[:, part], xr + j)
        total = XS[x, part, :].astype(F32)
        for r in (1, 3, 2):
            total = total + XR[r - 1, part, :].astype(F32)
        FO[part, :] = total.astype(BF16)
        for h in range(2):
            src = FO.at[part, pl.ds(h * CW, CW)]
            for r in (1, 3):
                send(src, hg_at(z, j, h), ag_s, ag + j * 3 + r - 1, {"z": zn(r)})
            send(src, hg_at(z, j, h), cc_s, cc, other)
            hg_at(z, j, h)[...] = FO[part, h * CW : (h + 1) * CW]

    def pair_ref(j):
        return hg.at[pl.ds(OFF[j], LEN[j]), pl.ds(0, SH)]

    def relay(j):
        phase("relay%d" % j)
        for r in (1, 3):
            got(pair_ref(j), ag + j * 3 + r - 1)
            h = r // 2
            src = hg_at(lax.rem(z + NZ - r, NZ), j, h)
            send(src, src, ag_s, ag + j * 3 + 1, {"z": zn(r)})
            for h in range(2):
                src = hg_at(lax.rem(z + NZ - r, NZ), j, h)
                send(src, src, cc_s, cc, other)

    def gather(j):
        phase("gather%d" % j)
        got(pair_ref(j), ag + j * 3 + 1)
        for h in range(2):
            src = hg_at(zn(2), j, h)
            send(src, src, cc_s, cc, other)

    last(0)
    for_core(3, 2)
    last(1)
    x_sum(0)
    for_core(3, 3)
    last(2)
    x_sum(1)
    relay(0)
    last(3)
    losses_out()
    x_sum(2)
    relay(1)
    gather(0)
    x_sum(3)
    relay(2)
    gather(1)
    relay(3)
    gather(2)
    losses_in()
    gather(3)

    phase("arrivals")
    got(lg.at[:, pl.ds(0, 3 * U)], lgs)
    got(gr.at[:, pl.ds(0, 3 * U)], grs)
    got(hg.at[:, pl.ds(0, NZ * SH)], cc)
    phase("drain")
    sent(W5.at[pl.ds(0, 60 * DB // NX), pl.ds(0, U)], ws_s)
    sent(AX.at[0:3], ax_s)
    sent(lg.at[:, pl.ds(0, 3 * U)], lg_s)
    sent(CN.at[0:3], cn_s)
    sent(STA.at[0:7], sa_s)
    sent(STB.at[0:3], sb_s)
    sent(gr.at[:, pl.ds(0, 3 * U)], gr_s)
    sent(H.at[:, pl.ds(0, D // 2)], cs_s)
    sent(RR.at[0:3], ring_s)
    sent(JL.at[0:3], jn_s)
    sent(XR, x_s)
    sent(XR, ag_s)
    sent(hg.at[:, pl.ds(0, NZ * SH)], cc_s)
    phase(None)
    assert used == {"s": NSEND, "r": NRECV, "l": NLOAD}, used


NSEND, NRECV, NLOAD = 14, 131, 5


def emit(lgv, grv, hgv, small, lg, gr, hg, tl, jl, sem):
    copies = [
        pltpu.make_async_copy(src, dst, sem.at[i])
        for i, (src, dst) in enumerate(((lgv, lg), (grv, gr), (hgv, hg)))
    ]
    for d in copies:
        d.start()
    tl[...] = small[0, :T]
    jl[...] = small[0, 384 : 384 + JOBS]
    for d in copies:
        d.wait()


def vmem(*shape, dtype=BF16):
    return pltpu.VMEM(shape, dtype)


def shards(hidden, weight, down, up, labels, jobs):
    hbm = pl.BlockSpec(memory_space=pl.ANY)
    vm = pl.BlockSpec(memory_space=pltpu.VMEM)
    held = pl.pallas_call(
        kernel,
        out_shape=(vmem(T, V), vmem(T, V), vmem(T, D), vmem(1, 512, dtype=F32)),
        in_specs=[hbm] * 4 + [vm] * 2,
        out_specs=(vm, vm, vm, vm),
        scratch_shapes=[
            vmem(S, D),
            vmem(D, U + 256),
            vmem(DB, V),
            vmem(NK, S, CW, dtype=F32),
            vmem(S, U),
            vmem(NX, T, U + 256),
            vmem(NZ, 2, S, CW),
            vmem(NX, T, SH),
            vmem(3, T, SH),
            vmem(T, SH),
            vmem(S, 128, dtype=F32),
            vmem(S, 128, dtype=F32),
            vmem(S, 128),
            vmem(128, U),
            vmem(NX, 3, 8, 128, dtype=F32),
            vmem(NZ * NC, 3, 16, 128, dtype=F32),
            vmem(NX, 3, 16, 128, dtype=F32),
            vmem(16, 128, dtype=F32),
            vmem(NY, 8, 128, dtype=F32),
            vmem(NY, 8, 128, dtype=F32),
            pltpu.SemaphoreType.DMA((NSEND,)),
            pltpu.SemaphoreType.DMA((NRECV,)),
            pltpu.SemaphoreType.DMA((NLOAD,)),
        ],
        compiler_params=pltpu.CompilerParams(
            collective_id=0, has_side_effects=True, vmem_limit_bytes=52 * 1024 * 1024
        ),
        name="step",
    )(hidden, weight, down, up, labels, jobs)
    return pl.pallas_call(
        emit,
        out_shape=(
            jax.ShapeDtypeStruct((T, V), BF16),
            jax.ShapeDtypeStruct((T, V), BF16),
            jax.ShapeDtypeStruct((T, D), BF16),
            jax.ShapeDtypeStruct((T,), F32),
            jax.ShapeDtypeStruct((JOBS,), F32),
        ),
        in_specs=[vm] * 4,
        out_specs=(hbm, hbm, hbm, vm, vm),
        scratch_shapes=[pltpu.SemaphoreType.DMA((3,))],
        compiler_params=pltpu.CompilerParams(vmem_limit_bytes=1024 * 1024),
        name="emit",
    )(*(pltpu.with_memory_space_constraint(i, pltpu.VMEM) for i in held))


def solution(mesh):
    split = Mesh(mesh.devices.reshape(NZ, NC, NX, NY), ("z", "c", "x", "y"))
    dp, vocab = ("x", "y"), ("z", "c")
    return jax.shard_map(
        shards,
        mesh=split,
        in_specs=(P(dp, None), P(dp, vocab), P(), P(None, vocab), P(dp), P(dp)),
        out_specs=(P(dp, vocab), P(dp, vocab), P(dp, None), P(dp), P()),
        check_vma=False,
    )
```

```python
import functools

import jax
import jax.numpy as jnp
from jax import lax
from jax.experimental import pallas as pl
from jax.experimental.pallas import tpu as pltpu
from jax.sharding import Mesh
from jax.sharding import PartitionSpec as P

MESH = pl.DeviceIdType.MESH
F32 = jnp.float32
BF16 = jnp.bfloat16

JOBS = 8
RANK = 16
NX = NY = NZ = 4
NC = 2
T = 352
S = NX * T
HT = T // 2
LEN = (112, 96, 80, 64)
OFF = (0, 112, 208, 288)
NQ = len(LEN)
NR = NQ - 1
RT = OFF[NR]
XT = LEN[NR]
D = 4096
DB = D // (NX * NY)
V = 4096
U = V // NX
CW = 256
NK = U // CW
SH = D // (NZ * NC)
TOKENS = S * NY
NB = S // 128


def fdot(a, b):
    return jnp.dot(a, b, preferred_element_type=F32)


def tdot(a, b):
    return lax.dot_general(a, b, (((1,), (1,)), ((), ())), preferred_element_type=F32)


def kernel(
    hid, w, ad, au, lab_in, job_in,
    lg, gr, hg, small,
    H, W5, WS, E, LT, G5, RR, XS, XR, XF, XFR, ZR, FO, COL, COL2, LI, AU, AX, STA, STB, TA, TB, JR, CN, JL,
    ssem, rsem, lsem,
):
    z, c, x, y = (lax.axis_index(a) for a in ("z", "c", "x", "y"))
    v = z * NC + c

    def al(i, m):
        return pl.multiple_of(i, m)

    def xn(r):
        return lax.rem(x + r, NX)

    def yn(r):
        return lax.rem(y + r, NY)

    def zn(r):
        return lax.rem(z + r, NZ)

    used = {"s": 0, "r": 0, "l": 0}

    def take(kind, n=1):
        at = used[kind]
        used[kind] = at + n
        return at

    def rcopy(src, dst, si, ri, dev):
        return pltpu.make_async_remote_copy(
            src_ref=src, dst_ref=dst, send_sem=ssem.at[si], recv_sem=rsem.at[ri],
            device_id=dev, device_id_type=MESH,
        )

    def send(src, dst, si, ri, dev):
        rcopy(src, dst, si, ri, dev).start()

    def got(ref, ri):
        rcopy(ref, ref, 0, ri, {"x": xn(1)}).wait_recv()

    def sent(ref, si):
        rcopy(ref, ref, si, 0, {"x": xn(1)}).wait_send()

    def load(src, dst, li):
        pltpu.make_async_copy(src, dst, lsem.at[li]).start()

    def loaded(ref, li):
        pltpu.make_async_copy(ref, ref, lsem.at[li]).wait()

    scope = []

    def phase(name):
        if scope:
            scope.pop().__exit__(None, None, None)
        if name:
            scope.append(jax.named_scope(name))
            scope[0].__enter__()

    phase("entry")
    bar = pltpu.get_barrier_semaphore()
    peers = (
        [{"x": xn(r)} for r in (1, 2, 3)]
        + [{"y": yn(r)} for r in (1, 2, 3)]
        + [{"z": zn(a), "c": lax.rem(c + b, NC)} for a in range(NZ) for b in range(NC) if a or b]
    )
    for dev in peers:
        pl.semaphore_signal(bar, inc=1, device_id=dev, device_id_type=MESH)

    l_w, l_own, l_h, l_up, l_down = (take("l") for _ in range(5))
    load(w, WS, l_w)
    own_rows = pl.ds(al((y * NX + x) * DB, DB), DB)
    load(w.at[:, pl.ds(al(x * U, U), U)], W5.at[own_rows, pl.ds(0, U)], l_own)
    for p in range(NX * NY):
        n = (p % NX) * NY + p // NX
        load(hid.at[:, pl.ds(n * DB, DB)], H.at[pl.ds(al(x * T, 16), T), pl.ds(p * DB, DB)], l_h)
    load(au.at[:, pl.ds(al(x * U, U), U)], AU, l_up)
    for p in range(NX * NY):
        n = (p % NX) * NY + p // NX
        for q in range(2):
            load(
                ad.at[pl.ds(n * DB, DB), :],
                W5.at[pl.ds(p * DB, DB), pl.ds(U + q * 128, 128)],
                l_down,
            )
    for q in range(3):
        n = min(128, T - q * 128)
        AX[x, q] = jnp.full((8, 128), -1.0, F32)
        AX[x, q, 0:1, 0:n] = lab_in[pl.ds(q * 128, n)].astype(F32).reshape(1, n)
        AX[x, q, 1:2, 0:n] = job_in[pl.ds(q * 128, n)].astype(F32).reshape(1, n)
    pl.semaphore_wait(bar, len(peers))

    ORDER = (1, 3, 2)
    wx = take("r", NK * 3)
    hx = take("r", 3)
    ax, lgs, cn, sa, sb, ta, tb, grs, jn, cc, xf, zr = (take("r") for _ in range(12))
    wy = take("r", NK * 6)
    hz = take("r", 3 * 3)
    hc = take("r", 3)
    ws_s, h_s, ax_s, lg_s, cn_s, sa_s, sb_s, ta_s, tb_s, gr_s, cs_s, ring_s, jn_s, x_s, xf_s, zr_s, ag_s, cc_s = (
        take("s") for _ in range(18)
    )

    def xp(r):
        return lax.rem(x + NX - r, NX)

    def wblock(row, k):
        return W5.at[row, pl.ds(k * CW, CW)]

    def send_w(k):
        for r in ORDER:
            send(
                WS.at[:, pl.ds(al(xn(r) * U + k * CW, CW), CW)],
                wblock(own_rows, k), ws_s, wx + k * 3 + r - 1, {"x": xn(r)},
            )

    def piece(dy, r, k):
        return wblock(pl.ds(al((yn(dy) * NX + xp(r)) * DB, DB), DB), k)

    def y_own(k, r):
        src = piece(0, r, k)
        if r:
            got(src, wx + k * 3 + r - 1)
        at = wy + k * 6
        send(src, src, ws_s, at + (r if r in (0, 2) else 4), {"y": yn(1)})
        send(src, src, ws_s, at + (4 if r in (0, 2) else r), {"y": yn(3)})

    def y_fwd(k, r):
        at = wy + k * 6
        src = piece(3 if r in (0, 2) else 1, r, k)
        got(src, at + r)
        send(src, src, ws_s, at + 5, {"y": yn(1 if r in (0, 2) else 3)})

    def w_near(k):
        got(wblock(pl.ds(0, 4 * DB), k), wy + k * 6 + 4)

    def w_far(k):
        got(wblock(pl.ds(0, 4 * DB), k), wy + k * 6 + 5)

    def w_end(k):
        w_near(k)
        w_far(k)

    other = {"c": 1 - c}

    def hpiece(xb, share, lo=0, n=T):
        return H.at[pl.ds(al(xb * T + lo, 16), n), pl.ds(al(share * SH, SH), SH)]

    def h_send(at, ri, dev):
        send(at, at, h_s, ri, dev)

    def h_in(r):
        mine = hpiece(xp(r), v)
        got(mine, hx + r - 1)
        b = hz + (r - 1) * 3
        h_send(mine, b + 0, {"z": zn(1)})
        h_send(mine, b + 1, {"z": zn(3)})
        h_send(mine, hc + r - 1, other)

    def h_fwd(r):
        xb = xp(r)
        b, d = hz + (r - 1) * 3, hc + r - 1
        left, right = zn(3) * NC + c, zn(1) * NC + c
        got(hpiece(xb, left), b + 0)
        h_send(hpiece(xb, left, 0, HT), b + 2, {"z": zn(1)})
        h_send(hpiece(xb, left), d, other)
        got(hpiece(xb, right), b + 1)
        h_send(hpiece(xb, right, HT, HT), b + 2, {"z": zn(3)})
        h_send(hpiece(xb, right), d, other)

    def h_last(r):
        far = hpiece(xp(r), zn(2) * NC + c)
        got(far, hz + (r - 1) * 3 + 2)
        h_send(far, hc + r - 1, other)

    def h_end(r):
        got(H.at[pl.ds(0, T), pl.ds(0, NZ * SH)], hc + r - 1)

    lane128 = lax.broadcasted_iota(jnp.int32, (T, 128), 1)
    rank_job = (lane128 // RANK).astype(F32)
    base = v * V + x * U
    lane_cw = lax.broadcasted_iota(jnp.int32, (T, CW), 1)
    my_cols = al(x * U, U)

    def lora_in(r):
        rows = pl.ds(al(xp(r) * T, 16), T)
        hit = COL[rows, 1:2] == rank_job
        a = fdot(H[rows, :], W5[:, U : U + 128])
        LI[rows, :] = jnp.where(hit, a, 0.0).astype(BF16)

    def lg_cols(k):
        return pl.ds(al(my_cols + k * CW, CW), CW)

    def lg_remote(k, r):
        src = LT.at[pl.ds(al(xp(r) * T, 16), T), pl.ds(al(k * CW, CW), CW)]
        send(src, lg.at[:, lg_cols(k)], lg_s, lgs, {"x": xp(r)})

    def lg_local(k):
        cols = pl.ds(al(k * CW, CW), CW)
        lg[:, lg_cols(k)] = LT[pl.ds(al(x * T, 16), T), cols]

    def part_of(rows, cols, dy):
        deep = pl.ds(al(yn(dy) * NX * DB, DB), NX * DB)
        return fdot(H[rows, deep], W5[deep, cols])

    def early(k, r):
        rows = pl.ds(al(xp(r) * T, 16), T)
        cols = pl.ds(al(k * CW, CW), CW)
        E[k, rows, :] = part_of(rows, cols, 0) + part_of(rows, cols, 1) + part_of(rows, cols, 3)

    def task(k, r, rest=False):
        rows = pl.ds(al(xp(r) * T, 16), T)
        cols = pl.ds(al(k * CW, CW), CW)
        if rest:
            a = E[k, rows, :] + part_of(rows, cols, 2)
        else:
            a = fdot(H[rows, :], W5[:, cols])
        a = a + fdot(LI[rows, :], AU[:, cols])
        LT[rows, cols] = a.astype(BF16)
        top = jnp.max(a, axis=1, keepdims=True)
        e = jnp.exp(a - top)
        E[k, rows, :] = e
        total = jnp.sum(e, axis=1, keepdims=True)
        ids = (lane_cw + (base + k * CW)).astype(F32)
        target = jnp.sum(jnp.where(ids == COL[rows, 0:1], a, 0.0), axis=1, keepdims=True)
        old = COL[rows, :]
        old = jnp.where(lane128 == 8 + k, top, old)
        old = jnp.where(lane128 == 12 + k, total, old)
        COL[rows, :] = jnp.where(lane128 == 16 + k, target, old)

    def turn(o):
        return jnp.where(o == 2, 3, jnp.where(o == 3, 2, o))

    def tasks(k0, nk, o0, no):
        def step(i, carry):
            k, o = k0 + i // no, o0 + lax.rem(i, no)
            r = turn(o)
            task(k, r)
            if o0:
                lg_remote(k, r)
            else:
                pl.when(r > 0)(lambda: lg_remote(k, r))
                pl.when(r == 0)(lambda: lg_local(k))
            return carry

        lax.fori_loop(0, nk * no, step, 0)

    def each_block(f):
        def step(o, carry):
            f(turn(o))
            return carry

        lax.fori_loop(0, NX, step, 0)

    loaded(WS, l_w)
    loaded(W5.at[own_rows, pl.ds(0, U)], l_own)
    send_w(0)
    for r in ORDER:
        send(AX.at[x], AX.at[x], ax_s, ax, {"x": xn(r)})
    for k in range(3):
        y_own(k, 0)
    loaded(H.at[pl.ds(0, T), :], l_h)

    def send_h(r):
        send(hpiece(x, v), hpiece(x, v), h_s, hx + r - 1, {"x": xn(r)})

    send_h(1)
    send_h(3)
    send_w(1)
    send_h(2)
    send_w(2)
    send_w(3)
    phase("p1a")
    y_fwd(0, 0)
    for r in ORDER:
        y_own(0, r)
    y_own(3, 0)
    phase("h_in13")
    h_in(1)
    h_in(3)
    phase("p1b")
    y_fwd(1, 0)
    y_fwd(0, 1)
    y_fwd(0, 3)
    for r in ORDER:
        y_own(1, r)
    y_fwd(0, 2)
    phase("cols")

    got(AX.at[0:3], ax)
    sub = lax.broadcasted_iota(jnp.int32, (8, 128), 0).astype(F32)
    counts = jnp.zeros((8, 128), F32)
    for xb in range(NX):
        for q in range(3):
            tile = AX[xb, q]
            n = min(128, T - q * 128)
            turned = jnp.concatenate([tile, jnp.zeros((120, 128), F32)], axis=0).T
            COL[pl.ds(xb * T + q * 128, n), :] = turned[:n]
            counts = counts + (tile[1:2, :] == sub).astype(F32)
    CN[y] = counts
    for r in (1, 3, 2):
        send(CN.at[y], CN.at[y], cn_s, cn, {"y": yn(r)})
    loaded(AU, l_up)
    loaded(W5.at[:, pl.ds(U, 256)], l_down)
    lora_in(0)
    phase("h_fwd1")
    h_fwd(1)
    phase("h_in2")
    h_in(2)
    phase("p1c")
    y_fwd(1, 1)
    y_fwd(1, 3)
    phase("h_fwd3")
    h_fwd(3)
    phase("y_fwd1")
    y_fwd(1, 2)
    phase("y_own2")
    for r in ORDER:
        y_own(2, r)
    phase("h_last1")
    h_last(1)
    phase("w_end0")
    w_end(0)
    phase("t0_0")
    tasks(0, 1, 0, 1)
    phase("h_end1")
    h_end(1)
    phase("t0_1")
    lora_in(1)
    tasks(0, 1, 1, 1)
    phase("y_own3")
    for r in ORDER:
        y_own(3, r)
    phase("w_end1")
    w_end(1)
    phase("t1_01")
    tasks(1, 1, 0, 2)
    phase("h_fwd2")
    h_fwd(2)
    phase("y_fwd2")
    y_fwd(2, 0)
    y_fwd(2, 1)
    phase("h_last3")
    h_last(3)
    h_end(3)
    phase("t01_3")
    lora_in(3)
    tasks(0, 2, 2, 1)
    phase("y_fwd2b")
    y_fwd(2, 3)
    y_fwd(2, 2)
    y_fwd(3, 0)
    phase("h_last2")
    h_last(2)
    y_fwd(3, 1)
    h_end(2)
    phase("t01_2")
    lora_in(2)
    tasks(0, 2, 3, 1)
    sent(H.at[pl.ds(0, 3 * T), :], h_s)
    phase("y_fwd3")
    y_fwd(3, 3)
    y_fwd(3, 2)
    phase("w_near3")
    w_near(3)
    phase("t3a")
    each_block(functools.partial(early, NK - 1))
    phase("w_end2")
    w_end(2)
    phase("t2")
    tasks(2, 1, 0, 4)
    phase("w_far3")
    w_far(3)
    phase("t3b")
    each_block(functools.partial(task, NK - 1, rest=True))
    phase("stats_a")

    STA[v] = jnp.broadcast_to(jnp.ones((1, 1, 1), F32), (2, 16, 128))
    TA[v] = jnp.zeros((16, 128), F32)
    JR[...] = jnp.full((16, 128), -1.0, F32)
    for b in range(NB):
        t = COL[b * 128 : (b + 1) * 128, :].T
        m, e, g = t[8:12], t[12:16], t[16:20]
        top = jnp.max(m, axis=0, keepdims=True)
        STA[v, 0, b : b + 1, :] = top
        STA[v, 1, b : b + 1, :] = jnp.sum(e * jnp.exp(m - top), axis=0, keepdims=True)
        TA[v, b : b + 1, :] = jnp.sum(g, axis=0, keepdims=True)
        JR[b : b + 1, :] = t[1:2]
    turns = [(a, b) for a in (2, 1, 3, 0) for b in range(NC) if a or b]
    for a, b in turns:
        dev = {"z": zn(a), "c": lax.rem(c + b, NC)}
        send(STA.at[v], STA.at[v], sa_s, sa, dev)
    for a, b in turns:
        send(TA.at[v], TA.at[v], ta_s, ta, {"z": zn(a), "c": lax.rem(c + b, NC)})
    phase("counts")
    got(CN.at[0:3], cn)
    counts = jnp.sum(CN[0] + CN[1] + CN[2] + CN[3], axis=1, keepdims=True)
    counts = jnp.maximum(counts, 1.0)
    per_job = TOKENS / (JOBS * counts)
    jobs = JR[...]
    weight = jnp.zeros((16, 128), F32)
    for j in range(JOBS):
        weight = jnp.where(jobs == float(j), per_job[j : j + 1, :], weight)
    phase("stats_w")
    got(STA.at[0:7], sa)

    def joined(ref, n):
        top = functools.reduce(jnp.maximum, [ref[i, 0] for i in range(n)])
        return top, functools.reduce(jnp.add, [ref[i, 1] * jnp.exp(ref[i, 0] - top) for i in range(n)])

    STB[x, 0], STB[x, 1] = joined(STA, NZ * NC)
    phase("stats_b")
    for r in (2, 1, 3):
        send(STB.at[x], STB.at[x], sb_s, sb, {"x": xn(r)})
    for r in ORDER:
        lg_remote(NK - 1, r)
    lg_local(NK - 1)
    got(STB.at[0:3], sb)
    phase("finish")
    top, e = joined(STB, NX)
    scaled = weight / e
    blank = jnp.zeros((125, 128), F32)
    for b in range(NB):
        parts = [i[b : b + 1] for i in (top, scaled, weight)]
        COL2[b * 128 : (b + 1) * 128, :] = jnp.concatenate(parts + [blank], axis=0).T

    def targets():
        got(TA.at[0:7], ta)
        TB[x] = functools.reduce(jnp.add, [TA[i] for i in range(NZ * NC)])
        for r in (2, 1, 3):
            send(TB.at[x], TB.at[x], tb_s, tb, {"x": xn(r)})

    row_cw = lax.broadcasted_iota(jnp.int32, (1, CW), 1)

    def gradient(j):
        part = pl.ds(OFF[j], LEN[j])

        def step(m, carry):
            rows = pl.ds(al(m * T + OFF[j], 16), LEN[j])
            cols = COL[rows, :]
            lab = cols[:, 0:1]
            weight = COL2[rows, 2:3]
            factors = jnp.exp(cols - COL2[rows, 0:1]) * COL2[rows, 1:2]
            for k in range(NK):
                ids = (row_cw + (base + k * CW)).astype(F32)
                g = E[k, rows, :] * factors[:, 8 + k : 9 + k] - jnp.where(lab == ids, weight, 0.0)
                G5[m, part, k * CW : (k + 1) * CW] = g.astype(BF16)
            return carry

        lax.fori_loop(0, NX, step, 0, unroll=True)
        phase("lora%d" % j)
        rows = G5[:, OFF[j] : OFF[j] + LEN[j], 0:U].reshape(NX * LEN[j], U)
        lora = tdot(rows, AU[...]).reshape(NX, LEN[j], 128)
        for m in range(NX):
            job = COL[m * T + OFF[j] : m * T + OFF[j] + LEN[j], 1:2]
            one = jnp.where(job == rank_job[: LEN[j]], lora[m], 0.0)
            high = one.astype(BF16)
            G5[m, part, U : U + 128] = high
            G5[m, part, U + 128 : U + 256] = (one - high.astype(F32)).astype(BF16)

    def send_rows(i):
        part = pl.ds(OFF[2 * i], LEN[2 * i] + LEN[2 * i + 1])
        for r in ORDER:
            send(G5.at[xn(r), part, pl.ds(0, U)], gr.at[part, pl.ds(my_cols, U)], gr_s, grs, {"x": xn(r)})
        gr[part, pl.ds(my_cols, U)] = G5[x, part, 0:U]

    cs_r = take("r", 32)
    ring_r = take("r", 6 * NR)

    def zt(s, h):
        return lax.rem(z + NZ + (2 * h - 1) * (s + 1), NZ)

    def span(j):
        return pl.ds(NX * OFF[j], NX * LEN[j])

    def unit(s, h, j, core):
        at = al((zt(s, h) * NC + core) * SH + h * CW, CW)
        g = G5[:, OFF[j] : OFF[j] + LEN[j], :].reshape(NX * LEN[j], U + 256)
        return tdot(g, W5[pl.ds(at, CW), :])

    def ps(s, h, j, at=0):
        return H.at[span(j), pl.ds(al(at + (s * 2 + h) * CW, CW), CW)]

    def ps_copy(s, h, j):
        i = (s * 2 + h) * NQ + j
        return rcopy(ps(s, h, j), ps(s, h, j, D // 2), cs_s, cs_r + i, other)

    def ring_copy(s, h, j):
        i = (s * 2 + h) * NR + j
        return rcopy(
            RR.at[s, h, span(j)], RR.at[s + 1, h, span(j)], ring_s, ring_r + i,
            {"z": lax.rem(z + NZ + 1 - 2 * h, NZ)},
        )

    def for_core(s, j):
        def step(h, carry):
            ps(s, h, j)[...] = unit(s, h, j, 1 - c).astype(BF16)
            ps_copy(s, h, j).start()
            return carry

        lax.fori_loop(0, 2, step, 0)

    def mine(s, h, j):
        a = unit(s, h, j, c)
        ps_copy(s, h, j).wait_recv()
        return a + ps(s, h, j, D // 2)[...].astype(F32)

    def with_ring(s, h, j):
        a = mine(s, h, j)
        ring_copy(s - 1, h, j).wait_recv()
        return a + RR[s, h, span(j), :].astype(F32)

    def own(s, j, get):
        def step(h, carry):
            RR[s, h, span(j), :] = get(s, h, j).astype(BF16)
            ring_copy(s, h, j).start()
            return carry

        lax.fori_loop(0, 2, step, 0)

    def own_x(s):
        def step(h, carry):
            cols = pl.ds(al(zt(s, h) * SH + h * CW, CW), CW)
            XF[:, :, cols] = mine(s, h, NR).astype(BF16).reshape(NX, XT, CW)
            return carry

        lax.fori_loop(0, 2, step, 0)

    def x_first():
        for r in (2, 1, 3):
            send(XF.at[xn(r)], XFR.at[r - 1], xf_s, xf, {"x": xn(r)})

    def x_first_sum():
        phase("xf_sum")
        got(XFR, xf)
        total = XF[x].astype(F32)
        for r in (1, 3, 2):
            total = total + XFR[r - 1].astype(F32)
        XF[x] = total.astype(BF16)
        for r in (2, 1, 3):
            send(XF.at[x, :, pl.ds(al(zn(r) * SH, SH), SH)], ZR.at[r - 1], zr_s, zr, {"z": zn(r)})

    def losses_out():
        phase("losses")
        got(TB.at[0:3], tb)
        loss = top + jnp.log(e) - (TB[0] + TB[1] + TB[2] + TB[3])
        sums = [jnp.sum(jnp.where(jobs == float(j), loss, 0.0), axis=0, keepdims=True) for j in range(JOBS)]
        JL[y] = jnp.concatenate(sums, axis=0)
        for r in (1, 3, 2):
            send(JL.at[y], JL.at[y], jn_s, jn, {"y": yn(r)})
        for b in range(NB):
            row = jnp.concatenate([loss[b : b + 1], jnp.zeros((127, 128), F32)], axis=0)
            COL2[b * 128 : (b + 1) * 128, :] = row.T
        for q in range(3):
            n = min(128, T - q * 128)
            t = COL2[pl.ds(al(x * T + q * 128, 8), n), :]
            if n < 128:
                t = jnp.concatenate([t, jnp.zeros((128 - n, 128), F32)], axis=0)
            small[0:1, q * 128 : (q + 1) * 128] = t.T[0:1]

    def losses_in():
        phase("losses2")
        got(JL.at[0:3], jn)
        total = jnp.sum(JL[0] + JL[1] + JL[2] + JL[3], axis=1, keepdims=True) / counts
        total = jnp.concatenate([jnp.broadcast_to(total, (8, 128)), jnp.zeros((120, 128), F32)], axis=0)
        small[0:1, 384:512] = total.T[0:1]

    units = ("g0 c00 g1 r0", "o00 c01 g2 o01", "c02 g3 o02 c03", "c10 c13 o10 c11", "c23 o11 c12 c33")
    units = units + ("f0 o12 f1 f2", "f3 x t c20", "c21 o20 c22 o21", "c30 o22 c31")
    for op in " ".join(units).split():
        phase(op)
        n = [int(i) for i in op[1:]]
        if op[0] == "g":
            gradient(n[0])
        elif op[0] == "r":
            send_rows(n[0])
        elif op[0] == "c":
            for_core(*n)
        elif op[0] == "f":
            own_x(n[0])
        elif op[0] == "x":
            x_first()
        elif op[0] == "t":
            targets()
        else:
            own(*n, with_ring if n[0] else mine)

    xr = take("r", NR)
    ag = take("r", 3 * NQ)

    def hg_at(zz, j, h):
        cols = pl.ds(al(((NC * c + h) * NY + zz) * DB, DB), DB)
        return hg.at[pl.ds(OFF[j], LEN[j]), cols]

    def last(j):
        part = pl.ds(OFF[j], LEN[j])
        phase("last%d" % j)
        for h in range(2):
            a = with_ring(NZ - 1, h, j)
            XS[:, OFF[j] : OFF[j] + LEN[j], h * CW : (h + 1) * CW] = a.astype(BF16).reshape(NX, LEN[j], CW)
        for r in (2, 1, 3):
            send(XS.at[xn(r), part], XR.at[r - 1, part], x_s, xr + j, {"x": xn(r)})

    def x_sum(j):
        part = pl.ds(OFF[j], LEN[j])
        phase("xsum%d" % j)
        got(XR.at[:, part], xr + j)
        total = XS[x, part, :].astype(F32)
        for r in (1, 3, 2):
            total = total + XR[r - 1, part, :].astype(F32)
        FO[part, :] = total.astype(BF16)
        push(j)

    def z_sum():
        phase("zsum")
        got(ZR, zr)
        total = XF[x, :, pl.ds(al(z * SH, SH), SH)].astype(F32)
        for r in (1, 3, 2):
            total = total + ZR[r - 1].astype(F32)
        FO[RT:T, :] = total.astype(BF16)
        push(NR)

    def push(j):
        part = pl.ds(OFF[j], LEN[j])
        for h in range(2):
            src = FO.at[part, pl.ds(h * CW, CW)]
            for r in (1, 3):
                send(src, hg_at(z, j, h), ag_s, ag + j * 3 + r - 1, {"z": zn(r)})
            send(src, hg_at(z, j, h), cc_s, cc, other)
            hg_at(z, j, h)[...] = FO[part, h * CW : (h + 1) * CW]

    def pair_ref(j):
        return hg.at[pl.ds(OFF[j], LEN[j]), pl.ds(0, SH)]

    def relay(j):
        phase("relay%d" % j)
        for r in (1, 3):
            got(pair_ref(j), ag + j * 3 + r - 1)
            h = r // 2
            src = hg_at(lax.rem(z + NZ - r, NZ), j, h)
            send(src, src, ag_s, ag + j * 3 + 1, {"z": zn(r)})
            for h in range(2):
                src = hg_at(lax.rem(z + NZ - r, NZ), j, h)
                send(src, src, cc_s, cc, other)

    def gather(j):
        phase("gather%d" % j)
        got(pair_ref(j), ag + j * 3 + 1)
        for h in range(2):
            src = hg_at(zn(2), j, h)
            send(src, src, cc_s, cc, other)

    last(0)
    for_core(3, 2)
    x_first_sum()
    last(1)
    x_sum(0)
    last(2)
    send_rows(1)
    z_sum()
    x_sum(1)
    relay(0)
    x_sum(2)
    relay(3)
    losses_out()
    relay(1)
    gather(0)
    gather(3)
    losses_in()
    relay(2)
    gather(1)
    gather(2)

    phase("arrivals")
    got(lg.at[:, pl.ds(0, 3 * U)], lgs)
    got(gr.at[:, pl.ds(0, 3 * U)], grs)
    got(hg.at[:, pl.ds(0, NZ * SH)], cc)
    phase("drain")
    sent(W5.at[pl.ds(0, 60 * DB // NX), pl.ds(0, U)], ws_s)
    sent(AX.at[0:3], ax_s)
    sent(lg.at[:, pl.ds(0, 3 * U)], lg_s)
    sent(CN.at[0:3], cn_s)
    sent(STA.at[0:7], sa_s)
    sent(STB.at[0:3], sb_s)
    sent(gr.at[:, pl.ds(0, 3 * U)], gr_s)
    sent(H.at[:, pl.ds(0, D // 2)], cs_s)
    sent(RR.at[0:3], ring_s)
    sent(JL.at[0:3], jn_s)
    sent(XR, x_s)
    sent(XFR, xf_s)
    sent(ZR, zr_s)
    sent(hg.at[:, pl.ds(0, 3 * SH)], ag_s)
    sent(TA.at[0:7], ta_s)
    sent(TB.at[0:3], tb_s)
    sent(hg.at[:, pl.ds(0, NZ * SH)], cc_s)
    phase(None)
    assert used == {"s": NSEND, "r": NRECV, "l": NLOAD}, used


NSEND, NRECV, NLOAD = 18, 128, 5


def emit(lgv, grv, hgv, small, lg, gr, hg, tl, jl, sem):
    copies = []
    for src, dst in ((lgv, lg), (grv, gr), (hgv, hg)):
        for i in range(4):
            part = pl.ds(i * 88, 88)
            copies.append(pltpu.make_async_copy(src.at[part], dst.at[part], sem.at[len(copies)]))
    for d in copies:
        d.start()
    tl[...] = small[0, :T]
    jl[...] = small[0, 384 : 384 + JOBS]
    for d in copies:
        d.wait()


def vmem(*shape, dtype=BF16):
    return pltpu.VMEM(shape, dtype)


def shards(hidden, weight, down, up, labels, jobs):
    hbm = pl.BlockSpec(memory_space=pl.ANY)
    vm = pl.BlockSpec(memory_space=pltpu.VMEM)
    held = pl.pallas_call(
        kernel,
        out_shape=(vmem(T, V), vmem(T, V), vmem(T, D), vmem(1, 512, dtype=F32)),
        in_specs=[hbm] * 4 + [vm] * 2,
        out_specs=(vm, vm, vm, vm),
        scratch_shapes=[
            vmem(S, D),
            vmem(D, U + 256),
            vmem(DB, V),
            vmem(NK, S, CW, dtype=F32),
            vmem(S, U),
            vmem(NX, T, U + 256),
            vmem(NZ, 2, NX * RT, CW),
            vmem(NX, RT, SH),
            vmem(3, RT, SH),
            vmem(NX, XT, NZ * SH),
            vmem(3, XT, NZ * SH),
            vmem(3, XT, SH),
            vmem(T, SH),
            vmem(S, 128, dtype=F32),
            vmem(S, 128, dtype=F32),
            vmem(S, 128),
            vmem(128, U),
            vmem(NX, 3, 8, 128, dtype=F32),
            vmem(NZ * NC, 2, 16, 128, dtype=F32),
            vmem(NX, 2, 16, 128, dtype=F32),
            vmem(NZ * NC, 16, 128, dtype=F32),
            vmem(NX, 16, 128, dtype=F32),
            vmem(16, 128, dtype=F32),
            vmem(NY, 8, 128, dtype=F32),
            vmem(NY, 8, 128, dtype=F32),
            pltpu.SemaphoreType.DMA((NSEND,)),
            pltpu.SemaphoreType.DMA((NRECV,)),
            pltpu.SemaphoreType.DMA((NLOAD,)),
        ],
        compiler_params=pltpu.CompilerParams(
            collective_id=0, has_side_effects=True, vmem_limit_bytes=53 * 1024 * 1024
        ),
        name="step",
    )(hidden, weight, down, up, labels, jobs)
    return pl.pallas_call(
        emit,
        out_shape=(
            jax.ShapeDtypeStruct((T, V), BF16),
            jax.ShapeDtypeStruct((T, V), BF16),
            jax.ShapeDtypeStruct((T, D), BF16),
            jax.ShapeDtypeStruct((T,), F32),
            jax.ShapeDtypeStruct((JOBS,), F32),
        ),
        in_specs=[vm] * 4,
        out_specs=(hbm, hbm, hbm, vm, vm),
        scratch_shapes=[pltpu.SemaphoreType.DMA((12,))],
        compiler_params=pltpu.CompilerParams(vmem_limit_bytes=1024 * 1024),
        name="emit",
    )(*(pltpu.with_memory_space_constraint(i, pltpu.VMEM) for i in held))


def solution(mesh):
    split = Mesh(mesh.devices.reshape(NZ, NC, NX, NY), ("z", "c", "x", "y"))
    dp, vocab = ("x", "y"), ("z", "c")
    return jax.shard_map(
        shards,
        mesh=split,
        in_specs=(P(dp, None), P(dp, vocab), P(), P(None, vocab), P(dp), P(dp)),
        out_specs=(P(dp, vocab), P(dp, vocab), P(dp, None), P(dp), P()),
        check_vma=False,
    )
```

```python
import functools

import jax
import jax.numpy as jnp
from jax import lax
from jax.experimental import pallas as pl
from jax.experimental.pallas import tpu as pltpu
from jax.sharding import Mesh
from jax.sharding import PartitionSpec as P

MESH = pl.DeviceIdType.MESH
F32 = jnp.float32
BF16 = jnp.bfloat16

JOBS = 8
RANK = 16
NX = NY = NZ = 4
NC = 2
T = 352
S = NX * T
HT = T // 2
LEN = (112, 112, 48, 80)
OFF = (0, 112, 224, 272)
NQ = len(LEN)
NR = NQ - 1
RT = OFF[NR]
XT = LEN[NR]
D = 4096
DB = D // (NX * NY)
V = 4096
U = V // NX
CW = 256
NK = U // CW
SH = D // (NZ * NC)
TOKENS = S * NY
NB = S // 128


def fdot(a, b):
    return jnp.dot(a, b, preferred_element_type=F32)


def tdot(a, b):
    return lax.dot_general(a, b, (((1,), (1,)), ((), ())), preferred_element_type=F32)


def kernel(
    hid, w, ad, au, lab_in, job_in,
    lg, gr, hg, small,
    H, W5, WS, E, LT, G5, RR, XS, XR, XQ, XF, XFR, XP, ZR, FO, COL, COL2, LI, AU, AX, STA, STB, TA, TB, JR, CN, JL,
    ssem, rsem, lsem,
):
    z, c, x, y = (lax.axis_index(a) for a in ("z", "c", "x", "y"))
    v = z * NC + c

    def al(i, m):
        return pl.multiple_of(i, m)

    def xn(r):
        return lax.rem(x + r, NX)

    def yn(r):
        return lax.rem(y + r, NY)

    def zn(r):
        return lax.rem(z + r, NZ)

    used = {"s": 0, "r": 0, "l": 0}

    def take(kind, n=1):
        at = used[kind]
        used[kind] = at + n
        return at

    def rcopy(src, dst, si, ri, dev):
        return pltpu.make_async_remote_copy(
            src_ref=src, dst_ref=dst, send_sem=ssem.at[si], recv_sem=rsem.at[ri],
            device_id=dev, device_id_type=MESH,
        )

    def send(src, dst, si, ri, dev):
        rcopy(src, dst, si, ri, dev).start()

    def got(ref, ri):
        rcopy(ref, ref, 0, ri, {"x": xn(1)}).wait_recv()

    def sent(ref, si):
        rcopy(ref, ref, si, 0, {"x": xn(1)}).wait_send()

    def load(src, dst, li):
        pltpu.make_async_copy(src, dst, lsem.at[li]).start()

    def loaded(ref, li):
        pltpu.make_async_copy(ref, ref, lsem.at[li]).wait()

    scope = []

    def phase(name):
        if scope:
            scope.pop().__exit__(None, None, None)
        if name:
            scope.append(jax.named_scope(name))
            scope[0].__enter__()

    phase("entry")
    bar = pltpu.get_barrier_semaphore()
    peers = (
        [{"x": xn(r)} for r in (1, 2, 3)]
        + [{"y": yn(r)} for r in (1, 2, 3)]
        + [{"z": zn(a), "c": lax.rem(c + b, NC)} for a in range(NZ) for b in range(NC) if a or b]
    )
    for dev in peers:
        pl.semaphore_signal(bar, inc=1, device_id=dev, device_id_type=MESH)

    l_w, l_own, l_h, l_up, l_down = (take("l") for _ in range(5))
    load(w, WS, l_w)
    own_rows = pl.ds(al((y * NX + x) * DB, DB), DB)
    load(w.at[:, pl.ds(al(x * U, U), U)], W5.at[own_rows, pl.ds(0, U)], l_own)
    for p in range(NX * NY):
        n = (p % NX) * NY + p // NX
        load(hid.at[:, pl.ds(n * DB, DB)], H.at[pl.ds(al(x * T, 16), T), pl.ds(p * DB, DB)], l_h)
    load(au.at[:, pl.ds(al(x * U, U), U)], AU, l_up)
    for p in range(NX * NY):
        n = (p % NX) * NY + p // NX
        for q in range(2):
            load(
                ad.at[pl.ds(n * DB, DB), :],
                W5.at[pl.ds(p * DB, DB), pl.ds(U + q * 128, 128)],
                l_down,
            )
    for q in range(3):
        n = min(128, T - q * 128)
        AX[x, q] = jnp.full((8, 128), -1.0, F32)
        AX[x, q, 0:1, 0:n] = lab_in[pl.ds(q * 128, n)].astype(F32).reshape(1, n)
        AX[x, q, 1:2, 0:n] = job_in[pl.ds(q * 128, n)].astype(F32).reshape(1, n)
    pl.semaphore_wait(bar, len(peers))

    ORDER = (1, 3, 2)
    wx = take("r", NK * 3)
    hx = take("r", 3)
    ax, lgs, cn, sa, sb, ta, tb, grs, jn, cc, zr = (take("r") for _ in range(11))
    xf = take("r", 3)
    wy = take("r", NK * 6)
    hz = take("r", 3 * 3)
    hc = take("r", 3)
    ws_s, h_s, ax_s, lg_s, cn_s, sa_s, sb_s, ta_s, tb_s, gr_s, cs_s, ring_s, jn_s, x_s, xf_s, zr_s, ag_s, cc_s = (
        take("s") for _ in range(18)
    )

    def xp(r):
        return lax.rem(x + NX - r, NX)

    def wblock(row, k):
        return W5.at[row, pl.ds(k * CW, CW)]

    def send_w(k):
        for r in ORDER:
            send(
                WS.at[:, pl.ds(al(xn(r) * U + k * CW, CW), CW)],
                wblock(own_rows, k), ws_s, wx + k * 3 + r - 1, {"x": xn(r)},
            )

    def piece(dy, r, k):
        return wblock(pl.ds(al((yn(dy) * NX + xp(r)) * DB, DB), DB), k)

    def y_own(k, r):
        src = piece(0, r, k)
        if r:
            got(src, wx + k * 3 + r - 1)
        at = wy + k * 6
        send(src, src, ws_s, at + (r if r in (0, 2) else 4), {"y": yn(1)})
        send(src, src, ws_s, at + (4 if r in (0, 2) else r), {"y": yn(3)})

    def y_fwd(k, r):
        at = wy + k * 6
        src = piece(3 if r in (0, 2) else 1, r, k)
        got(src, at + r)
        send(src, src, ws_s, at + 5, {"y": yn(1 if r in (0, 2) else 3)})

    def w_near(k):
        got(wblock(pl.ds(0, 4 * DB), k), wy + k * 6 + 4)

    def w_far(k):
        got(wblock(pl.ds(0, 4 * DB), k), wy + k * 6 + 5)

    def w_end(k):
        w_near(k)
        w_far(k)

    other = {"c": 1 - c}

    def hpiece(xb, share, lo=0, n=T):
        return H.at[pl.ds(al(xb * T + lo, 16), n), pl.ds(al(share * SH, SH), SH)]

    def h_send(at, ri, dev):
        send(at, at, h_s, ri, dev)

    def h_in(r):
        mine = hpiece(xp(r), v)
        got(mine, hx + r - 1)
        b = hz + (r - 1) * 3
        h_send(mine, b + 0, {"z": zn(1)})
        h_send(mine, b + 1, {"z": zn(3)})
        h_send(mine, hc + r - 1, other)

    def h_fwd(r):
        xb = xp(r)
        b, d = hz + (r - 1) * 3, hc + r - 1
        left, right = zn(3) * NC + c, zn(1) * NC + c
        got(hpiece(xb, left), b + 0)
        h_send(hpiece(xb, left, 0, HT), b + 2, {"z": zn(1)})
        h_send(hpiece(xb, left), d, other)
        got(hpiece(xb, right), b + 1)
        h_send(hpiece(xb, right, HT, HT), b + 2, {"z": zn(3)})
        h_send(hpiece(xb, right), d, other)

    def h_last(r):
        far = hpiece(xp(r), zn(2) * NC + c)
        got(far, hz + (r - 1) * 3 + 2)
        h_send(far, hc + r - 1, other)

    def h_end(r):
        got(H.at[pl.ds(0, T), pl.ds(0, NZ * SH)], hc + r - 1)

    lane128 = lax.broadcasted_iota(jnp.int32, (T, 128), 1)
    rank_job = (lane128 // RANK).astype(F32)
    base = v * V + x * U
    lane_cw = lax.broadcasted_iota(jnp.int32, (T, CW), 1)
    my_cols = al(x * U, U)

    def lora_in(r):
        rows = pl.ds(al(xp(r) * T, 16), T)
        hit = COL[rows, 1:2] == rank_job
        a = fdot(H[rows, :], W5[:, U : U + 128])
        LI[rows, :] = jnp.where(hit, a, 0.0).astype(BF16)

    def lg_cols(k):
        return pl.ds(al(my_cols + k * CW, CW), CW)

    def lg_remote(k, r):
        src = LT.at[pl.ds(al(xp(r) * T, 16), T), pl.ds(al(k * CW, CW), CW)]
        send(src, lg.at[:, lg_cols(k)], lg_s, lgs, {"x": xp(r)})

    def lg_local(k):
        cols = pl.ds(al(k * CW, CW), CW)
        lg[:, lg_cols(k)] = LT[pl.ds(al(x * T, 16), T), cols]

    def part_of(rows, cols, dy):
        deep = pl.ds(al(yn(dy) * NX * DB, DB), NX * DB)
        return fdot(H[rows, deep], W5[deep, cols])

    def early(k, r):
        rows = pl.ds(al(xp(r) * T, 16), T)
        cols = pl.ds(al(k * CW, CW), CW)
        E[k, rows, :] = part_of(rows, cols, 0) + part_of(rows, cols, 1) + part_of(rows, cols, 3)

    def task(k, r, rest=False):
        rows = pl.ds(al(xp(r) * T, 16), T)
        cols = pl.ds(al(k * CW, CW), CW)
        if rest:
            a = E[k, rows, :] + part_of(rows, cols, 2)
        else:
            a = fdot(H[rows, :], W5[:, cols])
        a = a + fdot(LI[rows, :], AU[:, cols])
        LT[rows, cols] = a.astype(BF16)
        top = jnp.max(a, axis=1, keepdims=True)
        e = jnp.exp(a - top)
        E[k, rows, :] = e
        total = jnp.sum(e, axis=1, keepdims=True)
        ids = (lane_cw + (base + k * CW)).astype(F32)
        target = jnp.sum(jnp.where(ids == COL[rows, 0:1], a, 0.0), axis=1, keepdims=True)
        old = COL[rows, :]
        old = jnp.where(lane128 == 8 + k, top, old)
        old = jnp.where(lane128 == 12 + k, total, old)
        COL[rows, :] = jnp.where(lane128 == 16 + k, target, old)

    def turn(o):
        return jnp.where(o == 2, 3, jnp.where(o == 3, 2, o))

    def tasks(k0, nk, o0, no):
        def step(i, carry):
            k, o = k0 + i // no, o0 + lax.rem(i, no)
            r = turn(o)
            task(k, r)
            if o0:
                lg_remote(k, r)
            else:
                pl.when(r > 0)(lambda: lg_remote(k, r))
                pl.when(r == 0)(lambda: lg_local(k))
            return carry

        lax.fori_loop(0, nk * no, step, 0)

    def each_block(f):
        def step(o, carry):
            f(turn(o))
            return carry

        lax.fori_loop(0, NX, step, 0)

    loaded(WS, l_w)
    loaded(W5.at[own_rows, pl.ds(0, U)], l_own)
    send_w(0)
    for r in ORDER:
        send(AX.at[x], AX.at[x], ax_s, ax, {"x": xn(r)})
    for k in range(3):
        y_own(k, 0)
    loaded(H.at[pl.ds(0, T), :], l_h)

    def send_h(r):
        send(hpiece(x, v), hpiece(x, v), h_s, hx + r - 1, {"x": xn(r)})

    send_h(1)
    send_h(3)
    send_w(1)
    send_h(2)
    send_w(2)
    send_w(3)
    phase("p1a")
    y_fwd(0, 0)
    for r in ORDER:
        y_own(0, r)
    y_own(3, 0)
    phase("h_in13")
    h_in(1)
    h_in(3)
    phase("p1b")
    y_fwd(1, 0)
    y_fwd(0, 1)
    y_fwd(0, 3)
    for r in ORDER:
        y_own(1, r)
    y_fwd(0, 2)
    phase("cols")

    got(AX.at[0:3], ax)
    sub = lax.broadcasted_iota(jnp.int32, (8, 128), 0).astype(F32)
    counts = jnp.zeros((8, 128), F32)
    for xb in range(NX):
        for q in range(3):
            tile = AX[xb, q]
            n = min(128, T - q * 128)
            turned = jnp.concatenate([tile, jnp.zeros((120, 128), F32)], axis=0).T
            COL[pl.ds(xb * T + q * 128, n), :] = turned[:n]
            counts = counts + (tile[1:2, :] == sub).astype(F32)
    CN[y] = counts
    for r in (1, 3, 2):
        send(CN.at[y], CN.at[y], cn_s, cn, {"y": yn(r)})
    loaded(AU, l_up)
    loaded(W5.at[:, pl.ds(U, 256)], l_down)
    lora_in(0)
    phase("h_fwd1")
    h_fwd(1)
    phase("h_in2")
    h_in(2)
    phase("p1c")
    y_fwd(1, 1)
    y_fwd(1, 3)
    phase("h_fwd3")
    h_fwd(3)
    phase("y_fwd1")
    y_fwd(1, 2)
    phase("y_own2")
    for r in ORDER:
        y_own(2, r)
    phase("h_last1")
    h_last(1)
    phase("w_end0")
    w_end(0)
    phase("t0_0")
    tasks(0, 1, 0, 1)
    phase("h_end1")
    h_end(1)
    phase("t0_1")
    lora_in(1)
    tasks(0, 1, 1, 1)
    phase("y_own3")
    for r in ORDER:
        y_own(3, r)
    phase("w_end1")
    w_end(1)
    phase("t1_01")
    tasks(1, 1, 0, 2)
    phase("h_fwd2")
    h_fwd(2)
    phase("y_fwd2")
    y_fwd(2, 0)
    y_fwd(2, 1)
    phase("h_last3")
    h_last(3)
    h_end(3)
    phase("t01_3")
    lora_in(3)
    tasks(0, 2, 2, 1)
    phase("y_fwd2b")
    y_fwd(2, 3)
    y_fwd(2, 2)
    y_fwd(3, 0)
    phase("h_last2")
    h_last(2)
    y_fwd(3, 1)
    h_end(2)
    phase("t01_2")
    lora_in(2)
    tasks(0, 2, 3, 1)
    sent(H.at[pl.ds(0, 3 * T), :], h_s)
    phase("y_fwd3")
    y_fwd(3, 3)
    y_fwd(3, 2)
    phase("w_near3")
    w_near(3)
    phase("t3a")
    each_block(functools.partial(early, NK - 1))
    phase("w_end2")
    w_end(2)
    phase("t2")
    tasks(2, 1, 0, 4)
    phase("w_far3")
    w_far(3)
    phase("t3b")
    each_block(functools.partial(task, NK - 1, rest=True))
    phase("stats_a")

    STA[v] = jnp.broadcast_to(jnp.ones((1, 1, 1), F32), (2, 16, 128))
    TA[v] = jnp.zeros((16, 128), F32)
    JR[...] = jnp.full((16, 128), -1.0, F32)
    for b in range(NB):
        t = COL[b * 128 : (b + 1) * 128, :].T
        m, e, g = t[8:12], t[12:16], t[16:20]
        top = jnp.max(m, axis=0, keepdims=True)
        STA[v, 0, b : b + 1, :] = top
        STA[v, 1, b : b + 1, :] = jnp.sum(e * jnp.exp(m - top), axis=0, keepdims=True)
        TA[v, b : b + 1, :] = jnp.sum(g, axis=0, keepdims=True)
        JR[b : b + 1, :] = t[1:2]
    turns = [(a, b) for a in (2, 1, 3, 0) for b in range(NC) if a or b]
    for a, b in turns:
        dev = {"z": zn(a), "c": lax.rem(c + b, NC)}
        send(STA.at[v], STA.at[v], sa_s, sa, dev)
    for a, b in turns:
        send(TA.at[v], TA.at[v], ta_s, ta, {"z": zn(a), "c": lax.rem(c + b, NC)})
    phase("counts")
    got(CN.at[0:3], cn)
    counts = jnp.sum(CN[0] + CN[1] + CN[2] + CN[3], axis=1, keepdims=True)
    counts = jnp.maximum(counts, 1.0)
    per_job = TOKENS / (JOBS * counts)
    jobs = JR[...]
    weight = jnp.zeros((16, 128), F32)
    for j in range(JOBS):
        weight = jnp.where(jobs == float(j), per_job[j : j + 1, :], weight)
    phase("stats_w")
    got(STA.at[0:7], sa)

    def joined(ref, n):
        top = functools.reduce(jnp.maximum, [ref[i, 0] for i in range(n)])
        return top, functools.reduce(jnp.add, [ref[i, 1] * jnp.exp(ref[i, 0] - top) for i in range(n)])

    STB[x, 0], STB[x, 1] = joined(STA, NZ * NC)
    phase("stats_b")
    for r in (2, 1, 3):
        send(STB.at[x], STB.at[x], sb_s, sb, {"x": xn(r)})
    for r in ORDER:
        lg_remote(NK - 1, r)
    lg_local(NK - 1)
    got(STB.at[0:3], sb)
    phase("finish")
    top, e = joined(STB, NX)
    scaled = weight / e
    blank = jnp.zeros((125, 128), F32)
    for b in range(NB):
        parts = [i[b : b + 1] for i in (top, scaled, weight)]
        COL2[b * 128 : (b + 1) * 128, :] = jnp.concatenate(parts + [blank], axis=0).T

    def targets():
        got(TA.at[0:7], ta)
        TB[x] = functools.reduce(jnp.add, [TA[i] for i in range(NZ * NC)])
        for r in (2, 1, 3):
            send(TB.at[x], TB.at[x], tb_s, tb, {"x": xn(r)})

    row_cw = lax.broadcasted_iota(jnp.int32, (1, CW), 1)

    def gradient(j):
        part = pl.ds(OFF[j], LEN[j])

        def step(m, carry):
            rows = pl.ds(al(m * T + OFF[j], 16), LEN[j])
            cols = COL[rows, :]
            lab = cols[:, 0:1]
            weight = COL2[rows, 2:3]
            factors = jnp.exp(cols - COL2[rows, 0:1]) * COL2[rows, 1:2]
            for k in range(NK):
                ids = (row_cw + (base + k * CW)).astype(F32)
                g = E[k, rows, :] * factors[:, 8 + k : 9 + k] - jnp.where(lab == ids, weight, 0.0)
                G5[m, part, k * CW : (k + 1) * CW] = g.astype(BF16)
            return carry

        lax.fori_loop(0, NX, step, 0, unroll=True)
        phase("lora%d" % j)
        rows = G5[:, OFF[j] : OFF[j] + LEN[j], 0:U].reshape(NX * LEN[j], U)
        lora = tdot(rows, AU[...]).reshape(NX, LEN[j], 128)
        for m in range(NX):
            job = COL[m * T + OFF[j] : m * T + OFF[j] + LEN[j], 1:2]
            one = jnp.where(job == rank_job[: LEN[j]], lora[m], 0.0)
            high = one.astype(BF16)
            G5[m, part, U : U + 128] = high
            G5[m, part, U + 128 : U + 256] = (one - high.astype(F32)).astype(BF16)

    def send_rows(i):
        part = pl.ds(OFF[2 * i], LEN[2 * i] + LEN[2 * i + 1])
        for r in ORDER:
            send(G5.at[xn(r), part, pl.ds(0, U)], gr.at[part, pl.ds(my_cols, U)], gr_s, grs, {"x": xn(r)})
        gr[part, pl.ds(my_cols, U)] = G5[x, part, 0:U]

    cs_r = take("r", 32)
    ring_r = take("r", 6 * NR)

    def zt(s, h):
        return lax.rem(z + NZ + (2 * h - 1) * (s + 1), NZ)

    def span(j):
        return pl.ds(NX * OFF[j], NX * LEN[j])

    def unit(s, h, j, core):
        at = al((zt(s, h) * NC + core) * SH + h * CW, CW)
        g = G5[:, OFF[j] : OFF[j] + LEN[j], :].reshape(NX * LEN[j], U + 256)
        return tdot(g, W5[pl.ds(at, CW), :])

    def ps(s, h, j, at=0):
        return H.at[span(j), pl.ds(al(at + (s * 2 + h) * CW, CW), CW)]

    def ps_copy(s, h, j):
        i = (s * 2 + h) * NQ + j
        return rcopy(ps(s, h, j), ps(s, h, j, D // 2), cs_s, cs_r + i, other)

    def ring_copy(s, h, j):
        i = (s * 2 + h) * NR + j
        return rcopy(
            RR.at[s, h, span(j)], RR.at[s + 1, h, span(j)], ring_s, ring_r + i,
            {"z": lax.rem(z + NZ + 1 - 2 * h, NZ)},
        )

    def for_core(s, j):
        def step(h, carry):
            ps(s, h, j)[...] = unit(s, h, j, 1 - c).astype(BF16)
            ps_copy(s, h, j).start()
            return carry

        lax.fori_loop(0, 2, step, 0)

    def mine(s, h, j):
        a = unit(s, h, j, c)
        ps_copy(s, h, j).wait_recv()
        return a + ps(s, h, j, D // 2)[...].astype(F32)

    def with_ring(s, h, j):
        a = mine(s, h, j)
        ring_copy(s - 1, h, j).wait_recv()
        return a + RR[s, h, span(j), :].astype(F32)

    def own(s, j, get):
        def step(h, carry):
            RR[s, h, span(j), :] = get(s, h, j).astype(BF16)
            ring_copy(s, h, j).start()
            return carry

        lax.fori_loop(0, 2, step, 0)

    def own_x(s):
        def step(h, carry):
            cols = pl.ds(al(zt(s, h) * SH + h * CW, CW), CW)
            XF[:, :, cols] = mine(s, h, NR).astype(BF16).reshape(NX, XT, CW)
            return carry

        lax.fori_loop(0, 2, step, 0)

    XH = NZ * SH // 2

    def xcols(i):
        return pl.ds(i * XH, XH)

    def x_first():
        far = XF.at[xn(2)]
        send(far.at[:, xcols(0)], XP.at[0], xf_s, xf, {"x": xn(1)})
        send(far.at[:, xcols(1)], XP.at[1], xf_s, xf + 1, {"x": xn(3)})
        send(XF.at[xn(1), :, xcols(1)], XFR.at[0, :, xcols(1)], xf_s, xf + 2, {"x": xn(1)})
        send(XF.at[xn(3), :, xcols(0)], XFR.at[1, :, xcols(0)], xf_s, xf + 2, {"x": xn(3)})

    def x_first_mid():
        for i, r in ((0, 1), (1, 3)):
            got(XP.at[i], xf + i)
            cols = slice(i * XH, (i + 1) * XH)
            both = XF[xn(r), :, cols].astype(F32) + XP[i].astype(F32)
            XF[xn(r), :, cols] = both.astype(BF16)
            send(XF.at[xn(r), :, xcols(i)], XFR.at[i, :, xcols(i)], xf_s, xf + 2, {"x": xn(r)})

    def x_first_sum():
        phase("xf_sum")
        got(XFR, xf + 2)
        total = XF[x].astype(F32) + XFR[0].astype(F32) + XFR[1].astype(F32)
        XF[x] = total.astype(BF16)
        for r in (2, 1, 3):
            send(XF.at[x, :, pl.ds(al(zn(r) * SH, SH), SH)], ZR.at[r - 1], zr_s, zr, {"z": zn(r)})

    def losses_out():
        phase("losses")
        got(TB.at[0:3], tb)
        loss = top + jnp.log(e) - (TB[0] + TB[1] + TB[2] + TB[3])
        sums = [jnp.sum(jnp.where(jobs == float(j), loss, 0.0), axis=0, keepdims=True) for j in range(JOBS)]
        JL[y] = jnp.concatenate(sums, axis=0)
        for r in (1, 3, 2):
            send(JL.at[y], JL.at[y], jn_s, jn, {"y": yn(r)})
        for b in range(NB):
            row = jnp.concatenate([loss[b : b + 1], jnp.zeros((127, 128), F32)], axis=0)
            COL2[b * 128 : (b + 1) * 128, :] = row.T
        for q in range(3):
            n = min(128, T - q * 128)
            t = COL2[pl.ds(al(x * T + q * 128, 8), n), :]
            if n < 128:
                t = jnp.concatenate([t, jnp.zeros((128 - n, 128), F32)], axis=0)
            small[0:1, q * 128 : (q + 1) * 128] = t.T[0:1]

    def losses_in():
        phase("losses2")
        got(JL.at[0:3], jn)
        total = jnp.sum(JL[0] + JL[1] + JL[2] + JL[3], axis=1, keepdims=True) / counts
        total = jnp.concatenate([jnp.broadcast_to(total, (8, 128)), jnp.zeros((120, 128), F32)], axis=0)
        small[0:1, 384:512] = total.T[0:1]

    units = ("g0 c00 g1 r0", "o00 c01 g2 o01", "c02 g3 o02 c03", "c10 c13 o10 c11", "c23 o11 c12 c33")
    units = units + ("f0 o12 f1 f2", "f3 x t c20", "c21 o20 c22 o21", "m c30 o22 c31")
    for op in " ".join(units).split():
        phase(op)
        n = [int(i) for i in op[1:]]
        if op[0] == "g":
            gradient(n[0])
        elif op[0] == "r":
            send_rows(n[0])
        elif op[0] == "c":
            for_core(*n)
        elif op[0] == "f":
            own_x(n[0])
        elif op[0] == "x":
            x_first()
        elif op[0] == "m":
            x_first_mid()
        elif op[0] == "t":
            targets()
        else:
            own(*n, with_ring if n[0] else mine)

    xr = take("r", 3 * NR)
    ag = take("r", 3 * NQ)

    def hg_at(zz, j, h):
        cols = pl.ds(al(((NC * c + h) * NY + zz) * DB, DB), DB)
        return hg.at[pl.ds(OFF[j], LEN[j]), cols]

    def last(j):
        part = pl.ds(OFF[j], LEN[j])
        phase("last%d" % j)
        for h in range(2):
            a = with_ring(NZ - 1, h, j)
            XS[:, OFF[j] : OFF[j] + LEN[j], h * CW : (h + 1) * CW] = a.astype(BF16).reshape(NX, LEN[j], CW)
        far = XS.at[xn(2), part]
        at = xr + j * 3
        send(far.at[:, pl.ds(0, CW)], XQ.at[0, part], x_s, at, {"x": xn(1)})
        send(far.at[:, pl.ds(CW, CW)], XQ.at[1, part], x_s, at + 1, {"x": xn(3)})
        send(XS.at[xn(1), part, pl.ds(CW, CW)], XR.at[0, part, pl.ds(CW, CW)], x_s, at + 2, {"x": xn(1)})
        send(XS.at[xn(3), part, pl.ds(0, CW)], XR.at[1, part, pl.ds(0, CW)], x_s, at + 2, {"x": xn(3)})

    def x_mid(j):
        part = pl.ds(OFF[j], LEN[j])
        phase("xmid%d" % j)
        at = xr + j * 3
        for i, r in ((0, 1), (1, 3)):
            got(XQ.at[i, part], at + i)
            cols = pl.ds(i * CW, CW)
            both = XS[xn(r), part, cols].astype(F32) + XQ[i, part, :].astype(F32)
            XS[xn(r), part, cols] = both.astype(BF16)
            send(XS.at[xn(r), part, cols], XR.at[i, part, cols], x_s, at + 2, {"x": xn(r)})

    def x_sum(j):
        part = pl.ds(OFF[j], LEN[j])
        phase("xsum%d" % j)
        got(XR.at[:, part], xr + j * 3 + 2)
        total = XS[x, part, :].astype(F32) + XR[0, part, :].astype(F32) + XR[1, part, :].astype(F32)
        FO[part, :] = total.astype(BF16)
        push(j)

    def z_sum():
        phase("zsum")
        got(ZR, zr)
        total = XF[x, :, pl.ds(al(z * SH, SH), SH)].astype(F32)
        for r in (1, 3, 2):
            total = total + ZR[r - 1].astype(F32)
        FO[RT:T, :] = total.astype(BF16)
        push(NR)

    def push(j):
        part = pl.ds(OFF[j], LEN[j])
        for h in range(2):
            src = FO.at[part, pl.ds(h * CW, CW)]
            for r in (1, 3):
                send(src, hg_at(z, j, h), ag_s, ag + j * 3 + r - 1, {"z": zn(r)})
            send(src, hg_at(z, j, h), cc_s, cc, other)
            hg_at(z, j, h)[...] = FO[part, h * CW : (h + 1) * CW]

    def pair_ref(j):
        return hg.at[pl.ds(OFF[j], LEN[j]), pl.ds(0, SH)]

    def relay(j):
        phase("relay%d" % j)
        for r in (1, 3):
            got(pair_ref(j), ag + j * 3 + r - 1)
            h = r // 2
            src = hg_at(lax.rem(z + NZ - r, NZ), j, h)
            send(src, src, ag_s, ag + j * 3 + 1, {"z": zn(r)})
            for h in range(2):
                src = hg_at(lax.rem(z + NZ - r, NZ), j, h)
                send(src, src, cc_s, cc, other)

    def gather(j):
        phase("gather%d" % j)
        got(pair_ref(j), ag + j * 3 + 1)
        for h in range(2):
            src = hg_at(zn(2), j, h)
            send(src, src, cc_s, cc, other)

    last(0)
    for_core(3, 2)
    x_mid(0)
    x_first_sum()
    last(1)
    x_sum(0)
    last(2)
    x_mid(1)
    x_mid(2)
    send_rows(1)
    z_sum()
    x_sum(1)
    relay(0)
    x_sum(2)
    relay(3)
    relay(1)
    gather(0)
    relay(2)
    gather(3)
    losses_out()
    gather(1)
    gather(2)
    losses_in()

    phase("arrivals")
    got(lg.at[:, pl.ds(0, 3 * U)], lgs)
    phase("arr_gr")
    got(gr.at[:, pl.ds(0, 3 * U)], grs)
    phase("arr_hg")
    got(hg.at[:, pl.ds(0, NZ * SH)], cc)
    phase("drain")
    sent(W5.at[pl.ds(0, 60 * DB // NX), pl.ds(0, U)], ws_s)
    sent(AX.at[0:3], ax_s)
    sent(lg.at[:, pl.ds(0, 3 * U)], lg_s)
    sent(CN.at[0:3], cn_s)
    sent(STA.at[0:7], sa_s)
    sent(STB.at[0:3], sb_s)
    sent(gr.at[:, pl.ds(0, 3 * U)], gr_s)
    sent(H.at[:, pl.ds(0, D // 2)], cs_s)
    sent(RR.at[0:3], ring_s)
    sent(JL.at[0:3], jn_s)
    sent(XS.at[0:3], x_s)
    sent(XF.at[0:3], xf_s)
    sent(ZR, zr_s)
    sent(hg.at[:, pl.ds(0, 3 * SH)], ag_s)
    sent(TA.at[0:7], ta_s)
    sent(TB.at[0:3], tb_s)
    sent(hg.at[:, pl.ds(0, NZ * SH)], cc_s)
    phase(None)
    assert used == {"s": NSEND, "r": NRECV, "l": NLOAD}, used


NSEND, NRECV, NLOAD = 18, 136, 5


def emit(lgv, grv, hgv, small, lg, gr, hg, tl, jl, sem):
    copies = []
    for src, dst in ((lgv, lg), (grv, gr), (hgv, hg)):
        for i in range(4):
            part = pl.ds(i * 88, 88)
            copies.append(pltpu.make_async_copy(src.at[part], dst.at[part], sem.at[len(copies)]))
    for d in copies:
        d.start()
    tl[...] = small[0, :T]
    jl[...] = small[0, 384 : 384 + JOBS]
    for d in copies:
        d.wait()


def vmem(*shape, dtype=BF16):
    return pltpu.VMEM(shape, dtype)


def shards(hidden, weight, down, up, labels, jobs):
    hbm = pl.BlockSpec(memory_space=pl.ANY)
    vm = pl.BlockSpec(memory_space=pltpu.VMEM)
    held = pl.pallas_call(
        kernel,
        out_shape=(vmem(T, V), vmem(T, V), vmem(T, D), vmem(1, 512, dtype=F32)),
        in_specs=[hbm] * 4 + [vm] * 2,
        out_specs=(vm, vm, vm, vm),
        scratch_shapes=[
            vmem(S, D),
            vmem(D, U + 256),
            vmem(DB, V),
            vmem(NK, S, CW, dtype=F32),
            vmem(S, U),
            vmem(NX, T, U + 256),
            vmem(NZ, 2, NX * RT, CW),
            vmem(NX, RT, SH),
            vmem(2, RT, SH),
            vmem(2, RT, CW),
            vmem(NX, XT, NZ * SH),
            vmem(2, XT, NZ * SH),
            vmem(2, XT, NZ * SH // 2),
            vmem(3, XT, SH),
            vmem(T, SH),
            vmem(S, 128, dtype=F32),
            vmem(S, 128, dtype=F32),
            vmem(S, 128),
            vmem(128, U),
            vmem(NX, 3, 8, 128, dtype=F32),
            vmem(NZ * NC, 2, 16, 128, dtype=F32),
            vmem(NX, 2, 16, 128, dtype=F32),
            vmem(NZ * NC, 16, 128, dtype=F32),
            vmem(NX, 16, 128, dtype=F32),
            vmem(16, 128, dtype=F32),
            vmem(NY, 8, 128, dtype=F32),
            vmem(NY, 8, 128, dtype=F32),
            pltpu.SemaphoreType.DMA((NSEND,)),
            pltpu.SemaphoreType.DMA((NRECV,)),
            pltpu.SemaphoreType.DMA((NLOAD,)),
        ],
        compiler_params=pltpu.CompilerParams(
            collective_id=0, has_side_effects=True, vmem_limit_bytes=53 * 1024 * 1024
        ),
        name="step",
    )(hidden, weight, down, up, labels, jobs)
    return pl.pallas_call(
        emit,
        out_shape=(
            jax.ShapeDtypeStruct((T, V), BF16),
            jax.ShapeDtypeStruct((T, V), BF16),
            jax.ShapeDtypeStruct((T, D), BF16),
            jax.ShapeDtypeStruct((T,), F32),
            jax.ShapeDtypeStruct((JOBS,), F32),
        ),
        in_specs=[vm] * 4,
        out_specs=(hbm, hbm, hbm, vm, vm),
        scratch_shapes=[pltpu.SemaphoreType.DMA((12,))],
        compiler_params=pltpu.CompilerParams(vmem_limit_bytes=1024 * 1024),
        name="emit",
    )(*(pltpu.with_memory_space_constraint(i, pltpu.VMEM) for i in held))


def solution(mesh):
    split = Mesh(mesh.devices.reshape(NZ, NC, NX, NY), ("z", "c", "x", "y"))
    dp, vocab = ("x", "y"), ("z", "c")
    return jax.shard_map(
        shards,
        mesh=split,
        in_specs=(P(dp, None), P(dp, vocab), P(), P(None, vocab), P(dp), P(dp)),
        out_specs=(P(dp, vocab), P(dp, vocab), P(dp, None), P(dp), P()),
        check_vma=False,
    )
```

```python
import functools

import jax
import jax.numpy as jnp
from jax import lax
from jax.experimental import pallas as pl
from jax.experimental.pallas import tpu as pltpu
from jax.sharding import Mesh
from jax.sharding import PartitionSpec as P

MESH = pl.DeviceIdType.MESH
F32 = jnp.float32
BF16 = jnp.bfloat16

JOBS = 8
RANK = 16
NX = NY = NZ = 4
NC = 2
T = 352
S = NX * T
HT = T // 2
LEN = (112, 112, 48, 80)
OFF = (0, 112, 224, 272)
NQ = len(LEN)
NR = NQ - 1
RT = OFF[NR]
XT = LEN[NR]
D = 4096
DB = D // (NX * NY)
V = 4096
U = V // NX
CW = 256
NK = U // CW
SH = D // (NZ * NC)
TOKENS = S * NY
NB = S // 128


def fdot(a, b):
    return jnp.dot(a, b, preferred_element_type=F32)


def tdot(a, b):
    return lax.dot_general(a, b, (((1,), (1,)), ((), ())), preferred_element_type=F32)


def kernel(
    hid, w, ad, au, lab_in, job_in,
    lg, gr, hg, small,
    H, W5, WS, E, LT, G5, RR, XS, XR, XQ, XF, XFR, XP, ZR, FO, COL, COL2, LI, AU, AX, STA, STB, TA, TB, JR, CN, JL,
    ssem, rsem, lsem,
):
    z, c, x, y = (lax.axis_index(a) for a in ("z", "c", "x", "y"))
    v = z * NC + c

    def al(i, m):
        return pl.multiple_of(i, m)

    def xn(r):
        return lax.rem(x + r, NX)

    def yn(r):
        return lax.rem(y + r, NY)

    def zn(r):
        return lax.rem(z + r, NZ)

    used = {"s": 0, "r": 0, "l": 0}

    def take(kind, n=1):
        at = used[kind]
        used[kind] = at + n
        return at

    def rcopy(src, dst, si, ri, dev):
        return pltpu.make_async_remote_copy(
            src_ref=src, dst_ref=dst, send_sem=ssem.at[si], recv_sem=rsem.at[ri],
            device_id=dev, device_id_type=MESH,
        )

    def send(src, dst, si, ri, dev):
        rcopy(src, dst, si, ri, dev).start()

    def got(ref, ri):
        rcopy(ref, ref, 0, ri, {"x": xn(1)}).wait_recv()

    def sent(ref, si):
        rcopy(ref, ref, si, 0, {"x": xn(1)}).wait_send()

    def load(src, dst, li):
        pltpu.make_async_copy(src, dst, lsem.at[li]).start()

    def loaded(ref, li):
        pltpu.make_async_copy(ref, ref, lsem.at[li]).wait()

    scope = []

    def phase(name):
        if scope:
            scope.pop().__exit__(None, None, None)
        if name:
            scope.append(jax.named_scope(name))
            scope[0].__enter__()

    phase("entry")
    bar = pltpu.get_barrier_semaphore()
    peers = (
        [{"x": xn(r)} for r in (1, 2, 3)]
        + [{"y": yn(r)} for r in (1, 2, 3)]
        + [{"z": zn(a), "c": lax.rem(c + b, NC)} for a in range(NZ) for b in range(NC) if a or b]
    )
    for dev in peers:
        pl.semaphore_signal(bar, inc=1, device_id=dev, device_id_type=MESH)

    l_w, l_own, l_h, l_up, l_down = (take("l") for _ in range(5))
    load(w, WS, l_w)
    own_rows = pl.ds(al((y * NX + x) * DB, DB), DB)
    load(w.at[:, pl.ds(al(x * U, U), U)], W5.at[own_rows, pl.ds(0, U)], l_own)
    for p in range(NX * NY):
        n = (p % NX) * NY + p // NX
        load(hid.at[:, pl.ds(n * DB, DB)], H.at[pl.ds(al(x * T, 16), T), pl.ds(p * DB, DB)], l_h)
    load(au.at[:, pl.ds(al(x * U, U), U)], AU, l_up)
    for p in range(NX * NY):
        n = (p % NX) * NY + p // NX
        for q in range(2):
            load(
                ad.at[pl.ds(n * DB, DB), :],
                W5.at[pl.ds(p * DB, DB), pl.ds(U + q * 128, 128)],
                l_down,
            )
    for q in range(3):
        n = min(128, T - q * 128)
        AX[x, q] = jnp.full((8, 128), -1.0, F32)
        AX[x, q, 0:1, 0:n] = lab_in[pl.ds(q * 128, n)].astype(F32).reshape(1, n)
        AX[x, q, 1:2, 0:n] = job_in[pl.ds(q * 128, n)].astype(F32).reshape(1, n)
    pl.semaphore_wait(bar, len(peers))

    ORDER = (1, 3, 2)
    wx = take("r", NK * 3)
    hx = take("r", 3)
    ax, lgs, cn, sa, sb, ta, tb, grs, jn, cc, zr = (take("r") for _ in range(11))
    xf = take("r", 3)
    wy = take("r", NK * 6)
    hz = take("r", 3 * 3)
    hc = take("r", 3)
    ws_s, h_s, ax_s, lg_s, cn_s, sa_s, sb_s, ta_s, tb_s, gr_s, cs_s, ring_s, jn_s, x_s, xf_s, zr_s, ag_s, cc_s = (
        take("s") for _ in range(18)
    )

    def xp(r):
        return lax.rem(x + NX - r, NX)

    def wblock(row, k):
        return W5.at[row, pl.ds(k * CW, CW)]

    def send_w(k):
        for r in ORDER:
            send(
                WS.at[:, pl.ds(al(xn(r) * U + k * CW, CW), CW)],
                wblock(own_rows, k), ws_s, wx + k * 3 + r - 1, {"x": xn(r)},
            )

    def piece(dy, r, k):
        return wblock(pl.ds(al((yn(dy) * NX + xp(r)) * DB, DB), DB), k)

    def y_own(k, r):
        src = piece(0, r, k)
        if r:
            got(src, wx + k * 3 + r - 1)
        at = wy + k * 6
        send(src, src, ws_s, at + (r if r in (0, 2) else 4), {"y": yn(1)})
        send(src, src, ws_s, at + (4 if r in (0, 2) else r), {"y": yn(3)})

    def y_fwd(k, r):
        at = wy + k * 6
        src = piece(3 if r in (0, 2) else 1, r, k)
        got(src, at + r)
        send(src, src, ws_s, at + 5, {"y": yn(1 if r in (0, 2) else 3)})

    def w_near(k):
        got(wblock(pl.ds(0, 4 * DB), k), wy + k * 6 + 4)

    def w_far(k):
        got(wblock(pl.ds(0, 4 * DB), k), wy + k * 6 + 5)

    def w_end(k):
        w_near(k)
        w_far(k)

    other = {"c": 1 - c}

    def hpiece(xb, share, lo=0, n=T):
        return H.at[pl.ds(al(xb * T + lo, 16), n), pl.ds(al(share * SH, SH), SH)]

    def h_send(at, ri, dev):
        send(at, at, h_s, ri, dev)

    def h_in(r):
        mine = hpiece(xp(r), v)
        got(mine, hx + r - 1)
        b = hz + (r - 1) * 3
        h_send(mine, b + 0, {"z": zn(1)})
        h_send(mine, b + 1, {"z": zn(3)})
        h_send(mine, hc + r - 1, other)

    def h_fwd(r):
        xb = xp(r)
        b, d = hz + (r - 1) * 3, hc + r - 1
        left, right = zn(3) * NC + c, zn(1) * NC + c
        got(hpiece(xb, left), b + 0)
        h_send(hpiece(xb, left, 0, HT), b + 2, {"z": zn(1)})
        h_send(hpiece(xb, left), d, other)
        got(hpiece(xb, right), b + 1)
        h_send(hpiece(xb, right, HT, HT), b + 2, {"z": zn(3)})
        h_send(hpiece(xb, right), d, other)

    def h_last(r):
        far = hpiece(xp(r), zn(2) * NC + c)
        got(far, hz + (r - 1) * 3 + 2)
        h_send(far, hc + r - 1, other)

    def h_end(r):
        got(H.at[pl.ds(0, T), pl.ds(0, NZ * SH)], hc + r - 1)

    lane128 = lax.broadcasted_iota(jnp.int32, (T, 128), 1)
    rank_job = (lane128 // RANK).astype(F32)
    base = v * V + x * U
    lane_cw = lax.broadcasted_iota(jnp.int32, (T, CW), 1)
    my_cols = al(x * U, U)

    def lora_in(r):
        rows = pl.ds(al(xp(r) * T, 16), T)
        hit = COL[rows, 1:2] == rank_job
        a = fdot(H[rows, :], W5[:, U : U + 128])
        LI[rows, :] = jnp.where(hit, a, 0.0).astype(BF16)

    def lg_cols(k):
        return pl.ds(al(my_cols + k * CW, CW), CW)

    def lg_remote(k, r):
        src = LT.at[pl.ds(al(xp(r) * T, 16), T), pl.ds(al(k * CW, CW), CW)]
        send(src, lg.at[:, lg_cols(k)], lg_s, lgs, {"x": xp(r)})

    def lg_local(k):
        cols = pl.ds(al(k * CW, CW), CW)
        lg[:, lg_cols(k)] = LT[pl.ds(al(x * T, 16), T), cols]

    def part_of(rows, cols, dy):
        deep = pl.ds(al(yn(dy) * NX * DB, DB), NX * DB)
        return fdot(H[rows, deep], W5[deep, cols])

    def early(k, r):
        rows = pl.ds(al(xp(r) * T, 16), T)
        cols = pl.ds(al(k * CW, CW), CW)
        E[k, rows, :] = part_of(rows, cols, 0) + part_of(rows, cols, 1) + part_of(rows, cols, 3)

    def task(k, r, rest=False):
        rows = pl.ds(al(xp(r) * T, 16), T)
        cols = pl.ds(al(k * CW, CW), CW)
        if rest:
            a = E[k, rows, :] + part_of(rows, cols, 2)
        else:
            a = fdot(H[rows, :], W5[:, cols])
        a = a + fdot(LI[rows, :], AU[:, cols])
        LT[rows, cols] = a.astype(BF16)
        top = jnp.max(a, axis=1, keepdims=True)
        e = jnp.exp(a - top)
        E[k, rows, :] = e
        total = jnp.sum(e, axis=1, keepdims=True)
        ids = (lane_cw + (base + k * CW)).astype(F32)
        target = jnp.sum(jnp.where(ids == COL[rows, 0:1], a, 0.0), axis=1, keepdims=True)
        old = COL[rows, :]
        old = jnp.where(lane128 == 8 + k, top, old)
        old = jnp.where(lane128 == 12 + k, total, old)
        COL[rows, :] = jnp.where(lane128 == 16 + k, target, old)

    def turn(o):
        return jnp.where(o == 2, 3, jnp.where(o == 3, 2, o))

    def tasks(k0, nk, o0, no):
        def step(i, carry):
            k, o = k0 + i // no, o0 + lax.rem(i, no)
            r = turn(o)
            task(k, r)
            if o0:
                lg_remote(k, r)
            else:
                pl.when(r > 0)(lambda: lg_remote(k, r))
                pl.when(r == 0)(lambda: lg_local(k))
            return carry

        lax.fori_loop(0, nk * no, step, 0)

    def each_block(f):
        def step(o, carry):
            f(turn(o))
            return carry

        lax.fori_loop(0, NX, step, 0)

    loaded(WS, l_w)
    loaded(W5.at[own_rows, pl.ds(0, U)], l_own)
    send_w(0)
    for r in ORDER:
        send(AX.at[x], AX.at[x], ax_s, ax, {"x": xn(r)})
    for k in range(3):
        y_own(k, 0)
    loaded(H.at[pl.ds(0, T), :], l_h)

    def send_h(r):
        send(hpiece(x, v), hpiece(x, v), h_s, hx + r - 1, {"x": xn(r)})

    send_h(1)
    send_h(3)
    send_w(1)
    send_h(2)
    send_w(2)
    send_w(3)
    phase("p1a")
    y_fwd(0, 0)
    for r in ORDER:
        y_own(0, r)
    y_own(3, 0)
    phase("h_in13")
    h_in(1)
    h_in(3)
    phase("p1b")
    y_fwd(1, 0)
    y_fwd(0, 1)
    y_fwd(0, 3)
    for r in ORDER:
        y_own(1, r)
    y_fwd(0, 2)
    phase("cols")

    got(AX.at[0:3], ax)
    sub = lax.broadcasted_iota(jnp.int32, (8, 128), 0).astype(F32)
    counts = jnp.zeros((8, 128), F32)
    for xb in range(NX):
        for q in range(3):
            tile = AX[xb, q]
            n = min(128, T - q * 128)
            turned = jnp.concatenate([tile, jnp.zeros((120, 128), F32)], axis=0).T
            COL[pl.ds(xb * T + q * 128, n), :] = turned[:n]
            counts = counts + (tile[1:2, :] == sub).astype(F32)
    CN[y] = counts
    for r in (1, 3, 2):
        send(CN.at[y], CN.at[y], cn_s, cn, {"y": yn(r)})
    loaded(AU, l_up)
    loaded(W5.at[:, pl.ds(U, 256)], l_down)
    lora_in(0)
    phase("h_fwd1")
    h_fwd(1)
    phase("h_in2")
    h_in(2)
    phase("p1c")
    y_fwd(1, 1)
    y_fwd(1, 3)
    phase("h_fwd3")
    h_fwd(3)
    phase("y_fwd1")
    y_fwd(1, 2)
    phase("y_own2")
    for r in ORDER:
        y_own(2, r)
    phase("h_last1")
    h_last(1)
    phase("w_end0")
    w_end(0)
    phase("t0_0")
    tasks(0, 1, 0, 1)
    phase("h_end1")
    h_end(1)
    phase("t0_1")
    lora_in(1)
    tasks(0, 1, 1, 1)
    phase("y_own3")
    for r in ORDER:
        y_own(3, r)
    phase("w_end1")
    w_end(1)
    phase("t1_01")
    tasks(1, 1, 0, 2)
    phase("h_fwd2")
    h_fwd(2)
    phase("y_fwd2")
    y_fwd(2, 0)
    y_fwd(2, 1)
    phase("h_last3")
    h_last(3)
    h_end(3)
    phase("t01_3")
    lora_in(3)
    tasks(0, 2, 2, 1)
    phase("y_fwd2b")
    y_fwd(2, 3)
    y_fwd(2, 2)
    y_fwd(3, 0)
    phase("h_last2")
    h_last(2)
    y_fwd(3, 1)
    h_end(2)
    phase("t01_2")
    lora_in(2)
    tasks(0, 2, 3, 1)
    sent(H.at[pl.ds(0, 3 * T), :], h_s)
    phase("y_fwd3")
    y_fwd(3, 3)
    y_fwd(3, 2)
    phase("w_near3")
    w_near(3)
    phase("t3a")
    each_block(functools.partial(early, NK - 1))
    phase("w_end2")
    w_end(2)
    phase("t2")
    tasks(2, 1, 0, 4)
    phase("w_far3")
    w_far(3)
    phase("t3b")
    each_block(functools.partial(task, NK - 1, rest=True))
    phase("stats_a")

    STA[v] = jnp.broadcast_to(jnp.ones((1, 1, 1), F32), (2, 16, 128))
    TA[v] = jnp.zeros((16, 128), F32)
    JR[...] = jnp.full((16, 128), -1.0, F32)
    for b in range(NB):
        t = COL[b * 128 : (b + 1) * 128, :].T
        m, e, g = t[8:12], t[12:16], t[16:20]
        top = jnp.max(m, axis=0, keepdims=True)
        STA[v, 0, b : b + 1, :] = top
        STA[v, 1, b : b + 1, :] = jnp.sum(e * jnp.exp(m - top), axis=0, keepdims=True)
        TA[v, b : b + 1, :] = jnp.sum(g, axis=0, keepdims=True)
        JR[b : b + 1, :] = t[1:2]
    turns = [(a, b) for a in (2, 1, 3, 0) for b in range(NC) if a or b]
    for a, b in turns:
        dev = {"z": zn(a), "c": lax.rem(c + b, NC)}
        send(STA.at[v], STA.at[v], sa_s, sa, dev)
    for a, b in turns:
        send(TA.at[v], TA.at[v], ta_s, ta, {"z": zn(a), "c": lax.rem(c + b, NC)})
    phase("counts")
    got(CN.at[0:3], cn)
    counts = jnp.sum(CN[0] + CN[1] + CN[2] + CN[3], axis=1, keepdims=True)
    counts = jnp.maximum(counts, 1.0)
    per_job = TOKENS / (JOBS * counts)
    jobs = JR[...]
    weight = jnp.zeros((16, 128), F32)
    for j in range(JOBS):
        weight = jnp.where(jobs == float(j), per_job[j : j + 1, :], weight)
    phase("stats_w")
    got(STA.at[0:7], sa)

    def joined(ref, n):
        top = functools.reduce(jnp.maximum, [ref[i, 0] for i in range(n)])
        return top, functools.reduce(jnp.add, [ref[i, 1] * jnp.exp(ref[i, 0] - top) for i in range(n)])

    STB[x, 0], STB[x, 1] = joined(STA, NZ * NC)
    phase("stats_b")
    for r in (2, 1, 3):
        send(STB.at[x], STB.at[x], sb_s, sb, {"x": xn(r)})
    for r in ORDER:
        lg_remote(NK - 1, r)
    lg_local(NK - 1)
    got(STB.at[0:3], sb)
    phase("finish")
    top, e = joined(STB, NX)
    scaled = weight / e
    blank = jnp.zeros((125, 128), F32)
    for b in range(NB):
        parts = [i[b : b + 1] for i in (top, scaled, weight)]
        COL2[b * 128 : (b + 1) * 128, :] = jnp.concatenate(parts + [blank], axis=0).T

    def targets():
        got(TA.at[0:7], ta)
        TB[x] = functools.reduce(jnp.add, [TA[i] for i in range(NZ * NC)])
        for r in (2, 1, 3):
            send(TB.at[x], TB.at[x], tb_s, tb, {"x": xn(r)})

    row_cw = lax.broadcasted_iota(jnp.int32, (1, CW), 1)

    def gradient(j):
        part = pl.ds(OFF[j], LEN[j])

        def step(m, carry):
            rows = pl.ds(al(m * T + OFF[j], 16), LEN[j])
            cols = COL[rows, :]
            lab = cols[:, 0:1]
            weight = COL2[rows, 2:3]
            factors = jnp.exp(cols - COL2[rows, 0:1]) * COL2[rows, 1:2]
            for k in range(NK):
                ids = (row_cw + (base + k * CW)).astype(F32)
                g = E[k, rows, :] * factors[:, 8 + k : 9 + k] - jnp.where(lab == ids, weight, 0.0)
                G5[m, part, k * CW : (k + 1) * CW] = g.astype(BF16)
            return carry

        lax.fori_loop(0, NX, step, 0, unroll=True)
        phase("lora%d" % j)
        rows = G5[:, OFF[j] : OFF[j] + LEN[j], 0:U].reshape(NX * LEN[j], U)
        lora = tdot(rows, AU[...]).reshape(NX, LEN[j], 128)
        for m in range(NX):
            job = COL[m * T + OFF[j] : m * T + OFF[j] + LEN[j], 1:2]
            one = jnp.where(job == rank_job[: LEN[j]], lora[m], 0.0)
            high = one.astype(BF16)
            G5[m, part, U : U + 128] = high
            G5[m, part, U + 128 : U + 256] = (one - high.astype(F32)).astype(BF16)

    def send_rows(i):
        part = pl.ds(OFF[2 * i], LEN[2 * i] + LEN[2 * i + 1])
        for r in ORDER:
            send(G5.at[xn(r), part, pl.ds(0, U)], gr.at[part, pl.ds(my_cols, U)], gr_s, grs, {"x": xn(r)})
        gr[part, pl.ds(my_cols, U)] = G5[x, part, 0:U]

    cs_r = take("r", 32)
    ring_r = take("r", 6 * NR)

    def zt(s, h):
        return lax.rem(z + NZ + (2 * h - 1) * (s + 1), NZ)

    def span(j):
        return pl.ds(NX * OFF[j], NX * LEN[j])

    def unit(s, h, j, core):
        at = al((zt(s, h) * NC + core) * SH + h * CW, CW)
        g = G5[:, OFF[j] : OFF[j] + LEN[j], :].reshape(NX * LEN[j], U + 256)
        return tdot(g, W5[pl.ds(at, CW), :])

    def ps(s, h, j, at=0):
        return H.at[span(j), pl.ds(al(at + (s * 2 + h) * CW, CW), CW)]

    def ps_copy(s, h, j):
        i = (s * 2 + h) * NQ + j
        return rcopy(ps(s, h, j), ps(s, h, j, D // 2), cs_s, cs_r + i, other)

    def ring_copy(s, h, j):
        i = (s * 2 + h) * NR + j
        return rcopy(
            RR.at[s, h, span(j)], RR.at[s + 1, h, span(j)], ring_s, ring_r + i,
            {"z": lax.rem(z + NZ + 1 - 2 * h, NZ)},
        )

    def for_core(s, j):
        def step(h, carry):
            ps(s, h, j)[...] = unit(s, h, j, 1 - c).astype(BF16)
            ps_copy(s, h, j).start()
            return carry

        lax.fori_loop(0, 2, step, 0)

    def mine(s, h, j):
        a = unit(s, h, j, c)
        ps_copy(s, h, j).wait_recv()
        return a + ps(s, h, j, D // 2)[...].astype(F32)

    def with_ring(s, h, j):
        a = mine(s, h, j)
        ring_copy(s - 1, h, j).wait_recv()
        return a + RR[s, h, span(j), :].astype(F32)

    def own(s, j, get):
        def step(h, carry):
            RR[s, h, span(j), :] = get(s, h, j).astype(BF16)
            ring_copy(s, h, j).start()
            return carry

        lax.fori_loop(0, 2, step, 0)

    def own_x(s):
        def step(h, carry):
            cols = pl.ds(al(zt(s, h) * SH + h * CW, CW), CW)
            XF[:, :, cols] = mine(s, h, NR).astype(BF16).reshape(NX, XT, CW)
            return carry

        lax.fori_loop(0, 2, step, 0)

    XH = NZ * SH // 2

    def xcols(i):
        return pl.ds(i * XH, XH)

    def x_first():
        far = XF.at[xn(2)]
        send(far.at[:, xcols(0)], XP.at[0], xf_s, xf, {"x": xn(1)})
        send(far.at[:, xcols(1)], XP.at[1], xf_s, xf + 1, {"x": xn(3)})
        send(XF.at[xn(1), :, xcols(1)], XFR.at[0, :, xcols(1)], xf_s, xf + 2, {"x": xn(1)})
        send(XF.at[xn(3), :, xcols(0)], XFR.at[1, :, xcols(0)], xf_s, xf + 2, {"x": xn(3)})

    def x_first_mid():
        for i, r in ((0, 1), (1, 3)):
            got(XP.at[i], xf + i)
            cols = slice(i * XH, (i + 1) * XH)
            both = XF[xn(r), :, cols].astype(F32) + XP[i].astype(F32)
            XF[xn(r), :, cols] = both.astype(BF16)
            send(XF.at[xn(r), :, xcols(i)], XFR.at[i, :, xcols(i)], xf_s, xf + 2, {"x": xn(r)})

    def x_first_sum():
        phase("xf_sum")
        got(XFR, xf + 2)
        total = XF[x].astype(F32) + XFR[0].astype(F32) + XFR[1].astype(F32)
        XF[x] = total.astype(BF16)
        for r in (2, 1, 3):
            send(XF.at[x, :, pl.ds(al(zn(r) * SH, SH), SH)], ZR.at[r - 1], zr_s, zr, {"z": zn(r)})

    def losses_out():
        phase("losses")
        got(TB.at[0:3], tb)
        loss = top + jnp.log(e) - (TB[0] + TB[1] + TB[2] + TB[3])
        sums = [jnp.sum(jnp.where(jobs == float(j), loss, 0.0), axis=0, keepdims=True) for j in range(JOBS)]
        JL[y] = jnp.concatenate(sums, axis=0)
        for r in (1, 3, 2):
            send(JL.at[y], JL.at[y], jn_s, jn, {"y": yn(r)})
        for b in range(NB):
            row = jnp.concatenate([loss[b : b + 1], jnp.zeros((127, 128), F32)], axis=0)
            COL2[b * 128 : (b + 1) * 128, :] = row.T
        for q in range(3):
            n = min(128, T - q * 128)
            t = COL2[pl.ds(al(x * T + q * 128, 8), n), :]
            if n < 128:
                t = jnp.concatenate([t, jnp.zeros((128 - n, 128), F32)], axis=0)
            small[0:1, q * 128 : (q + 1) * 128] = t.T[0:1]

    def losses_in():
        phase("losses2")
        got(JL.at[0:3], jn)
        total = jnp.sum(JL[0] + JL[1] + JL[2] + JL[3], axis=1, keepdims=True) / counts
        total = jnp.concatenate([jnp.broadcast_to(total, (8, 128)), jnp.zeros((120, 128), F32)], axis=0)
        small[0:1, 384:512] = total.T[0:1]

    units = ("g0 c00 g1 r0", "o00 c01 g2 o01", "c02 g3 o02 c03", "c10 c13 o10 c11", "c23 o11 c12 c33")
    units = units + ("f0 o12 f1 f2", "f3 x t c20", "c21 o20 c22 o21", "m c30 o22 c31")
    for op in " ".join(units).split():
        phase(op)
        n = [int(i) for i in op[1:]]
        if op[0] == "g":
            gradient(n[0])
        elif op[0] == "r":
            send_rows(n[0])
        elif op[0] == "c":
            for_core(*n)
        elif op[0] == "f":
            own_x(n[0])
        elif op[0] == "x":
            x_first()
        elif op[0] == "m":
            x_first_mid()
        elif op[0] == "t":
            targets()
        else:
            own(*n, with_ring if n[0] else mine)

    xr = take("r", 3 * NR)
    ag = take("r", 3 * NQ)

    def hg_at(zz, j, h):
        cols = pl.ds(al(((NC * c + h) * NY + zz) * DB, DB), DB)
        return hg.at[pl.ds(OFF[j], LEN[j]), cols]

    def last(j):
        part = pl.ds(OFF[j], LEN[j])
        phase("last%d" % j)
        for h in range(2):
            a = with_ring(NZ - 1, h, j)
            XS[:, OFF[j] : OFF[j] + LEN[j], h * CW : (h + 1) * CW] = a.astype(BF16).reshape(NX, LEN[j], CW)
        far = XS.at[xn(2), part]
        at = xr + j * 3
        send(far.at[:, pl.ds(0, CW)], XQ.at[0, part], x_s, at, {"x": xn(1)})
        send(far.at[:, pl.ds(CW, CW)], XQ.at[1, part], x_s, at + 1, {"x": xn(3)})
        send(XS.at[xn(1), part, pl.ds(CW, CW)], XR.at[0, part, pl.ds(CW, CW)], x_s, at + 2, {"x": xn(1)})
        send(XS.at[xn(3), part, pl.ds(0, CW)], XR.at[1, part, pl.ds(0, CW)], x_s, at + 2, {"x": xn(3)})

    def x_mid(j):
        part = pl.ds(OFF[j], LEN[j])
        phase("xmid%d" % j)
        at = xr + j * 3
        for i, r in ((0, 1), (1, 3)):
            got(XQ.at[i, part], at + i)
            cols = pl.ds(i * CW, CW)
            both = XS[xn(r), part, cols].astype(F32) + XQ[i, part, :].astype(F32)
            XS[xn(r), part, cols] = both.astype(BF16)
            send(XS.at[xn(r), part, cols], XR.at[i, part, cols], x_s, at + 2, {"x": xn(r)})

    def x_sum(j):
        part = pl.ds(OFF[j], LEN[j])
        phase("xsum%d" % j)
        got(XR.at[:, part], xr + j * 3 + 2)
        total = XS[x, part, :].astype(F32) + XR[0, part, :].astype(F32) + XR[1, part, :].astype(F32)
        FO[part, :] = total.astype(BF16)
        push(j)

    def z_sum():
        phase("zsum")
        got(ZR, zr)
        total = XF[x, :, pl.ds(al(z * SH, SH), SH)].astype(F32)
        for r in (1, 3, 2):
            total = total + ZR[r - 1].astype(F32)
        FO[RT:T, :] = total.astype(BF16)
        push(NR)

    def push(j):
        part = pl.ds(OFF[j], LEN[j])
        for h in range(2):
            src = FO.at[part, pl.ds(h * CW, CW)]
            for r in (1, 3):
                send(src, hg_at(z, j, h), ag_s, ag + j * 3 + r - 1, {"z": zn(r)})
            send(src, hg_at(z, j, h), cc_s, cc, other)
            hg_at(z, j, h)[...] = FO[part, h * CW : (h + 1) * CW]

    def pair_ref(j):
        return hg.at[pl.ds(OFF[j], LEN[j]), pl.ds(0, SH)]

    def relay(j):
        phase("relay%d" % j)
        for r in (1, 3):
            got(pair_ref(j), ag + j * 3 + r - 1)
            h = r // 2
            src = hg_at(lax.rem(z + NZ - r, NZ), j, h)
            send(src, src, ag_s, ag + j * 3 + 1, {"z": zn(r)})
            for h in range(2):
                src = hg_at(lax.rem(z + NZ - r, NZ), j, h)
                send(src, src, cc_s, cc, other)

    def gather(j):
        phase("gather%d" % j)
        got(pair_ref(j), ag + j * 3 + 1)
        for h in range(2):
            src = hg_at(zn(2), j, h)
            send(src, src, cc_s, cc, other)

    last(0)
    for_core(3, 2)
    last(1)
    x_mid(0)
    x_first_sum()
    last(2)
    x_sum(0)
    x_mid(1)
    x_mid(2)
    send_rows(1)
    z_sum()
    x_sum(1)
    relay(0)
    x_sum(2)
    relay(3)
    relay(1)
    gather(0)
    relay(2)
    gather(3)
    losses_out()
    gather(1)
    gather(2)
    losses_in()

    phase("arrivals")
    got(lg.at[:, pl.ds(0, 3 * U)], lgs)
    phase("arr_gr")
    got(gr.at[:, pl.ds(0, 3 * U)], grs)
    phase("arr_hg")
    got(hg.at[:, pl.ds(0, NZ * SH)], cc)
    phase("drain")
    sent(W5.at[pl.ds(0, 60 * DB // NX), pl.ds(0, U)], ws_s)
    sent(AX.at[0:3], ax_s)
    sent(lg.at[:, pl.ds(0, 3 * U)], lg_s)
    sent(CN.at[0:3], cn_s)
    sent(STA.at[0:7], sa_s)
    sent(STB.at[0:3], sb_s)
    sent(gr.at[:, pl.ds(0, 3 * U)], gr_s)
    sent(H.at[:, pl.ds(0, D // 2)], cs_s)
    sent(RR.at[0:3], ring_s)
    sent(JL.at[0:3], jn_s)
    sent(XS.at[0:3], x_s)
    sent(XF.at[0:3], xf_s)
    sent(ZR, zr_s)
    sent(hg.at[:, pl.ds(0, 3 * SH)], ag_s)
    sent(TA.at[0:7], ta_s)
    sent(TB.at[0:3], tb_s)
    sent(hg.at[:, pl.ds(0, NZ * SH)], cc_s)
    phase(None)
    assert used == {"s": NSEND, "r": NRECV, "l": NLOAD}, used


NSEND, NRECV, NLOAD = 18, 136, 5


def emit(lgv, grv, hgv, small, lg, gr, hg, tl, jl, sem):
    copies = []
    for src, dst in ((lgv, lg), (grv, gr), (hgv, hg)):
        for i in range(4):
            part = pl.ds(i * 88, 88)
            copies.append(pltpu.make_async_copy(src.at[part], dst.at[part], sem.at[len(copies)]))
    for d in copies:
        d.start()
    tl[...] = small[0, :T]
    jl[...] = small[0, 384 : 384 + JOBS]
    for d in copies:
        d.wait()


def vmem(*shape, dtype=BF16):
    return pltpu.VMEM(shape, dtype)


def shards(hidden, weight, down, up, labels, jobs):
    hbm = pl.BlockSpec(memory_space=pl.ANY)
    vm = pl.BlockSpec(memory_space=pltpu.VMEM)
    held = pl.pallas_call(
        kernel,
        out_shape=(vmem(T, V), vmem(T, V), vmem(T, D), vmem(1, 512, dtype=F32)),
        in_specs=[hbm] * 4 + [vm] * 2,
        out_specs=(vm, vm, vm, vm),
        scratch_shapes=[
            vmem(S, D),
            vmem(D, U + 256),
            vmem(DB, V),
            vmem(NK, S, CW, dtype=F32),
            vmem(S, U),
            vmem(NX, T, U + 256),
            vmem(NZ, 2, NX * RT, CW),
            vmem(NX, RT, SH),
            vmem(2, RT, SH),
            vmem(2, RT, CW),
            vmem(NX, XT, NZ * SH),
            vmem(2, XT, NZ * SH),
            vmem(2, XT, NZ * SH // 2),
            vmem(3, XT, SH),
            vmem(T, SH),
            vmem(S, 128, dtype=F32),
            vmem(S, 128, dtype=F32),
            vmem(S, 128),
            vmem(128, U),
            vmem(NX, 3, 8, 128, dtype=F32),
            vmem(NZ * NC, 2, 16, 128, dtype=F32),
            vmem(NX, 2, 16, 128, dtype=F32),
            vmem(NZ * NC, 16, 128, dtype=F32),
            vmem(NX, 16, 128, dtype=F32),
            vmem(16, 128, dtype=F32),
            vmem(NY, 8, 128, dtype=F32),
            vmem(NY, 8, 128, dtype=F32),
            pltpu.SemaphoreType.DMA((NSEND,)),
            pltpu.SemaphoreType.DMA((NRECV,)),
            pltpu.SemaphoreType.DMA((NLOAD,)),
        ],
        compiler_params=pltpu.CompilerParams(
            collective_id=0, has_side_effects=True, vmem_limit_bytes=53 * 1024 * 1024
        ),
        name="step",
    )(hidden, weight, down, up, labels, jobs)
    return pl.pallas_call(
        emit,
        out_shape=(
            jax.ShapeDtypeStruct((T, V), BF16),
            jax.ShapeDtypeStruct((T, V), BF16),
            jax.ShapeDtypeStruct((T, D), BF16),
            jax.ShapeDtypeStruct((T,), F32),
            jax.ShapeDtypeStruct((JOBS,), F32),
        ),
        in_specs=[vm] * 4,
        out_specs=(hbm, hbm, hbm, vm, vm),
        scratch_shapes=[pltpu.SemaphoreType.DMA((12,))],
        compiler_params=pltpu.CompilerParams(vmem_limit_bytes=1024 * 1024),
        name="emit",
    )(*(pltpu.with_memory_space_constraint(i, pltpu.VMEM) for i in held))


def solution(mesh):
    split = Mesh(mesh.devices.reshape(NZ, NC, NX, NY), ("z", "c", "x", "y"))
    dp, vocab = ("x", "y"), ("z", "c")
    return jax.shard_map(
        shards,
        mesh=split,
        in_specs=(P(dp, None), P(dp, vocab), P(), P(None, vocab), P(dp), P(dp)),
        out_specs=(P(dp, vocab), P(dp, vocab), P(dp, None), P(dp), P()),
        check_vma=False,
    )
```

```python
import functools

import jax
import jax.numpy as jnp
from jax import lax
from jax.experimental import pallas as pl
from jax.experimental.pallas import tpu as pltpu
from jax.sharding import Mesh
from jax.sharding import PartitionSpec as P

MESH = pl.DeviceIdType.MESH
F32 = jnp.float32
BF16 = jnp.bfloat16

JOBS = 8
RANK = 16
NX = NY = NZ = 4
NC = 2
T = 352
S = NX * T
HT = T // 2
LEN = (112, 112, 48, 80)
OFF = (0, 112, 224, 272)
NQ = len(LEN)
NR = NQ - 1
RT = OFF[NR]
XT = LEN[NR]
D = 4096
DB = D // (NX * NY)
V = 4096
U = V // NX
CW = 256
NK = U // CW
SH = D // (NZ * NC)
TOKENS = S * NY
NB = S // 128


def fdot(a, b):
    return jnp.dot(a, b, preferred_element_type=F32)


def tdot(a, b):
    return lax.dot_general(a, b, (((1,), (1,)), ((), ())), preferred_element_type=F32)


def kernel(
    hid, w, ad, au, lab_in, job_in,
    lg, gr, hg, small,
    H, W5, WS, E, LT, G5, RR, XS, XR, XQ, XF, XFR, XP, ZR, FO, COL, COL2, LI, AU, AX, STA, STB, TA, TB, JR, CN, JL,
    ssem, rsem, lsem,
):
    z, c, x, y = (lax.axis_index(a) for a in ("z", "c", "x", "y"))
    v = z * NC + c

    def al(i, m):
        return pl.multiple_of(i, m)

    def xn(r):
        return lax.rem(x + r, NX)

    def yn(r):
        return lax.rem(y + r, NY)

    def zn(r):
        return lax.rem(z + r, NZ)

    used = {"s": 0, "r": 0, "l": 0}

    def take(kind, n=1):
        at = used[kind]
        used[kind] = at + n
        return at

    def rcopy(src, dst, si, ri, dev):
        return pltpu.make_async_remote_copy(
            src_ref=src, dst_ref=dst, send_sem=ssem.at[si], recv_sem=rsem.at[ri],
            device_id=dev, device_id_type=MESH,
        )

    def send(src, dst, si, ri, dev):
        rcopy(src, dst, si, ri, dev).start()

    def got(ref, ri):
        rcopy(ref, ref, 0, ri, {"x": xn(1)}).wait_recv()

    def sent(ref, si):
        rcopy(ref, ref, si, 0, {"x": xn(1)}).wait_send()

    def load(src, dst, li):
        pltpu.make_async_copy(src, dst, lsem.at[li]).start()

    def loaded(ref, li):
        pltpu.make_async_copy(ref, ref, lsem.at[li]).wait()

    scope = []

    def phase(name):
        if scope:
            scope.pop().__exit__(None, None, None)
        if name:
            scope.append(jax.named_scope(name))
            scope[0].__enter__()

    phase("entry")
    bar = pltpu.get_barrier_semaphore()
    peers = (
        [{"x": xn(r)} for r in (1, 2, 3)]
        + [{"y": yn(r)} for r in (1, 2, 3)]
        + [{"z": zn(a), "c": lax.rem(c + b, NC)} for a in range(NZ) for b in range(NC) if a or b]
    )
    for dev in peers:
        pl.semaphore_signal(bar, inc=1, device_id=dev, device_id_type=MESH)

    l_w, l_own, l_h, l_up, l_down = (take("l") for _ in range(5))
    load(w, WS, l_w)
    own_rows = pl.ds(al((y * NX + x) * DB, DB), DB)
    load(w.at[:, pl.ds(al(x * U, U), U)], W5.at[own_rows, pl.ds(0, U)], l_own)
    for p in range(NX * NY):
        n = (p % NX) * NY + p // NX
        load(hid.at[:, pl.ds(n * DB, DB)], H.at[pl.ds(al(x * T, 16), T), pl.ds(p * DB, DB)], l_h)
    load(au.at[:, pl.ds(al(x * U, U), U)], AU, l_up)
    for p in range(NX * NY):
        n = (p % NX) * NY + p // NX
        for q in range(2):
            load(
                ad.at[pl.ds(n * DB, DB), :],
                W5.at[pl.ds(p * DB, DB), pl.ds(U + q * 128, 128)],
                l_down,
            )
    for q in range(3):
        n = min(128, T - q * 128)
        AX[x, q] = jnp.full((8, 128), -1.0, F32)
        AX[x, q, 0:1, 0:n] = lab_in[pl.ds(q * 128, n)].astype(F32).reshape(1, n)
        AX[x, q, 1:2, 0:n] = job_in[pl.ds(q * 128, n)].astype(F32).reshape(1, n)
    pl.semaphore_wait(bar, len(peers))

    ORDER = (1, 3, 2)
    wx = take("r", NK * 3)
    hx = take("r", 3)
    ax, lgs, cn, sa, sb, ta, tb, grs, jn, cc, zr = (take("r") for _ in range(11))
    xf = take("r", 3)
    wy = take("r", NK * 6)
    hz = take("r", 3 * 3)
    hc = take("r", 3)
    ws_s, h_s, ax_s, lg_s, cn_s, sa_s, sb_s, ta_s, tb_s, gr_s, cs_s, ring_s, jn_s, x_s, xf_s, zr_s, ag_s, cc_s = (
        take("s") for _ in range(18)
    )

    def xp(r):
        return lax.rem(x + NX - r, NX)

    def wblock(row, k):
        return W5.at[row, pl.ds(k * CW, CW)]

    def send_w(k):
        for r in ORDER:
            send(
                WS.at[:, pl.ds(al(xn(r) * U + k * CW, CW), CW)],
                wblock(own_rows, k), ws_s, wx + k * 3 + r - 1, {"x": xn(r)},
            )

    def piece(dy, r, k):
        return wblock(pl.ds(al((yn(dy) * NX + xp(r)) * DB, DB), DB), k)

    def y_own(k, r):
        src = piece(0, r, k)
        if r:
            got(src, wx + k * 3 + r - 1)
        at = wy + k * 6
        send(src, src, ws_s, at + (r if r in (0, 2) else 4), {"y": yn(1)})
        send(src, src, ws_s, at + (4 if r in (0, 2) else r), {"y": yn(3)})

    def y_fwd(k, r):
        at = wy + k * 6
        src = piece(3 if r in (0, 2) else 1, r, k)
        got(src, at + r)
        send(src, src, ws_s, at + 5, {"y": yn(1 if r in (0, 2) else 3)})

    def w_near(k):
        got(wblock(pl.ds(0, 4 * DB), k), wy + k * 6 + 4)

    def w_far(k):
        got(wblock(pl.ds(0, 4 * DB), k), wy + k * 6 + 5)

    def w_end(k):
        w_near(k)
        w_far(k)

    other = {"c": 1 - c}

    def hpiece(xb, share, lo=0, n=T):
        return H.at[pl.ds(al(xb * T + lo, 16), n), pl.ds(al(share * SH, SH), SH)]

    def h_send(at, ri, dev):
        send(at, at, h_s, ri, dev)

    def h_in(r):
        mine = hpiece(xp(r), v)
        got(mine, hx + r - 1)
        b = hz + (r - 1) * 3
        h_send(mine, b + 0, {"z": zn(1)})
        h_send(mine, b + 1, {"z": zn(3)})
        h_send(mine, hc + r - 1, other)

    def h_fwd(r):
        xb = xp(r)
        b, d = hz + (r - 1) * 3, hc + r - 1
        left, right = zn(3) * NC + c, zn(1) * NC + c
        got(hpiece(xb, left), b + 0)
        h_send(hpiece(xb, left, 0, HT), b + 2, {"z": zn(1)})
        h_send(hpiece(xb, left), d, other)
        got(hpiece(xb, right), b + 1)
        h_send(hpiece(xb, right, HT, HT), b + 2, {"z": zn(3)})
        h_send(hpiece(xb, right), d, other)

    def h_last(r):
        far = hpiece(xp(r), zn(2) * NC + c)
        got(far, hz + (r - 1) * 3 + 2)
        h_send(far, hc + r - 1, other)

    def h_end(r):
        got(H.at[pl.ds(0, T), pl.ds(0, NZ * SH)], hc + r - 1)

    lane128 = lax.broadcasted_iota(jnp.int32, (T, 128), 1)
    rank_job = (lane128 // RANK).astype(F32)
    base = v * V + x * U
    lane_cw = lax.broadcasted_iota(jnp.int32, (T, CW), 1)
    my_cols = al(x * U, U)

    def lora_in(r):
        rows = pl.ds(al(xp(r) * T, 16), T)
        hit = COL[rows, 1:2] == rank_job
        a = fdot(H[rows, :], W5[:, U : U + 128])
        LI[rows, :] = jnp.where(hit, a, 0.0).astype(BF16)

    def lg_cols(k):
        return pl.ds(al(my_cols + k * CW, CW), CW)

    def lg_remote(k, r):
        src = LT.at[pl.ds(al(xp(r) * T, 16), T), pl.ds(al(k * CW, CW), CW)]
        send(src, lg.at[:, lg_cols(k)], lg_s, lgs, {"x": xp(r)})

    def lg_local(k):
        cols = pl.ds(al(k * CW, CW), CW)
        lg[:, lg_cols(k)] = LT[pl.ds(al(x * T, 16), T), cols]

    def part_of(rows, cols, dy):
        deep = pl.ds(al(yn(dy) * NX * DB, DB), NX * DB)
        return fdot(H[rows, deep], W5[deep, cols])

    def early(k, r):
        rows = pl.ds(al(xp(r) * T, 16), T)
        cols = pl.ds(al(k * CW, CW), CW)
        E[k, rows, :] = part_of(rows, cols, 0) + part_of(rows, cols, 1) + part_of(rows, cols, 3)

    def task(k, r, rest=False):
        rows = pl.ds(al(xp(r) * T, 16), T)
        cols = pl.ds(al(k * CW, CW), CW)
        if rest:
            a = E[k, rows, :] + part_of(rows, cols, 2)
        else:
            a = fdot(H[rows, :], W5[:, cols])
        a = a + fdot(LI[rows, :], AU[:, cols])
        LT[rows, cols] = a.astype(BF16)
        top = jnp.max(a, axis=1, keepdims=True)
        e = jnp.exp(a - top)
        E[k, rows, :] = e
        total = jnp.sum(e, axis=1, keepdims=True)
        ids = (lane_cw + (base + k * CW)).astype(F32)
        target = jnp.sum(jnp.where(ids == COL[rows, 0:1], a, 0.0), axis=1, keepdims=True)
        old = COL[rows, :]
        old = jnp.where(lane128 == 8 + k, top, old)
        old = jnp.where(lane128 == 12 + k, total, old)
        COL[rows, :] = jnp.where(lane128 == 16 + k, target, old)

    def turn(o):
        return jnp.where(o == 2, 3, jnp.where(o == 3, 2, o))

    def tasks(k0, nk, o0, no, rest=False):
        def step(i, carry):
            k, o = k0 + i // no, o0 + lax.rem(i, no)
            r = turn(o)
            task(k, r, rest)
            if o0:
                lg_remote(k, r)
            else:
                pl.when(r > 0)(lambda: lg_remote(k, r))
                pl.when(r == 0)(lambda: lg_local(k))
            return carry

        lax.fori_loop(0, nk * no, step, 0)

    def each_block(f):
        def step(o, carry):
            f(turn(o))
            return carry

        lax.fori_loop(0, NX, step, 0)

    loaded(WS, l_w)
    loaded(W5.at[own_rows, pl.ds(0, U)], l_own)
    send_w(0)
    for r in ORDER:
        send(AX.at[x], AX.at[x], ax_s, ax, {"x": xn(r)})
    for k in range(3):
        y_own(k, 0)
    loaded(H.at[pl.ds(0, T), :], l_h)

    def send_h(r):
        send(hpiece(x, v), hpiece(x, v), h_s, hx + r - 1, {"x": xn(r)})

    send_h(1)
    send_h(3)
    send_w(1)
    send_h(2)
    send_w(2)
    send_w(3)
    phase("p1a")
    y_fwd(0, 0)
    for r in ORDER:
        y_own(0, r)
    y_own(3, 0)
    phase("h_in13")
    h_in(1)
    h_in(3)
    phase("p1b")
    y_fwd(1, 0)
    y_fwd(0, 1)
    y_fwd(0, 3)
    for r in ORDER:
        y_own(1, r)
    y_fwd(0, 2)
    phase("cols")

    got(AX.at[0:3], ax)
    sub = lax.broadcasted_iota(jnp.int32, (8, 128), 0).astype(F32)
    counts = jnp.zeros((8, 128), F32)
    for xb in range(NX):
        for q in range(3):
            tile = AX[xb, q]
            n = min(128, T - q * 128)
            turned = jnp.concatenate([tile, jnp.zeros((120, 128), F32)], axis=0).T
            COL[pl.ds(xb * T + q * 128, n), :] = turned[:n]
            counts = counts + (tile[1:2, :] == sub).astype(F32)
    CN[y] = counts
    for r in (1, 3, 2):
        send(CN.at[y], CN.at[y], cn_s, cn, {"y": yn(r)})
    loaded(AU, l_up)
    loaded(W5.at[:, pl.ds(U, 256)], l_down)
    lora_in(0)
    phase("h_fwd1")
    h_fwd(1)
    phase("h_in2")
    h_in(2)
    phase("p1c")
    y_fwd(1, 1)
    y_fwd(1, 3)
    phase("h_fwd3")
    h_fwd(3)
    phase("y_fwd1")
    y_fwd(1, 2)
    phase("y_own2")
    for r in ORDER:
        y_own(2, r)
    phase("h_last1")
    h_last(1)
    phase("w_end0")
    w_end(0)
    phase("t0_0")
    tasks(0, 1, 0, 1)
    phase("h_end1")
    h_end(1)
    phase("t0_1")
    lora_in(1)
    tasks(0, 1, 1, 1)
    phase("y_own3")
    for r in ORDER:
        y_own(3, r)
    phase("w_end1")
    w_end(1)
    phase("t1_01")
    tasks(1, 1, 0, 2)
    phase("h_fwd2")
    h_fwd(2)
    phase("y_fwd2")
    y_fwd(2, 0)
    y_fwd(2, 1)
    phase("h_last3")
    h_last(3)
    h_end(3)
    phase("t01_3")
    lora_in(3)
    tasks(0, 2, 2, 1)
    phase("y_fwd2b")
    y_fwd(2, 3)
    y_fwd(2, 2)
    y_fwd(3, 0)
    phase("h_last2")
    h_last(2)
    y_fwd(3, 1)
    h_end(2)
    phase("t01_2")
    lora_in(2)
    tasks(0, 2, 3, 1)
    sent(H.at[pl.ds(0, 3 * T), :], h_s)
    phase("y_fwd3")
    y_fwd(3, 3)
    y_fwd(3, 2)
    phase("w_near2")
    w_near(2)
    phase("t2a")
    each_block(functools.partial(early, NK - 2))
    phase("w_near3")
    w_near(3)
    phase("t3a")
    each_block(functools.partial(early, NK - 1))
    phase("w_far2")
    w_far(2)
    phase("t2b")
    tasks(2, 1, 0, 4, True)
    phase("w_far3")
    w_far(3)
    phase("t3b")
    each_block(functools.partial(task, NK - 1, rest=True))
    phase("stats_a")

    STA[v] = jnp.broadcast_to(jnp.ones((1, 1, 1), F32), (2, 16, 128))
    TA[v] = jnp.zeros((16, 128), F32)
    JR[...] = jnp.full((16, 128), -1.0, F32)
    for b in range(NB):
        t = COL[b * 128 : (b + 1) * 128, :].T
        m, e, g = t[8:12], t[12:16], t[16:20]
        top = jnp.max(m, axis=0, keepdims=True)
        STA[v, 0, b : b + 1, :] = top
        STA[v, 1, b : b + 1, :] = jnp.sum(e * jnp.exp(m - top), axis=0, keepdims=True)
        TA[v, b : b + 1, :] = jnp.sum(g, axis=0, keepdims=True)
        JR[b : b + 1, :] = t[1:2]
    turns = [(a, b) for a in (2, 1, 3, 0) for b in range(NC) if a or b]
    for a, b in turns:
        dev = {"z": zn(a), "c": lax.rem(c + b, NC)}
        send(STA.at[v], STA.at[v], sa_s, sa, dev)
    for a, b in turns:
        send(TA.at[v], TA.at[v], ta_s, ta, {"z": zn(a), "c": lax.rem(c + b, NC)})
    phase("counts")
    got(CN.at[0:3], cn)
    counts = jnp.sum(CN[0] + CN[1] + CN[2] + CN[3], axis=1, keepdims=True)
    counts = jnp.maximum(counts, 1.0)
    per_job = TOKENS / (JOBS * counts)
    jobs = JR[...]
    weight = jnp.zeros((16, 128), F32)
    for j in range(JOBS):
        weight = jnp.where(jobs == float(j), per_job[j : j + 1, :], weight)
    phase("stats_w")
    got(STA.at[0:7], sa)

    def joined(ref, n):
        top = functools.reduce(jnp.maximum, [ref[i, 0] for i in range(n)])
        return top, functools.reduce(jnp.add, [ref[i, 1] * jnp.exp(ref[i, 0] - top) for i in range(n)])

    STB[x, 0], STB[x, 1] = joined(STA, NZ * NC)
    phase("stats_b")
    for r in (2, 1, 3):
        send(STB.at[x], STB.at[x], sb_s, sb, {"x": xn(r)})
    for r in ORDER:
        lg_remote(NK - 1, r)
    lg_local(NK - 1)
    got(STB.at[0:3], sb)
    phase("finish")
    top, e = joined(STB, NX)
    scaled = weight / e
    blank = jnp.zeros((125, 128), F32)
    for b in range(NB):
        parts = [i[b : b + 1] for i in (top, scaled, weight)]
        COL2[b * 128 : (b + 1) * 128, :] = jnp.concatenate(parts + [blank], axis=0).T

    def targets():
        got(TA.at[0:7], ta)
        TB[x] = functools.reduce(jnp.add, [TA[i] for i in range(NZ * NC)])
        for r in (2, 1, 3):
            send(TB.at[x], TB.at[x], tb_s, tb, {"x": xn(r)})

    row_cw = lax.broadcasted_iota(jnp.int32, (1, CW), 1)

    def gradient(j):
        part = pl.ds(OFF[j], LEN[j])

        def step(m, carry):
            rows = pl.ds(al(m * T + OFF[j], 16), LEN[j])
            cols = COL[rows, :]
            lab = cols[:, 0:1]
            weight = COL2[rows, 2:3]
            factors = jnp.exp(cols - COL2[rows, 0:1]) * COL2[rows, 1:2]
            for k in range(NK):
                ids = (row_cw + (base + k * CW)).astype(F32)
                g = E[k, rows, :] * factors[:, 8 + k : 9 + k] - jnp.where(lab == ids, weight, 0.0)
                G5[m, part, k * CW : (k + 1) * CW] = g.astype(BF16)
            return carry

        lax.fori_loop(0, NX, step, 0, unroll=True)
        phase("lora%d" % j)
        rows = G5[:, OFF[j] : OFF[j] + LEN[j], 0:U].reshape(NX * LEN[j], U)
        lora = tdot(rows, AU[...]).reshape(NX, LEN[j], 128)
        for m in range(NX):
            job = COL[m * T + OFF[j] : m * T + OFF[j] + LEN[j], 1:2]
            one = jnp.where(job == rank_job[: LEN[j]], lora[m], 0.0)
            high = one.astype(BF16)
            G5[m, part, U : U + 128] = high
            G5[m, part, U + 128 : U + 256] = (one - high.astype(F32)).astype(BF16)

    def send_rows(i):
        part = pl.ds(OFF[2 * i], LEN[2 * i] + LEN[2 * i + 1])
        for r in ORDER:
            send(G5.at[xn(r), part, pl.ds(0, U)], gr.at[part, pl.ds(my_cols, U)], gr_s, grs, {"x": xn(r)})
        gr[part, pl.ds(my_cols, U)] = G5[x, part, 0:U]

    cs_r = take("r", 32)
    ring_r = take("r", 6 * NR)

    def zt(s, h):
        return lax.rem(z + NZ + (2 * h - 1) * (s + 1), NZ)

    def span(j):
        return pl.ds(NX * OFF[j], NX * LEN[j])

    def unit(s, h, j, core):
        at = al((zt(s, h) * NC + core) * SH + h * CW, CW)
        g = G5[:, OFF[j] : OFF[j] + LEN[j], :].reshape(NX * LEN[j], U + 256)
        return tdot(g, W5[pl.ds(at, CW), :])

    def ps(s, h, j, at=0):
        return H.at[span(j), pl.ds(al(at + (s * 2 + h) * CW, CW), CW)]

    def ps_copy(s, h, j):
        i = (s * 2 + h) * NQ + j
        return rcopy(ps(s, h, j), ps(s, h, j, D // 2), cs_s, cs_r + i, other)

    def ring_copy(s, h, j):
        i = (s * 2 + h) * NR + j
        return rcopy(
            RR.at[s, h, span(j)], RR.at[s + 1, h, span(j)], ring_s, ring_r + i,
            {"z": lax.rem(z + NZ + 1 - 2 * h, NZ)},
        )

    def for_core(s, j):
        def step(h, carry):
            ps(s, h, j)[...] = unit(s, h, j, 1 - c).astype(BF16)
            ps_copy(s, h, j).start()
            return carry

        lax.fori_loop(0, 2, step, 0)

    def mine(s, h, j):
        a = unit(s, h, j, c)
        ps_copy(s, h, j).wait_recv()
        return a + ps(s, h, j, D // 2)[...].astype(F32)

    def with_ring(s, h, j):
        a = mine(s, h, j)
        ring_copy(s - 1, h, j).wait_recv()
        return a + RR[s, h, span(j), :].astype(F32)

    def own(s, j, get):
        def step(h, carry):
            RR[s, h, span(j), :] = get(s, h, j).astype(BF16)
            ring_copy(s, h, j).start()
            return carry

        lax.fori_loop(0, 2, step, 0)

    def own_x(s):
        def step(h, carry):
            cols = pl.ds(al(zt(s, h) * SH + h * CW, CW), CW)
            XF[:, :, cols] = mine(s, h, NR).astype(BF16).reshape(NX, XT, CW)
            return carry

        lax.fori_loop(0, 2, step, 0)

    XH = NZ * SH // 2

    def xcols(i):
        return pl.ds(i * XH, XH)

    def x_first():
        far = XF.at[xn(2)]
        send(far.at[:, xcols(0)], XP.at[0], xf_s, xf, {"x": xn(1)})
        send(far.at[:, xcols(1)], XP.at[1], xf_s, xf + 1, {"x": xn(3)})
        send(XF.at[xn(1), :, xcols(1)], XFR.at[0, :, xcols(1)], xf_s, xf + 2, {"x": xn(1)})
        send(XF.at[xn(3), :, xcols(0)], XFR.at[1, :, xcols(0)], xf_s, xf + 2, {"x": xn(3)})

    def x_first_mid():
        for i, r in ((0, 1), (1, 3)):
            got(XP.at[i], xf + i)
            cols = slice(i * XH, (i + 1) * XH)
            both = XF[xn(r), :, cols].astype(F32) + XP[i].astype(F32)
            XF[xn(r), :, cols] = both.astype(BF16)
            send(XF.at[xn(r), :, xcols(i)], XFR.at[i, :, xcols(i)], xf_s, xf + 2, {"x": xn(r)})

    def x_first_sum():
        phase("xf_sum")
        got(XFR, xf + 2)
        total = XF[x].astype(F32) + XFR[0].astype(F32) + XFR[1].astype(F32)
        XF[x] = total.astype(BF16)
        for r in (2, 1, 3):
            send(XF.at[x, :, pl.ds(al(zn(r) * SH, SH), SH)], ZR.at[r - 1], zr_s, zr, {"z": zn(r)})

    def losses_out():
        phase("losses")
        got(TB.at[0:3], tb)
        loss = top + jnp.log(e) - (TB[0] + TB[1] + TB[2] + TB[3])
        sums = [jnp.sum(jnp.where(jobs == float(j), loss, 0.0), axis=0, keepdims=True) for j in range(JOBS)]
        JL[y] = jnp.concatenate(sums, axis=0)
        for r in (1, 3, 2):
            send(JL.at[y], JL.at[y], jn_s, jn, {"y": yn(r)})
        for b in range(NB):
            row = jnp.concatenate([loss[b : b + 1], jnp.zeros((127, 128), F32)], axis=0)
            COL2[b * 128 : (b + 1) * 128, :] = row.T
        for q in range(3):
            n = min(128, T - q * 128)
            t = COL2[pl.ds(al(x * T + q * 128, 8), n), :]
            if n < 128:
                t = jnp.concatenate([t, jnp.zeros((128 - n, 128), F32)], axis=0)
            small[0:1, q * 128 : (q + 1) * 128] = t.T[0:1]

    def losses_in():
        phase("losses2")
        got(JL.at[0:3], jn)
        total = jnp.sum(JL[0] + JL[1] + JL[2] + JL[3], axis=1, keepdims=True) / counts
        total = jnp.concatenate([jnp.broadcast_to(total, (8, 128)), jnp.zeros((120, 128), F32)], axis=0)
        small[0:1, 384:512] = total.T[0:1]

    units = ("g0 c00 g1 r0", "o00 c01 g2 o01", "c02 g3 o02 c03", "c10 c13 o10 c11", "c23 o11 c12 c33")
    units = units + ("f0 o12 f1 f2", "f3 x t c20", "c21 o20 c22 o21", "m c30 o22 c31")
    for op in " ".join(units).split():
        phase(op)
        n = [int(i) for i in op[1:]]
        if op[0] == "g":
            gradient(n[0])
        elif op[0] == "r":
            send_rows(n[0])
        elif op[0] == "c":
            for_core(*n)
        elif op[0] == "f":
            own_x(n[0])
        elif op[0] == "x":
            x_first()
        elif op[0] == "m":
            x_first_mid()
        elif op[0] == "t":
            targets()
        else:
            own(*n, with_ring if n[0] else mine)

    xr = take("r", 3 * NR)
    ag = take("r", 3 * NQ)

    def hg_at(zz, j, h):
        cols = pl.ds(al(((NC * c + h) * NY + zz) * DB, DB), DB)
        return hg.at[pl.ds(OFF[j], LEN[j]), cols]

    def last(j):
        part = pl.ds(OFF[j], LEN[j])
        phase("last%d" % j)
        for h in range(2):
            a = with_ring(NZ - 1, h, j)
            XS[:, OFF[j] : OFF[j] + LEN[j], h * CW : (h + 1) * CW] = a.astype(BF16).reshape(NX, LEN[j], CW)
        far = XS.at[xn(2), part]
        at = xr + j * 3
        send(far.at[:, pl.ds(0, CW)], XQ.at[0, part], x_s, at, {"x": xn(1)})
        send(far.at[:, pl.ds(CW, CW)], XQ.at[1, part], x_s, at + 1, {"x": xn(3)})
        send(XS.at[xn(1), part, pl.ds(CW, CW)], XR.at[0, part, pl.ds(CW, CW)], x_s, at + 2, {"x": xn(1)})
        send(XS.at[xn(3), part, pl.ds(0, CW)], XR.at[1, part, pl.ds(0, CW)], x_s, at + 2, {"x": xn(3)})

    def x_mid(j):
        part = pl.ds(OFF[j], LEN[j])
        phase("xmid%d" % j)
        at = xr + j * 3
        for i, r in ((0, 1), (1, 3)):
            got(XQ.at[i, part], at + i)
            cols = pl.ds(i * CW, CW)
            both = XS[xn(r), part, cols].astype(F32) + XQ[i, part, :].astype(F32)
            XS[xn(r), part, cols] = both.astype(BF16)
            send(XS.at[xn(r), part, cols], XR.at[i, part, cols], x_s, at + 2, {"x": xn(r)})

    def x_sum(j):
        part = pl.ds(OFF[j], LEN[j])
        phase("xsum%d" % j)
        got(XR.at[:, part], xr + j * 3 + 2)
        total = XS[x, part, :].astype(F32) + XR[0, part, :].astype(F32) + XR[1, part, :].astype(F32)
        FO[part, :] = total.astype(BF16)
        push(j)

    def z_sum():
        phase("zsum")
        got(ZR, zr)
        total = XF[x, :, pl.ds(al(z * SH, SH), SH)].astype(F32)
        for r in (1, 3, 2):
            total = total + ZR[r - 1].astype(F32)
        FO[RT:T, :] = total.astype(BF16)
        push(NR)

    def push(j):
        part = pl.ds(OFF[j], LEN[j])
        for h in range(2):
            src = FO.at[part, pl.ds(h * CW, CW)]
            for r in (1, 3):
                send(src, hg_at(z, j, h), ag_s, ag + j * 3 + r - 1, {"z": zn(r)})
            send(src, hg_at(z, j, h), cc_s, cc, other)
            hg_at(z, j, h)[...] = FO[part, h * CW : (h + 1) * CW]

    def pair_ref(j):
        return hg.at[pl.ds(OFF[j], LEN[j]), pl.ds(0, SH)]

    def relay(j):
        phase("relay%d" % j)
        for r in (1, 3):
            got(pair_ref(j), ag + j * 3 + r - 1)
            h = r // 2
            src = hg_at(lax.rem(z + NZ - r, NZ), j, h)
            send(src, src, ag_s, ag + j * 3 + 1, {"z": zn(r)})
            for h in range(2):
                src = hg_at(lax.rem(z + NZ - r, NZ), j, h)
                send(src, src, cc_s, cc, other)

    def gather(j):
        phase("gather%d" % j)
        got(pair_ref(j), ag + j * 3 + 1)
        for h in range(2):
            src = hg_at(zn(2), j, h)
            send(src, src, cc_s, cc, other)

    last(0)
    for_core(3, 2)
    x_mid(0)
    x_first_sum()
    last(1)
    x_sum(0)
    last(2)
    x_mid(1)
    x_mid(2)
    send_rows(1)
    z_sum()
    x_sum(1)
    relay(0)
    x_sum(2)
    relay(3)
    relay(1)
    gather(0)
    relay(2)
    gather(3)
    losses_out()
    gather(1)
    gather(2)
    losses_in()

    phase("arrivals")
    got(lg.at[:, pl.ds(0, 3 * U)], lgs)
    phase("arr_gr")
    got(gr.at[:, pl.ds(0, 3 * U)], grs)
    phase("arr_hg")
    got(hg.at[:, pl.ds(0, NZ * SH)], cc)
    phase("drain")
    sent(W5.at[pl.ds(0, 60 * DB // NX), pl.ds(0, U)], ws_s)
    sent(AX.at[0:3], ax_s)
    sent(lg.at[:, pl.ds(0, 3 * U)], lg_s)
    sent(CN.at[0:3], cn_s)
    sent(STA.at[0:7], sa_s)
    sent(STB.at[0:3], sb_s)
    sent(gr.at[:, pl.ds(0, 3 * U)], gr_s)
    sent(H.at[:, pl.ds(0, D // 2)], cs_s)
    sent(RR.at[0:3], ring_s)
    sent(JL.at[0:3], jn_s)
    sent(XS.at[0:3], x_s)
    sent(XF.at[0:3], xf_s)
    sent(ZR, zr_s)
    sent(hg.at[:, pl.ds(0, 3 * SH)], ag_s)
    sent(TA.at[0:7], ta_s)
    sent(TB.at[0:3], tb_s)
    sent(hg.at[:, pl.ds(0, NZ * SH)], cc_s)
    phase(None)
    assert used == {"s": NSEND, "r": NRECV, "l": NLOAD}, used


NSEND, NRECV, NLOAD = 18, 136, 5


def emit(lgv, grv, hgv, small, lg, gr, hg, tl, jl, sem):
    copies = []
    for src, dst in ((lgv, lg), (grv, gr), (hgv, hg)):
        for i in range(4):
            part = pl.ds(i * 88, 88)
            copies.append(pltpu.make_async_copy(src.at[part], dst.at[part], sem.at[len(copies)]))
    for d in copies:
        d.start()
    tl[...] = small[0, :T]
    jl[...] = small[0, 384 : 384 + JOBS]
    for d in copies:
        d.wait()


def vmem(*shape, dtype=BF16):
    return pltpu.VMEM(shape, dtype)


def shards(hidden, weight, down, up, labels, jobs):
    hbm = pl.BlockSpec(memory_space=pl.ANY)
    vm = pl.BlockSpec(memory_space=pltpu.VMEM)
    held = pl.pallas_call(
        kernel,
        out_shape=(vmem(T, V), vmem(T, V), vmem(T, D), vmem(1, 512, dtype=F32)),
        in_specs=[hbm] * 4 + [vm] * 2,
        out_specs=(vm, vm, vm, vm),
        scratch_shapes=[
            vmem(S, D),
            vmem(D, U + 256),
            vmem(DB, V),
            vmem(NK, S, CW, dtype=F32),
            vmem(S, U),
            vmem(NX, T, U + 256),
            vmem(NZ, 2, NX * RT, CW),
            vmem(NX, RT, SH),
            vmem(2, RT, SH),
            vmem(2, RT, CW),
            vmem(NX, XT, NZ * SH),
            vmem(2, XT, NZ * SH),
            vmem(2, XT, NZ * SH // 2),
            vmem(3, XT, SH),
            vmem(T, SH),
            vmem(S, 128, dtype=F32),
            vmem(S, 128, dtype=F32),
            vmem(S, 128),
            vmem(128, U),
            vmem(NX, 3, 8, 128, dtype=F32),
            vmem(NZ * NC, 2, 16, 128, dtype=F32),
            vmem(NX, 2, 16, 128, dtype=F32),
            vmem(NZ * NC, 16, 128, dtype=F32),
            vmem(NX, 16, 128, dtype=F32),
            vmem(16, 128, dtype=F32),
            vmem(NY, 8, 128, dtype=F32),
            vmem(NY, 8, 128, dtype=F32),
            pltpu.SemaphoreType.DMA((NSEND,)),
            pltpu.SemaphoreType.DMA((NRECV,)),
            pltpu.SemaphoreType.DMA((NLOAD,)),
        ],
        compiler_params=pltpu.CompilerParams(
            collective_id=0, has_side_effects=True, vmem_limit_bytes=53 * 1024 * 1024
        ),
        name="step",
    )(hidden, weight, down, up, labels, jobs)
    return pl.pallas_call(
        emit,
        out_shape=(
            jax.ShapeDtypeStruct((T, V), BF16),
            jax.ShapeDtypeStruct((T, V), BF16),
            jax.ShapeDtypeStruct((T, D), BF16),
            jax.ShapeDtypeStruct((T,), F32),
            jax.ShapeDtypeStruct((JOBS,), F32),
        ),
        in_specs=[vm] * 4,
        out_specs=(hbm, hbm, hbm, vm, vm),
        scratch_shapes=[pltpu.SemaphoreType.DMA((12,))],
        compiler_params=pltpu.CompilerParams(vmem_limit_bytes=1024 * 1024),
        name="emit",
    )(*(pltpu.with_memory_space_constraint(i, pltpu.VMEM) for i in held))


def solution(mesh):
    split = Mesh(mesh.devices.reshape(NZ, NC, NX, NY), ("z", "c", "x", "y"))
    dp, vocab = ("x", "y"), ("z", "c")
    return jax.shard_map(
        shards,
        mesh=split,
        in_specs=(P(dp, None), P(dp, vocab), P(), P(None, vocab), P(dp), P(dp)),
        out_specs=(P(dp, vocab), P(dp, vocab), P(dp, None), P(dp), P()),
        check_vma=False,
    )
```
